512 devices in a mesh: row: 32 (over z, y_lo, core), col: 16 (over x, y_hi).
Axes of the slice: x: 4, y: 8 (y_hi: 4, y_lo: 2; y = y_hi * 2 + y_lo), z: 8, core: 2. Of those that a mesh axis runs over, the one named last changes fastest.
Arguments:
- pair_exchange: bfloat16 [1024, 16, 1024], P(('row', 'col')), may hold values from -6 to 6
- conduction: bfloat16 [1024, 4, 1024], P(('row', 'col')), may hold values from -6 to 6
- valence: bfloat16 [1024, 4, 1024], P(('row', 'col')), may hold values from -6 to 6
- coulomb: float32 [1024], replicated, may hold values from 0.5 to 5
- screening: float32 [289, 1024], replicated, may hold values from 0.1 to 1
- energies: float32 [1024, 16], P(('row', 'col')), may hold values from 1 to 9
- vectors: bfloat16 [1024, 512], P(('row', 'col')), may hold values from -6 to 6
- k_coords: int32 [1024, 2], P(('row', 'col')), may hold values from 0 to 31, as said below
Outputs:
- residual_block: float32 [1024, 512], P(('row', 'col'))
- alpha: float32 [32, 32], replicated
The draws below stay inside these ranges and needn't reach their ends.
Inputs may be any that keep to these rules, and one draw needn't show every extreme that they name: `k_coords`: each row holds a k-point's coordinates on the periodic 32 x 32 mesh, first then second; every mesh point occurs exactly once.
All inputs are finite; a program needn't handle non-finite values.
Results may differ from the reference program's by a relative error of at most 0.0028.
Values may be sent and summed in bfloat16 or wider, within the bound.
No kernel may reach another device: no remote copies, remote signals or barrier semaphores. Data moves between devices by JAX's collectives and lax.ppermute only.
A program may use at most 64 MiB of HBM per device.

```python
import math
import jax
import jax.numpy as jnp
from jax import lax

NV = 4
NC = 4
NB = 16
NG = 1024
NVEC = 32
MX = 32
NK = 1024
MY = 32
NT = 16384
NQF = 289


def draw_energies(key, part):
    ramp = 1.0 + 2.0 * jnp.arange(NK, dtype=jnp.float32)[:, None] / NK
    base = jnp.exp(jax.random.uniform(key, (NK, NB), jnp.float32, 0.0, math.log(3.0)))
    return (base * ramp).astype(jnp.float32)


def draw_k_coords(key, part):
    order = jax.random.permutation(key, NK)
    return jnp.stack([order // MY, order % MY], axis=1).astype(jnp.int32)


def block_levels(key, dims, shards, least, largest):
    level = 1.0
    for axis_at, blocks in shards:
        draws = jax.random.uniform(jax.random.fold_in(jax.random.fold_in(key, 6), axis_at), (blocks,), jnp.float32, least / len(shards), largest / len(shards))
        level = level * jnp.repeat(jnp.exp(draws), dims[axis_at] // blocks).reshape((-1,) + (1,) * (len(dims) - 1 - axis_at))
    return level


def bell_draw(own_key, extent, spread, limit, cuts=(), kind=jnp.bfloat16):
    factor_of = block_levels(own_key, extent, cuts, -0.22, 0.18) if cuts else 1.0
    values = jax.random.normal(own_key, extent, jnp.float32) * spread * factor_of
    return jnp.minimum(jnp.maximum(values, -limit), limit).astype(kind)


def setup_inputs(seed: int = 0) -> dict:
    key_of = jax.random.split(jax.random.key(seed), 9)
    pair_exchange = bell_draw(key_of[0], (NK, NB, NG), 1.0, 6.0, ((0, 512),))
    conduction = bell_draw(key_of[1], (NK, NC, NG), 1.0, 6.0, ((0, 512),))
    valence = bell_draw(key_of[2], (NK, NV, NG), 1.0, 6.0, ((0, 512),))
    coulomb = jnp.clip(jnp.exp(jax.random.uniform(key_of[3], (NG,), jnp.float32, math.log(0.5), math.log(5.0))), 0.5, 5.0)
    screening = jnp.clip(jnp.exp(jax.random.uniform(key_of[4], (NQF, NG), jnp.float32, math.log(0.1), math.log(1.0))), 0.1, 1.0)
    energies = draw_energies(jax.random.fold_in(key_of[8], 71), 0)
    vectors = bell_draw(key_of[6], (NK, NB * NVEC), 1.0, 6.0, ((0, 512),))
    k_coords = draw_k_coords(jax.random.fold_in(key_of[8], 71), 0)
    return dict(pair_exchange=pair_exchange, conduction=conduction, valence=valence, coulomb=coulomb, screening=screening, energies=energies, vectors=vectors, k_coords=k_coords)


highest = lax.Precision.HIGHEST


def reference(pair_exchange, conduction, valence, coulomb, screening, energies, vectors, k_coords):
    moving = vectors.astype(jnp.float32).reshape(NK, NB, NVEC)
    joined = (valence.astype(jnp.float32)[:, :, None, :] * conduction.astype(jnp.float32)[:, None, :, :]).reshape(NK, NB, NG)
    pair_rows = lax.optimization_barrier(joined.astype(jnp.bfloat16)).astype(jnp.float32)
    along_first = jnp.arange(MX)
    along_second = jnp.arange(MY)
    fold_first = jnp.minimum(along_first, MX - along_first)
    fold_second = jnp.minimum(along_second, MY - along_second)
    mesh_index = (fold_first[:, None] * (MY // 2 + 1) + fold_second[None, :]).astype(jnp.int32)
    spectrum = jnp.fft.fft2(screening[mesh_index], axes=(0, 1)).real
    density = jnp.einsum("ktg,ktn->gn", pair_exchange.astype(jnp.float32), moving, precision=highest)
    place_first = k_coords[:, 0]
    place_second = k_coords[:, 1]
    block_size = 64 if NG % 64 == 0 else NG

    def one_block(running, anchor):
        piece_rows = lax.dynamic_slice_in_dim(pair_rows, anchor, block_size, 2)
        projected = jnp.einsum("ktg,ktn->kgn", piece_rows, moving, precision=highest)
        mesh_grid = jnp.zeros((MX, MY, block_size, NVEC), jnp.float32).at[place_first, place_second].set(projected)
        spectrum_part = lax.dynamic_slice_in_dim(spectrum, anchor, block_size, 2)
        potential = jnp.fft.ifft2(jnp.fft.fft2(mesh_grid, axes=(0, 1)) * spectrum_part[:, :, :, None], axes=(0, 1)).real
        sampled = potential[place_first, place_second]
        return running + jnp.einsum("ktg,kgn->ktn", piece_rows, sampled, precision=highest), None

    anchors = (jnp.arange(NG // block_size) * block_size).astype(jnp.int32)
    direct, _ = lax.scan(one_block, jnp.zeros((NK, NB, NVEC), jnp.float32), anchors)
    exchange_term = jnp.einsum("ktg,gn->ktn", pair_exchange.astype(jnp.float32) * coulomb, density, precision=highest)
    applied = energies[:, :, None] * moving + (2.0 / NT) * exchange_term - direct / NK
    alpha = jnp.einsum("ktm,ktn->mn", moving, applied, precision=highest) / NT
    residual = applied - jnp.einsum("ktm,mn->ktn", moving, alpha, precision=highest)
    return residual.reshape(NK, NB * NVEC), alpha
```

```python
import jax
import jax.numpy as jnp
import numpy as np
from jax import lax
from jax.experimental import pallas as pl
from jax.experimental.pallas import tpu as pltpu
from jax.sharding import Mesh
from jax.sharding import PartitionSpec as P

MX = 32
MY = 32
NK = 1024
NB = 16
NG = 1024
NV = 32
NT = NK * NB
NQ = 289
NAMES = ("zh", "zl", "yl", "c", "x", "yh")
SIZES = (4, 2, 2, 2, 4, 4)
A = ("x", "yh", "yl")
B = ("zh", "zl", "c")
NA = 32
NBB = 16
ND = NA * NBB
HALF = NG // 2
LANES = 128

f32 = jnp.float32
bf16 = jnp.bfloat16
HIGH = lax.Precision.HIGHEST


def split_table(x):
    hi = x.astype(bf16)
    lo = (x - hi.astype(np.float64)).astype(bf16)
    return np.concatenate([hi, lo], axis=0)


def cas_tables():
    m = np.arange(32)
    phase = 2.0 * np.pi * ((m[:, None] * m[None, :]) % 32) / 32.0
    cas = np.cos(phase) + np.sin(phase)
    first = np.repeat(cas, 32, axis=1)
    second = np.tile(cas, (1, 32)) / 32.0
    return split_table(first), split_table(second)


def cos_table():
    f = np.arange(17)
    m = np.arange(32)
    weight = np.where((f == 0) | (f == 16), 1.0, 2.0)
    c = weight[:, None] * np.cos(2.0 * np.pi * ((f[:, None] * m[None, :]) % 32) / 32.0)
    return np.einsum("im,jn->ijmn", c, c).reshape(NQ, NK).astype(np.float32)


def iota(shape, axis):
    return lax.broadcasted_iota(jnp.int32, shape, axis)


def block_sum(x):
    x = x + pltpu.roll(x, 32, 1)
    return x + pltpu.roll(x, 64, 1)


def keep_block(x, wanted):
    return jnp.where(iota(x.shape, 1) // 32 == wanted, x, 0.0)


def spread_vectors(vec_ref, wide):
    rows = [
        vec_ref[k : k + 1, v * LANES : (v + 1) * LANES].astype(f32)
        for k in range(2)
        for v in range(4)
    ]
    x8 = jnp.concatenate(rows, axis=0)
    for c in range(4):
        wide[pl.ds(c, 8, stride=4), :] = x8
    x = wide[...]
    return block_sum(keep_block(x, iota(x.shape, 0) % 4))


def energy_column(energy_ref):
    first = jnp.broadcast_to(energy_ref[0:1, :], (NB, NB))
    second = jnp.broadcast_to(energy_ref[1:2, :], (NB, NB))
    e = jnp.concatenate([first, second], axis=0)
    return jnp.sum(
        jnp.where(iota(e.shape, 1) == iota(e.shape, 0) % NB, e, 0.0), axis=1, keepdims=True
    )


def exchange_rows(pe_ref):
    return jnp.concatenate(
        [pe_ref[k, :, g * HALF : (g + 1) * HALF] for g in range(2) for k in range(2)], axis=0
    )


def dot_t(x, y):
    return lax.dot_general(x, y, (((0,), (0,)), ((), ())), preferred_element_type=f32)


def dot_nt(x, y):
    return lax.dot_general(x, y, (((1,), (1,)), ((), ())), preferred_element_type=f32)


def pack_kernel(coords, cond, val, pe, vec, energy, msg, pairs, gram, wide, rows, lines):
    x = spread_vectors(vec, wide)
    for k in range(2):
        cf = cond[k].astype(f32)
        vf = val[k].astype(f32)
        for v in range(4):
            both = vf[v : v + 1, :] * cf
            for g in range(2):
                at = k * 32 + g * 16 + v * 4
                rows[at : at + 4, :] = both[:, g * HALF : (g + 1) * HALF]
    left = rows[...].astype(bf16)
    pairs[...] = left
    xp = jnp.concatenate([x[0:16], x[0:16], x[16:32], x[16:32]], axis=0)
    xp = keep_block(xp, iota(xp.shape, 0) // 16).astype(bf16)
    xd = jnp.concatenate([x, x], axis=0)
    xd = keep_block(xd, iota(xd.shape, 0) // 32).astype(bf16)
    lane = iota((1, LANES), 1)
    place = jnp.zeros((1, LANES), f32)
    for k in range(2):
        for s in range(2):
            place = jnp.where(lane == 64 + 2 * k + s, coords[k, s].astype(f32), place)
    lines[pl.ds(0, ND, stride=2), :] = dot_t(left, xp)
    lines[pl.ds(1, ND, stride=2), :] = dot_t(exchange_rows(pe), xd) + place
    msg[...] = lines[...].astype(bf16)
    gram[...] = lax.dot_general(
        x[:, 0:32],
        energy_column(energy) * x,
        (((0,), (0,)), ((), ())),
        precision=HIGH,
        preferred_element_type=f32,
    )


def spectrum_kernel(where, low, high, cos, lam):
    lane = iota((NQ, LANES), 1)
    out = []
    for ref in (low, high):
        column = jnp.sum(jnp.where(lane == where[1], ref[...], 0.0), axis=1, keepdims=True)
        out.append(jnp.sum(column * cos[...], axis=0, keepdims=True))
    lam[...] = jnp.concatenate(out + [jnp.zeros((6, NK), f32)], axis=0)


def spectral_kernel(where, got, lam, gram, coulomb, first, second, msg, lines, wide):
    lines[...] = got[...].astype(f32)
    proj = lines[pl.ds(0, ND, stride=2), :].astype(bf16)
    rest = lines[pl.ds(1, ND, stride=2), :]
    basis = []
    hat = None
    slot = iota((ND, 64), 1) % 32
    for k in range(2):
        at = [rest[:, 64 + 2 * k + s : 65 + 2 * k + s].astype(jnp.int32) for s in range(2)]
        ones = [jnp.where(slot == p, 1.0, 0.0).astype(bf16) for p in at]
        ta = jnp.dot(ones[0], first[...], preferred_element_type=f32)
        tb = jnp.dot(ones[1], second[...], preferred_element_type=f32)
        t = (ta * tb).astype(bf16)
        basis.append(t)
        part = dot_t(proj, t)[k * 64 : (k + 1) * 64]
        hat = part if hat is None else hat + part
    scale = jnp.concatenate(
        [jnp.broadcast_to(lam[0:1, :], (32, NK)), jnp.broadcast_to(lam[1:2, :], (32, NK))], axis=0
    )
    scaled = (hat * scale).astype(bf16)
    hat = hat.astype(bf16)
    none = jnp.zeros((64, NK), bf16)
    lines[0:ND, :] = dot_nt(basis[0], jnp.concatenate([scaled, none], axis=0)) + dot_nt(
        basis[1], jnp.concatenate([none, scaled], axis=0)
    )
    for a in range(NA):
        msg[a, 0:16, :] = lines[pl.ds(a, NBB, stride=NA), :].astype(bf16)
    direct = dot_nt(hat[0:32], jnp.concatenate([scaled[0:32]] * 4, axis=0)) + dot_nt(
        hat[32:64], jnp.concatenate([scaled[32:64]] * 4, axis=0)
    )
    lane = iota((1, LANES), 1)
    dens = jnp.sum(rest, axis=0, keepdims=True)
    index = iota((8, LANES), 0) * LANES + iota((8, LANES), 1)
    outer = jnp.zeros((32, LANES), f32)
    cd = jnp.zeros((1, LANES), f32)
    for g in range(2):
        factor = jnp.sum(jnp.where(index == where[0] + g * HALF, coulomb[...], 0.0), keepdims=True)
        own = jnp.where(lane // 32 == g, dens, 0.0)
        row = block_sum(own)
        column = jnp.sum(
            jnp.where(iota((32, LANES), 0) == iota((32, LANES), 1), row, 0.0), axis=1, keepdims=True
        )
        outer = outer + column * (factor * row)
        cd = cd + factor * own
    alpha = (gram[...] + (2.0 / NT) * outer - direct / NK) / NT
    wide[...] = keep_block(alpha, iota((32, LANES), 0) % 4)
    packed = wide[pl.ds(0, 8, stride=4), :]
    for c in range(1, 4):
        packed = packed + wide[pl.ds(c, 8, stride=4), :]
    tail = jnp.concatenate([packed, jnp.broadcast_to(cd, (8, LANES))], axis=0).astype(bf16)
    msg[:, 16:32, :] = jnp.broadcast_to(tail[None], (NA, 16, LANES))


def relay_kernel(got, msg, lines):
    for a in range(NA):
        lines[a * 32 : (a + 1) * 32, :] = got[a].astype(f32)
    alpha = lines[16:24, :]
    for a in range(1, NA):
        alpha = alpha + lines[a * 32 + 16 : a * 32 + 24, :]
    hi = alpha.astype(bf16)
    lo = (alpha - hi.astype(f32)).astype(bf16)
    cd = lines[pl.ds(24, NA, stride=32), :].astype(bf16)
    tail = jnp.concatenate([cd, hi, lo], axis=0)
    for s in range(NBB):
        msg[s, 0:32, :] = lines[pl.ds(s, NA, stride=32), :].astype(bf16)
        msg[s, 32:80, :] = tail


def finish_kernel(got, pairs, pe, vec, energy, out, alpha_out, wide, rows):
    x = spread_vectors(vec, wide)
    potential = got[:, 0:32, :].reshape(ND, LANES)
    field = got[:, 32:64, :].reshape(ND, LANES)
    direct = jnp.dot(pairs[...], potential, preferred_element_type=f32)
    direct = block_sum(keep_block(direct, iota(direct.shape, 0) // 16))
    direct = jnp.concatenate([direct[0:16] + direct[16:32], direct[32:48] + direct[48:64]], axis=0)
    exchange = jnp.dot(exchange_rows(pe), field, preferred_element_type=f32)
    exchange = block_sum(keep_block(exchange, iota(exchange.shape, 0) // 32))
    exchange = exchange[0:32] + exchange[32:64]
    applied = energy_column(energy) * x + (2.0 / NT) * exchange - direct / NK
    alpha = jnp.zeros((16, LANES), f32)
    for b in range(NBB):
        alpha = alpha + got[b, 64:80, :].astype(f32)
    alpha = alpha[0:8] + alpha[8:16]
    for c in range(4):
        wide[pl.ds(c, 8, stride=4), :] = alpha
    full = wide[...]
    full = block_sum(keep_block(full, iota(full.shape, 0) % 4))
    alpha_out[...] = full[:, 0:32]
    shift = jnp.dot(x[:, 0:32], full, precision=HIGH, preferred_element_type=f32)
    rows[...] = keep_block(applied - shift, iota((32, LANES), 0) % 4)
    packed = rows[pl.ds(0, 8, stride=4), :]
    for c in range(1, 4):
        packed = packed + rows[pl.ds(c, 8, stride=4), :]
    for k in range(2):
        for v in range(4):
            out[k : k + 1, v * LANES : (v + 1) * LANES] = packed[k * 4 + v : k * 4 + v + 1, :]


def vmem():
    return pl.BlockSpec(memory_space=pltpu.VMEM)


def smem():
    return pl.BlockSpec(memory_space=pltpu.SMEM)


def sds(shape, dtype):
    return jax.ShapeDtypeStruct(shape, dtype)


def on_device(pair_exchange, conduction, valence, coulomb, screening, energies, vectors, k_coords):
    mine = lax.axis_index(B) * NA + lax.axis_index(A)
    msg, pairs, gram = pl.pallas_call(
        pack_kernel,
        out_shape=(sds((2 * ND, LANES), bf16), sds((64, HALF), bf16), sds((32, LANES), f32)),
        in_specs=[smem()] + [vmem()] * 5,
        out_specs=(vmem(),) * 3,
        scratch_shapes=[
            pltpu.VMEM((32, LANES), f32),
            pltpu.VMEM((64, HALF), f32),
            pltpu.VMEM((2 * ND, LANES), f32),
        ],
        name="pack",
    )(k_coords, conduction, valence, pair_exchange, vectors, energies)
    got = lax.all_to_all(msg.reshape(ND, 2, LANES), B + A, 0, 0, tiled=True)
    place = jnp.stack([mine // LANES, mine % LANES]).astype(jnp.int32)
    lam = pl.pallas_call(
        spectrum_kernel,
        out_shape=sds((8, NK), f32),
        grid_spec=pltpu.PrefetchScalarGridSpec(
            num_scalar_prefetch=1,
            grid=(1,),
            in_specs=[
                pl.BlockSpec((NQ, LANES), lambda i, w: (0, w[0])),
                pl.BlockSpec((NQ, LANES), lambda i, w: (0, w[0] + HALF // LANES)),
                pl.BlockSpec((NQ, NK), lambda i, w: (0, 0)),
            ],
            out_specs=pl.BlockSpec((8, NK), lambda i, w: (0, 0)),
        ),
        name="spectrum",
    )(place, screening, screening, cos_table())
    first, second = cas_tables()
    out = pl.pallas_call(
        spectral_kernel,
        out_shape=sds((NA, 32, LANES), bf16),
        in_specs=[smem()] + [vmem()] * 6,
        out_specs=vmem(),
        scratch_shapes=[pltpu.VMEM((2 * ND, LANES), f32), pltpu.VMEM((32, LANES), f32)],
        name="spectral",
    )(
        mine.reshape(1).astype(jnp.int32),
        got.reshape(2 * ND, LANES),
        lam,
        gram,
        coulomb.reshape(8, LANES),
        first,
        second,
    )
    got = lax.all_to_all(out, A, 0, 0, tiled=True)
    out = pl.pallas_call(
        relay_kernel,
        out_shape=sds((NBB, 80, LANES), bf16),
        in_specs=[vmem()],
        out_specs=vmem(),
        scratch_shapes=[pltpu.VMEM((NA * 32, LANES), f32)],
        name="relay",
    )(got)
    got = lax.all_to_all(out, B, 0, 0, tiled=True)
    return pl.pallas_call(
        finish_kernel,
        out_shape=(sds((2, NB * NV), f32), sds((NV, NV), f32)),
        in_specs=[vmem()] * 5,
        out_specs=(vmem(), vmem()),
        scratch_shapes=[pltpu.VMEM((32, LANES), f32), pltpu.VMEM((32, LANES), f32)],
        name="finish",
    )(got, pairs, pair_exchange, vectors, energies)


def solution(mesh):
    split = Mesh(mesh.devices.reshape(SIZES), NAMES)
    return jax.shard_map(
        on_device,
        mesh=split,
        in_specs=(
            P(NAMES, None, None),
            P(NAMES, None, None),
            P(NAMES, None, None),
            P(),
            P(),
            P(NAMES, None),
            P(NAMES, None),
            P(NAMES, None),
        ),
        out_specs=(P(NAMES, None), P()),
        check_vma=False,
    )
```

```python
import jax
import jax.numpy as jnp
import numpy as np
from jax import lax
from jax.experimental import pallas as pl
from jax.experimental.pallas import tpu as pltpu
from jax.sharding import Mesh
from jax.sharding import PartitionSpec as P

MX = 32
MY = 32
NK = 1024
NB = 16
NG = 1024
NV = 32
NT = NK * NB
NQ = 289
NAMES = ("zh", "zl", "yl", "c", "x", "yh")
SIZES = (4, 2, 2, 2, 4, 4)
A = ("x", "yh", "yl")
B = ("zh", "zl", "c")
NA = 32
NBB = 16
ND = NA * NBB
HALF = NG // 2
ROWS = 26
LANES = 128

f32 = jnp.float32
bf16 = jnp.bfloat16
HIGH = lax.Precision.HIGHEST


def split_table(x):
    hi = x.astype(bf16)
    lo = (x - hi.astype(np.float64)).astype(bf16)
    return np.concatenate([hi, lo], axis=0)


def cas_tables():
    m = np.arange(32)
    phase = 2.0 * np.pi * ((m[:, None] * m[None, :]) % 32) / 32.0
    cas = np.cos(phase) + np.sin(phase)
    first = np.repeat(cas, 32, axis=1)
    second = np.tile(cas, (1, 32)) / 32.0
    return split_table(first), split_table(second)


def cos_table():
    f = np.arange(17)
    m = np.arange(32)
    weight = np.where((f == 0) | (f == 16), 1.0, 2.0)
    c = weight[:, None] * np.cos(2.0 * np.pi * ((f[:, None] * m[None, :]) % 32) / 32.0)
    return np.einsum("im,jn->ijmn", c, c).reshape(NQ, NK).astype(np.float32)


def iota(shape, axis):
    return lax.broadcasted_iota(jnp.int32, shape, axis)


def block_sum(x):
    x = x + pltpu.roll(x, 32, 1)
    return x + pltpu.roll(x, 64, 1)


def keep_block(x, wanted):
    return jnp.where(iota(x.shape, 1) // 32 == wanted, x, 0.0)


def spread_vectors(vec_ref, wide):
    rows = [
        vec_ref[k : k + 1, v * LANES : (v + 1) * LANES].astype(f32)
        for k in range(2)
        for v in range(4)
    ]
    x8 = jnp.concatenate(rows, axis=0)
    for c in range(4):
        wide[pl.ds(c, 8, stride=4), :] = x8
    x = wide[...]
    return block_sum(keep_block(x, iota(x.shape, 0) % 4))


def energy_column(energy_ref):
    first = jnp.broadcast_to(energy_ref[0:1, :], (NB, NB))
    second = jnp.broadcast_to(energy_ref[1:2, :], (NB, NB))
    e = jnp.concatenate([first, second], axis=0)
    return jnp.sum(
        jnp.where(iota(e.shape, 1) == iota(e.shape, 0) % NB, e, 0.0), axis=1, keepdims=True
    )


def exchange_rows(pe_ref):
    return jnp.concatenate(
        [pe_ref[k, :, g * HALF : (g + 1) * HALF] for g in range(2) for k in range(2)], axis=0
    )


def dot_t(x, y):
    return lax.dot_general(x, y, (((0,), (0,)), ((), ())), preferred_element_type=f32)


def dot_nt(x, y):
    return lax.dot_general(x, y, (((1,), (1,)), ((), ())), preferred_element_type=f32)


def pack_kernel(
    mine, coords, cond, val, pe, vec, energy, low, high, cos, msg, pairs, gram, lam, wide, rows, lines
):
    x = spread_vectors(vec, wide)
    for k in range(2):
        cf = cond[k].astype(f32)
        vf = val[k].astype(f32)
        for v in range(4):
            both = vf[v : v + 1, :] * cf
            for g in range(2):
                at = k * 32 + g * 16 + v * 4
                rows[at : at + 4, :] = both[:, g * HALF : (g + 1) * HALF]
    left = rows[...].astype(bf16)
    pairs[...] = left
    xp = jnp.concatenate([x[0:16], x[0:16], x[16:32], x[16:32]], axis=0)
    xp = keep_block(xp, iota(xp.shape, 0) // 16).astype(bf16)
    xd = jnp.concatenate([x, x], axis=0)
    xd = keep_block(xd, iota(xd.shape, 0) // 32).astype(bf16)
    lane = iota((1, LANES), 1)
    place = jnp.zeros((1, LANES), f32)
    for k in range(2):
        for s in range(2):
            place = jnp.where(lane == 64 + 2 * k + s, coords[k, s].astype(f32), place)
    lines[pl.ds(0, ND, stride=2), :] = dot_t(left, xp)
    lines[pl.ds(1, ND, stride=2), :] = dot_t(exchange_rows(pe), xd) + place
    msg[...] = lines[...].astype(bf16)
    gram[...] = lax.dot_general(
        x[:, 0:32],
        energy_column(energy) * x,
        (((0,), (0,)), ((), ())),
        precision=HIGH,
        preferred_element_type=f32,
    )
    own = iota((NQ, LANES), 1) == mine[0] % LANES
    out = []
    for ref in (low, high):
        column = jnp.sum(jnp.where(own, ref[...], 0.0), axis=1, keepdims=True)
        out.append(jnp.sum(column * cos[...], axis=0, keepdims=True))
    lam[...] = jnp.concatenate(out + [jnp.zeros((6, NK), f32)], axis=0)


def spectral_kernel(where, got, lam, gram, coulomb, first, second, msg, lines, wide):
    lines[...] = got[...].astype(f32)
    proj = lines[pl.ds(0, ND, stride=2), :].astype(bf16)
    rest = lines[pl.ds(1, ND, stride=2), :]
    basis = []
    hat = None
    slot = iota((ND, 64), 1) % 32
    for k in range(2):
        at = [rest[:, 64 + 2 * k + s : 65 + 2 * k + s].astype(jnp.int32) for s in range(2)]
        ones = [jnp.where(slot == p, 1.0, 0.0).astype(bf16) for p in at]
        ta = jnp.dot(ones[0], first[...], preferred_element_type=f32)
        tb = jnp.dot(ones[1], second[...], preferred_element_type=f32)
        exact = ta * tb
        hi = exact.astype(bf16)
        lo = (exact - hi.astype(f32)).astype(bf16)
        basis.append((hi, lo))
        part = (dot_t(proj, hi) + dot_t(proj, lo))[k * 64 : (k + 1) * 64]
        hat = part if hat is None else hat + part
    scale = jnp.concatenate(
        [jnp.broadcast_to(lam[0:1, :], (32, NK)), jnp.broadcast_to(lam[1:2, :], (32, NK))], axis=0
    )
    exact = hat * scale
    scaled = exact.astype(bf16)
    finer = (exact - scaled.astype(f32)).astype(bf16)
    hat = hat.astype(bf16)
    both = jnp.concatenate([scaled, finer], axis=0)
    side = iota((ND, LANES), 1) // 64
    back = []
    for hi, lo in basis:
        r = dot_nt(hi, both)
        back.append(r + pltpu.roll(r, 64, 1) + dot_nt(lo, jnp.concatenate([scaled] * 2, axis=0)))
    back = jnp.where(side == 0, back[0], back[1])
    for b in range(NBB):
        lines[pl.ds(b, NA, stride=ROWS), :] = back[b * NA : (b + 1) * NA]
    direct = dot_nt(hat[0:32], jnp.concatenate([scaled[0:32]] * 4, axis=0)) + dot_nt(
        hat[32:64], jnp.concatenate([scaled[32:64]] * 4, axis=0)
    )
    lane = iota((1, LANES), 1)
    dens = jnp.sum(rest, axis=0, keepdims=True)
    index = iota((8, LANES), 0) * LANES + iota((8, LANES), 1)
    outer = jnp.zeros((32, LANES), f32)
    cd = jnp.zeros((1, LANES), f32)
    for g in range(2):
        factor = jnp.sum(jnp.where(index == where[0] + g * HALF, coulomb[...], 0.0), keepdims=True)
        own = jnp.where(lane // 32 == g, dens, 0.0)
        row = block_sum(own)
        column = jnp.sum(
            jnp.where(iota((32, LANES), 0) == iota((32, LANES), 1), row, 0.0), axis=1, keepdims=True
        )
        outer = outer + column * (factor * row)
        cd = cd + factor * own
    alpha = (gram[...] + (2.0 / NT) * outer - direct / NK) / NT
    wide[...] = keep_block(alpha, iota((32, LANES), 0) % 4)
    packed = wide[pl.ds(0, 8, stride=4), :]
    for c in range(1, 4):
        packed = packed + wide[pl.ds(c, 8, stride=4), :]
    tail = jnp.concatenate([packed, cd, jnp.zeros((1, LANES), f32)], axis=0)
    for r in range(ROWS - NBB):
        lines[pl.ds(NBB + r, NA, stride=ROWS), :] = jnp.broadcast_to(tail[r : r + 1], (NA, LANES))
    msg[...] = lines[0 : NA * ROWS, :].astype(bf16)


def relay_kernel(got, msg, lines):
    lines[...] = got[...].astype(f32)
    alpha = []
    for r in range(8):
        part = lines[pl.ds(NBB + r, NA, stride=ROWS), :]
        alpha.append(jnp.sum(part, axis=0, keepdims=True))
    alpha = jnp.concatenate(alpha, axis=0)
    hi = alpha.astype(bf16).astype(f32)
    cd = lines[pl.ds(NBB + 8, NA, stride=ROWS), :]
    cd = cd[0:16] + pltpu.roll(cd[16:32], 64, 1)
    tail = jnp.concatenate([cd, hi, alpha - hi], axis=0).astype(bf16)
    for b in range(NBB):
        msg[b, 0:32, :] = lines[pl.ds(b, NA, stride=ROWS), :].astype(bf16)
        msg[b, 32:64, :] = tail


def finish_kernel(got, pairs, pe, vec, energy, out, alpha_out, wide, rows):
    x = spread_vectors(vec, wide)
    potential = got[:, 0:32, :].reshape(ND, LANES)
    field = []
    for b in range(NBB):
        part = got[b, 32:48, :].astype(f32)
        field += [part, pltpu.roll(part, 64, 1)]
    field = jnp.concatenate(field, axis=0).astype(bf16)
    direct = jnp.dot(pairs[...], potential, preferred_element_type=f32)
    direct = block_sum(keep_block(direct, iota(direct.shape, 0) // 16))
    direct = jnp.concatenate([direct[0:16] + direct[16:32], direct[32:48] + direct[48:64]], axis=0)
    exchange = jnp.dot(exchange_rows(pe), field, preferred_element_type=f32)
    exchange = block_sum(keep_block(exchange, iota(exchange.shape, 0) // 32))
    exchange = exchange[0:32] + exchange[32:64]
    applied = energy_column(energy) * x + (2.0 / NT) * exchange - direct / NK
    alpha = jnp.zeros((16, LANES), f32)
    for b in range(NBB):
        alpha = alpha + got[b, 48:64, :].astype(f32)
    alpha = alpha[0:8] + alpha[8:16]
    for c in range(4):
        wide[pl.ds(c, 8, stride=4), :] = alpha
    full = wide[...]
    full = block_sum(keep_block(full, iota(full.shape, 0) % 4))
    alpha_out[...] = full[:, 0:32]
    shift = jnp.dot(x[:, 0:32], full, precision=HIGH, preferred_element_type=f32)
    rows[...] = keep_block(applied - shift, iota((32, LANES), 0) % 4)
    packed = rows[pl.ds(0, 8, stride=4), :]
    for c in range(1, 4):
        packed = packed + rows[pl.ds(c, 8, stride=4), :]
    for k in range(2):
        for v in range(4):
            out[k : k + 1, v * LANES : (v + 1) * LANES] = packed[k * 4 + v : k * 4 + v + 1, :]


def vmem():
    return pl.BlockSpec(memory_space=pltpu.VMEM)


def smem():
    return pl.BlockSpec(memory_space=pltpu.SMEM)


def room(mib):
    return pltpu.CompilerParams(vmem_limit_bytes=mib << 20)


def sds(shape, dtype):
    return jax.ShapeDtypeStruct(shape, dtype)


def on_device(pair_exchange, conduction, valence, coulomb, screening, energies, vectors, k_coords):
    mine = (lax.axis_index(B) * NA + lax.axis_index(A)).reshape(1).astype(jnp.int32)
    fixed2 = lambda i, *w: (0, 0)
    fixed3 = lambda i, *w: (0, 0, 0)
    msg, pairs, gram, lam = pl.pallas_call(
        pack_kernel,
        out_shape=(
            sds((2 * ND, LANES), bf16),
            sds((64, HALF), bf16),
            sds((32, LANES), f32),
            sds((8, NK), f32),
        ),
        grid_spec=pltpu.PrefetchScalarGridSpec(
            num_scalar_prefetch=2,
            grid=(1,),
            in_specs=[
                pl.BlockSpec(conduction.shape, fixed3),
                pl.BlockSpec(valence.shape, fixed3),
                pl.BlockSpec(pair_exchange.shape, fixed3),
                pl.BlockSpec(vectors.shape, fixed2),
                pl.BlockSpec(energies.shape, fixed2),
                pl.BlockSpec((NQ, LANES), lambda i, w, c: (0, w[0] // LANES)),
                pl.BlockSpec((NQ, LANES), lambda i, w, c: (0, w[0] // LANES + HALF // LANES)),
                pl.BlockSpec((NQ, NK), fixed2),
            ],
            out_specs=[
                pl.BlockSpec((2 * ND, LANES), fixed2),
                pl.BlockSpec((64, HALF), fixed2),
                pl.BlockSpec((32, LANES), fixed2),
                pl.BlockSpec((8, NK), fixed2),
            ],
            scratch_shapes=[
                pltpu.VMEM((32, LANES), f32),
                pltpu.VMEM((64, HALF), f32),
                pltpu.VMEM((2 * ND, LANES), f32),
            ],
        ),
        compiler_params=room(12),
        name="pack",
    )(
        mine,
        k_coords,
        conduction,
        valence,
        pair_exchange,
        vectors,
        energies,
        screening,
        screening,
        cos_table(),
    )
    got = lax.all_to_all(msg.reshape(ND, 2, LANES), B + A, 0, 0, tiled=True)
    first, second = cas_tables()
    out = pl.pallas_call(
        spectral_kernel,
        out_shape=sds((NA * ROWS, LANES), bf16),
        in_specs=[smem()] + [vmem()] * 6,
        out_specs=vmem(),
        scratch_shapes=[pltpu.VMEM((2 * ND, LANES), f32), pltpu.VMEM((32, LANES), f32)],
        compiler_params=room(28),
        name="spectral",
    )(
        mine,
        got.reshape(2 * ND, LANES),
        lam,
        gram,
        coulomb.reshape(8, LANES),
        first,
        second,
    )
    got = lax.all_to_all(out.reshape(NA, ROWS // 2, 2, LANES), A, 0, 0, tiled=True)
    out = pl.pallas_call(
        relay_kernel,
        out_shape=sds((NBB, 64, LANES), bf16),
        in_specs=[vmem()],
        out_specs=vmem(),
        scratch_shapes=[pltpu.VMEM((NA * ROWS, LANES), f32)],
        compiler_params=room(8),
        name="relay",
    )(got.reshape(NA * ROWS, LANES))
    got = lax.all_to_all(out, B, 0, 0, tiled=True)
    return pl.pallas_call(
        finish_kernel,
        out_shape=(sds((2, NB * NV), f32), sds((NV, NV), f32)),
        in_specs=[vmem()] * 5,
        out_specs=(vmem(), vmem()),
        scratch_shapes=[pltpu.VMEM((32, LANES), f32), pltpu.VMEM((32, LANES), f32)],
        compiler_params=room(8),
        name="finish",
    )(got, pairs, pair_exchange, vectors, energies)


def solution(mesh):
    split = Mesh(mesh.devices.reshape(SIZES), NAMES)
    return jax.shard_map(
        on_device,
        mesh=split,
        in_specs=(
            P(NAMES, None, None),
            P(NAMES, None, None),
            P(NAMES, None, None),
            P(),
            P(),
            P(NAMES, None),
            P(NAMES, None),
            P(NAMES, None),
        ),
        out_specs=(P(NAMES, None), P()),
        check_vma=False,
    )
```

```python
import jax
import jax.numpy as jnp
import numpy as np
from jax import lax
from jax.experimental import pallas as pl
from jax.experimental.pallas import tpu as pltpu
from jax.sharding import Mesh
from jax.sharding import PartitionSpec as P

MX = 32
MY = 32
NK = 1024
NB = 16
NG = 1024
NV = 32
NT = NK * NB
NQ = 289
NAMES = ("zh", "zl", "yl", "c", "x", "yh")
SIZES = (4, 2, 2, 2, 4, 4)
A = ("x", "yh", "yl")
B = ("zh", "zl", "c")
NA = 32
NBB = 16
ND = NA * NBB
HALF = NG // 2
ROWS = 26
LANES = 128

f32 = jnp.float32
bf16 = jnp.bfloat16
HIGH = lax.Precision.HIGHEST


def split_table(x):
    hi = x.astype(bf16)
    lo = (x - hi.astype(np.float64)).astype(bf16)
    return np.concatenate([hi, lo], axis=0)


def cas_tables():
    m = np.arange(32)
    phase = 2.0 * np.pi * ((m[:, None] * m[None, :]) % 32) / 32.0
    cas = np.cos(phase) + np.sin(phase)
    first = np.repeat(cas, 32, axis=1)
    second = np.tile(cas, (1, 32)) / 32.0
    return split_table(first), split_table(second)


def cos_table():
    f = np.arange(17)
    m = np.arange(32)
    weight = np.where((f == 0) | (f == 16), 1.0, 2.0)
    c = weight[:, None] * np.cos(2.0 * np.pi * ((f[:, None] * m[None, :]) % 32) / 32.0)
    return np.einsum("im,jn->ijmn", c, c).reshape(NQ, NK).astype(np.float32)


def iota(shape, axis):
    return lax.broadcasted_iota(jnp.int32, shape, axis)


def block_sum(x):
    x = x + pltpu.roll(x, 32, 1)
    return x + pltpu.roll(x, 64, 1)


def keep_block(x, wanted):
    return jnp.where(iota(x.shape, 1) // 32 == wanted, x, 0.0)


def spread_vectors(vec_ref, wide):
    rows = [
        vec_ref[k : k + 1, v * LANES : (v + 1) * LANES].astype(f32)
        for k in range(2)
        for v in range(4)
    ]
    x8 = jnp.concatenate(rows, axis=0)
    for c in range(4):
        wide[pl.ds(c, 8, stride=4), :] = x8
    x = wide[...]
    return block_sum(keep_block(x, iota(x.shape, 0) % 4))


def energy_column(energy_ref):
    first = jnp.broadcast_to(energy_ref[0:1, :], (NB, NB))
    second = jnp.broadcast_to(energy_ref[1:2, :], (NB, NB))
    e = jnp.concatenate([first, second], axis=0)
    return jnp.sum(
        jnp.where(iota(e.shape, 1) == iota(e.shape, 0) % NB, e, 0.0), axis=1, keepdims=True
    )


def exchange_rows(pe_ref):
    return jnp.concatenate(
        [pe_ref[k, :, g * HALF : (g + 1) * HALF] for g in range(2) for k in range(2)], axis=0
    )


def dot_t(x, y):
    return lax.dot_general(x, y, (((0,), (0,)), ((), ())), preferred_element_type=f32)


def dot_nt(x, y):
    return lax.dot_general(x, y, (((1,), (1,)), ((), ())), preferred_element_type=f32)


def pack_kernel(
    mine, coords, cond, val, pe, vec, energy, *refs
):
    del mine
    far, (msg, pairs, gram), near, (wide, rows, lines, sem) = refs[:3], refs[3:6], refs[6:9], refs[9:]
    copies = [pltpu.make_async_copy(far[i], near[i], sem.at[i]) for i in range(3)]
    for copy in copies:
        copy.start()
    x = spread_vectors(vec, wide)
    for k in range(2):
        cf = cond[k].astype(f32)
        vf = val[k].astype(f32)
        for v in range(4):
            both = vf[v : v + 1, :] * cf
            for g in range(2):
                at = k * 32 + g * 16 + v * 4
                rows[at : at + 4, :] = both[:, g * HALF : (g + 1) * HALF]
    left = rows[...].astype(bf16)
    pairs[...] = left
    xp = jnp.concatenate([x[0:16], x[0:16], x[16:32], x[16:32]], axis=0)
    xp = keep_block(xp, iota(xp.shape, 0) // 16).astype(bf16)
    xd = jnp.concatenate([x, x], axis=0)
    xd = keep_block(xd, iota(xd.shape, 0) // 32).astype(bf16)
    lane = iota((1, LANES), 1)
    place = jnp.zeros((1, LANES), f32)
    for k in range(2):
        for s in range(2):
            place = jnp.where(lane == 64 + 2 * k + s, coords[k : k + 1, s : s + 1].astype(f32), place)
    lines[pl.ds(0, ND, stride=2), :] = dot_t(left, xp)
    lines[pl.ds(1, ND, stride=2), :] = dot_t(exchange_rows(pe), xd) + place
    msg[...] = lines[...].astype(bf16)
    gram[...] = lax.dot_general(
        x[:, 0:32],
        energy_column(energy) * x,
        (((0,), (0,)), ((), ())),
        precision=HIGH,
        preferred_element_type=f32,
    )
    for copy in copies:
        copy.wait()


def spectrum(mine, tiles, cos):
    own = iota((NQ, LANES), 1) == mine % LANES
    out = []
    for g in range(2):
        column = jnp.sum(jnp.where(own, tiles[g], 0.0), axis=1, keepdims=True)
        line = jnp.sum(column * cos[...], axis=0, keepdims=True)
        out.append(jnp.broadcast_to(line, (32, NK)))
    return jnp.concatenate(out, axis=0)


def spectral_kernel(
    where, got, gram, coulomb, first, second, table, far, msg, lines, wide, tiles, cos, sem
):
    tile = pl.multiple_of((where[0] // LANES) * LANES, LANES)
    copies = [
        pltpu.make_async_copy(table.at[:, pl.ds(tile + g * HALF, LANES)], tiles.at[g], sem.at[g])
        for g in range(2)
    ]
    copies.append(pltpu.make_async_copy(far, cos, sem.at[2]))
    for copy in copies:
        copy.start()
    lines[...] = got[...].astype(f32)
    proj = lines[pl.ds(0, ND, stride=2), :].astype(bf16)
    rest = lines[pl.ds(1, ND, stride=2), :]
    basis = []
    hat = None
    slot = iota((ND, 64), 1) % 32
    for k in range(2):
        at = [rest[:, 64 + 2 * k + s : 65 + 2 * k + s].astype(jnp.int32) for s in range(2)]
        ones = [jnp.where(slot == p, 1.0, 0.0).astype(bf16) for p in at]
        ta = jnp.dot(ones[0], first[...], preferred_element_type=f32)
        tb = jnp.dot(ones[1], second[...], preferred_element_type=f32)
        exact = ta * tb
        hi = exact.astype(bf16)
        lo = (exact - hi.astype(f32)).astype(bf16)
        basis.append((hi, lo))
        part = (dot_t(proj, hi) + dot_t(proj, lo))[k * 64 : (k + 1) * 64]
        hat = part if hat is None else hat + part
    for copy in copies:
        copy.wait()
    scale = spectrum(where[0], tiles, cos)
    exact = hat * scale
    scaled = exact.astype(bf16)
    finer = (exact - scaled.astype(f32)).astype(bf16)
    hat = hat.astype(bf16)
    both = jnp.concatenate([scaled, finer], axis=0)
    side = iota((ND, LANES), 1) // 64
    back = []
    for hi, lo in basis:
        r = dot_nt(hi, both)
        back.append(r + pltpu.roll(r, 64, 1) + dot_nt(lo, jnp.concatenate([scaled] * 2, axis=0)))
    back = jnp.where(side == 0, back[0], back[1])
    for b in range(NBB):
        lines[pl.ds(b, NA, stride=ROWS), :] = back[b * NA : (b + 1) * NA]
    direct = dot_nt(hat[0:32], jnp.concatenate([scaled[0:32]] * 4, axis=0)) + dot_nt(
        hat[32:64], jnp.concatenate([scaled[32:64]] * 4, axis=0)
    )
    lane = iota((1, LANES), 1)
    dens = jnp.sum(rest, axis=0, keepdims=True)
    index = iota((8, LANES), 0) * LANES + iota((8, LANES), 1)
    outer = jnp.zeros((32, LANES), f32)
    cd = jnp.zeros((1, LANES), f32)
    for g in range(2):
        factor = jnp.sum(jnp.where(index == where[0] + g * HALF, coulomb[...], 0.0), keepdims=True)
        own = jnp.where(lane // 32 == g, dens, 0.0)
        row = block_sum(own)
        column = jnp.sum(
            jnp.where(iota((32, LANES), 0) == iota((32, LANES), 1), row, 0.0), axis=1, keepdims=True
        )
        outer = outer + column * (factor * row)
        cd = cd + factor * own
    alpha = (gram[...] + (2.0 / NT) * outer - direct / NK) / NT
    wide[...] = keep_block(alpha, iota((32, LANES), 0) % 4)
    packed = wide[pl.ds(0, 8, stride=4), :]
    for c in range(1, 4):
        packed = packed + wide[pl.ds(c, 8, stride=4), :]
    tail = jnp.concatenate([packed, cd, jnp.zeros((1, LANES), f32)], axis=0)
    for r in range(ROWS - NBB):
        lines[pl.ds(NBB + r, NA, stride=ROWS), :] = jnp.broadcast_to(tail[r : r + 1], (NA, LANES))
    msg[...] = lines[0 : NA * ROWS, :].astype(bf16)


def relay_kernel(got, msg, lines):
    lines[...] = got[...].astype(f32)
    alpha = []
    for r in range(8):
        part = lines[pl.ds(NBB + r, NA, stride=ROWS), :]
        alpha.append(jnp.sum(part, axis=0, keepdims=True))
    alpha = jnp.concatenate(alpha, axis=0)
    hi = alpha.astype(bf16).astype(f32)
    cd = lines[pl.ds(NBB + 8, NA, stride=ROWS), :]
    cd = cd[0:16] + pltpu.roll(cd[16:32], 64, 1)
    tail = jnp.concatenate([cd, hi, alpha - hi], axis=0).astype(bf16)
    for b in range(NBB):
        msg[b, 0:32, :] = lines[pl.ds(b, NA, stride=ROWS), :].astype(bf16)
        msg[b, 32:64, :] = tail


def finish_kernel(got, pairs, pe, vec, energy, out, alpha_out, wide, rows):
    x = spread_vectors(vec, wide)
    potential = got[:, 0:32, :].reshape(ND, LANES)
    field = []
    for b in range(NBB):
        part = got[b, 32:48, :].astype(f32)
        field += [part, pltpu.roll(part, 64, 1)]
    field = jnp.concatenate(field, axis=0).astype(bf16)
    direct = jnp.dot(pairs[...], potential, preferred_element_type=f32)
    direct = block_sum(keep_block(direct, iota(direct.shape, 0) // 16))
    direct = jnp.concatenate([direct[0:16] + direct[16:32], direct[32:48] + direct[48:64]], axis=0)
    exchange = jnp.dot(exchange_rows(pe), field, preferred_element_type=f32)
    exchange = block_sum(keep_block(exchange, iota(exchange.shape, 0) // 32))
    exchange = exchange[0:32] + exchange[32:64]
    applied = energy_column(energy) * x + (2.0 / NT) * exchange - direct / NK
    alpha = jnp.zeros((16, LANES), f32)
    for b in range(NBB):
        alpha = alpha + got[b, 48:64, :].astype(f32)
    alpha = alpha[0:8] + alpha[8:16]
    for c in range(4):
        wide[pl.ds(c, 8, stride=4), :] = alpha
    full = wide[...]
    full = block_sum(keep_block(full, iota(full.shape, 0) % 4))
    alpha_out[...] = full[:, 0:32]
    shift = jnp.dot(x[:, 0:32], full, precision=HIGH, preferred_element_type=f32)
    rows[...] = keep_block(applied - shift, iota((32, LANES), 0) % 4)
    packed = rows[pl.ds(0, 8, stride=4), :]
    for c in range(1, 4):
        packed = packed + rows[pl.ds(c, 8, stride=4), :]
    for k in range(2):
        for v in range(4):
            out[k : k + 1, v * LANES : (v + 1) * LANES] = packed[k * 4 + v : k * 4 + v + 1, :]


def vmem():
    return pl.BlockSpec(memory_space=pltpu.VMEM)


def smem():
    return pl.BlockSpec(memory_space=pltpu.SMEM)


def room(mib):
    return pltpu.CompilerParams(vmem_limit_bytes=mib << 20)


def in_hbm(x):
    return pltpu.with_memory_space_constraint(jnp.asarray(x), pltpu.HBM)


def sds(shape, dtype):
    return jax.ShapeDtypeStruct(shape, dtype)


def on_device(pair_exchange, conduction, valence, coulomb, screening, energies, vectors, k_coords):
    mine = (lax.axis_index(B) * NA + lax.axis_index(A)).reshape(1).astype(jnp.int32)
    first, second = cas_tables()
    near = [
        in_hbm(v) for v in (k_coords, conduction, valence, pair_exchange, vectors, energies)
    ] + [in_hbm(v) for v in (first, second, coulomb.reshape(8, LANES))]
    any_space = pl.BlockSpec(memory_space=pl.ANY)
    fixed2 = lambda i, *w: (0, 0)
    fixed3 = lambda i, *w: (0, 0, 0)
    msg, pairs, gram, first, second, bare = pl.pallas_call(
        pack_kernel,
        out_shape=(
            sds((2 * ND, LANES), bf16),
            sds((64, HALF), bf16),
            sds((32, LANES), f32),
            sds((64, NK), bf16),
            sds((64, NK), bf16),
            sds((8, LANES), f32),
        ),
        grid_spec=pltpu.PrefetchScalarGridSpec(
            num_scalar_prefetch=1,
            grid=(1,),
            in_specs=[
                pl.BlockSpec(k_coords.shape, fixed2),
                pl.BlockSpec(conduction.shape, fixed3),
                pl.BlockSpec(valence.shape, fixed3),
                pl.BlockSpec(pair_exchange.shape, fixed3),
                pl.BlockSpec(vectors.shape, fixed2),
                pl.BlockSpec(energies.shape, fixed2),
                any_space,
                any_space,
                any_space,
            ],
            out_specs=[
                pl.BlockSpec((2 * ND, LANES), fixed2),
                pl.BlockSpec((64, HALF), fixed2),
                pl.BlockSpec((32, LANES), fixed2),
                pl.BlockSpec((64, NK), fixed2),
                pl.BlockSpec((64, NK), fixed2),
                pl.BlockSpec((8, LANES), fixed2),
            ],
            scratch_shapes=[
                pltpu.VMEM((32, LANES), f32),
                pltpu.VMEM((64, HALF), f32),
                pltpu.VMEM((2 * ND, LANES), f32),
                pltpu.SemaphoreType.DMA((3,)),
            ],
        ),
        compiler_params=room(12),
        name="pack",
    )(mine, *near)
    got = lax.all_to_all(msg.reshape(ND, 2, LANES), B + A, 0, 0, tiled=True)
    out = pl.pallas_call(
        spectral_kernel,
        out_shape=sds((NA * ROWS, LANES), bf16),
        in_specs=[smem()] + [vmem()] * 5 + [any_space] * 2,
        out_specs=vmem(),
        scratch_shapes=[
            pltpu.VMEM((2 * ND, LANES), f32),
            pltpu.VMEM((32, LANES), f32),
            pltpu.VMEM((2, NQ, LANES), f32),
            pltpu.VMEM((NQ, NK), f32),
            pltpu.SemaphoreType.DMA((3,)),
        ],
        compiler_params=room(28),
        name="spectral",
    )(
        mine,
        got.reshape(2 * ND, LANES),
        gram,
        bare,
        first,
        second,
        in_hbm(screening),
        in_hbm(cos_table()),
    )
    got = lax.all_to_all(out.reshape(NA, ROWS // 2, 2, LANES), A, 0, 0, tiled=True)
    out = pl.pallas_call(
        relay_kernel,
        out_shape=sds((NBB, 64, LANES), bf16),
        in_specs=[vmem()],
        out_specs=vmem(),
        scratch_shapes=[pltpu.VMEM((NA * ROWS, LANES), f32)],
        compiler_params=room(8),
        name="relay",
    )(got.reshape(NA * ROWS, LANES))
    got = lax.all_to_all(out, B, 0, 0, tiled=True)
    return pl.pallas_call(
        finish_kernel,
        out_shape=(sds((2, NB * NV), f32), sds((NV, NV), f32)),
        in_specs=[vmem()] * 5,
        out_specs=(vmem(), vmem()),
        scratch_shapes=[pltpu.VMEM((32, LANES), f32), pltpu.VMEM((32, LANES), f32)],
        compiler_params=room(8),
        name="finish",
    )(got, pairs, pair_exchange, vectors, energies)


def solution(mesh):
    split = Mesh(mesh.devices.reshape(SIZES), NAMES)
    return jax.shard_map(
        on_device,
        mesh=split,
        in_specs=(
            P(NAMES, None, None),
            P(NAMES, None, None),
            P(NAMES, None, None),
            P(),
            P(),
            P(NAMES, None),
            P(NAMES, None),
            P(NAMES, None),
        ),
        out_specs=(P(NAMES, None), P()),
        check_vma=False,
    )
```

```python
import jax
import jax.numpy as jnp
import numpy as np
from jax import lax
from jax.experimental import pallas as pl
from jax.experimental.pallas import tpu as pltpu
from jax.sharding import Mesh
from jax.sharding import PartitionSpec as P

MX = 32
MY = 32
NK = 1024
NB = 16
NG = 1024
NV = 32
NT = NK * NB
NQ = 289
NAMES = ("zh", "zl", "yl", "c", "x", "yh")
SIZES = (4, 2, 2, 2, 4, 4)
A = ("zh", "zl", "yh", "yl")
B = ("x", "c")
NA = 64
NBB = 8
ND = NA * NBB
HALF = NG // 2
ROWS = NBB + 10
FIELD = NA + NA // 2
WIDE = FIELD + 16
LANES = 128

f32 = jnp.float32
bf16 = jnp.bfloat16
HIGH = lax.Precision.HIGHEST


def split_table(x):
    hi = x.astype(bf16)
    lo = (x - hi.astype(np.float64)).astype(bf16)
    return np.concatenate([hi, lo], axis=0)


def cas_tables():
    m = np.arange(32)
    phase = 2.0 * np.pi * ((m[:, None] * m[None, :]) % 32) / 32.0
    cas = np.cos(phase) + np.sin(phase)
    first = np.repeat(cas, 32, axis=1)
    second = np.tile(cas, (1, 32)) / 32.0
    return split_table(first), split_table(second)


def cos_table():
    f = np.arange(17)
    m = np.arange(32)
    weight = np.where((f == 0) | (f == 16), 1.0, 2.0)
    c = weight[:, None] * np.cos(2.0 * np.pi * ((f[:, None] * m[None, :]) % 32) / 32.0)
    return np.einsum("im,jn->ijmn", c, c).reshape(NQ, NK).astype(np.float32)


def iota(shape, axis):
    return lax.broadcasted_iota(jnp.int32, shape, axis)


def block_sum(x):
    x = x + pltpu.roll(x, 32, 1)
    return x + pltpu.roll(x, 64, 1)


def keep_block(x, wanted):
    return jnp.where(iota(x.shape, 1) // 32 == wanted, x, 0.0)


def spread_vectors(vec_ref, wide):
    rows = [
        vec_ref[k : k + 1, v * LANES : (v + 1) * LANES].astype(f32)
        for k in range(2)
        for v in range(4)
    ]
    x8 = jnp.concatenate(rows, axis=0)
    for c in range(4):
        wide[pl.ds(c, 8, stride=4), :] = x8
    x = wide[...]
    return block_sum(keep_block(x, iota(x.shape, 0) % 4))


def energy_column(energy_ref):
    first = jnp.broadcast_to(energy_ref[0:1, :], (NB, NB))
    second = jnp.broadcast_to(energy_ref[1:2, :], (NB, NB))
    e = jnp.concatenate([first, second], axis=0)
    return jnp.sum(
        jnp.where(iota(e.shape, 1) == iota(e.shape, 0) % NB, e, 0.0), axis=1, keepdims=True
    )


def exchange_rows(pe_ref):
    return jnp.concatenate(
        [pe_ref[k, :, g * HALF : (g + 1) * HALF] for g in range(2) for k in range(2)], axis=0
    )


def dot_t(x, y):
    return lax.dot_general(x, y, (((0,), (0,)), ((), ())), preferred_element_type=f32)


def dot_nt(x, y):
    return lax.dot_general(x, y, (((1,), (1,)), ((), ())), preferred_element_type=f32)


def pack_kernel(
    mine, coords, cond, val, pe, vec, energy, *refs
):
    del mine
    far, (msg, pairs, gram), near, (wide, rows, lines, sem) = refs[:3], refs[3:6], refs[6:9], refs[9:]
    copies = [pltpu.make_async_copy(far[i], near[i], sem.at[i]) for i in range(3)]
    for copy in copies:
        copy.start()
    x = spread_vectors(vec, wide)
    for k in range(2):
        cf = cond[k].astype(f32)
        vf = val[k].astype(f32)
        for v in range(4):
            both = vf[v : v + 1, :] * cf
            for g in range(2):
                at = k * 32 + g * 16 + v * 4
                rows[at : at + 4, :] = both[:, g * HALF : (g + 1) * HALF]
    left = rows[...].astype(bf16)
    pairs[...] = left
    xp = jnp.concatenate([x[0:16], x[0:16], x[16:32], x[16:32]], axis=0)
    xp = keep_block(xp, iota(xp.shape, 0) // 16).astype(bf16)
    xd = jnp.concatenate([x, x], axis=0)
    xd = keep_block(xd, iota(xd.shape, 0) // 32).astype(bf16)
    lane = iota((1, LANES), 1)
    place = jnp.zeros((1, LANES), f32)
    for k in range(2):
        for s in range(2):
            place = jnp.where(lane == 64 + 2 * k + s, coords[k : k + 1, s : s + 1].astype(f32), place)
    lines[pl.ds(0, ND, stride=2), :] = dot_t(left, xp)
    lines[pl.ds(1, ND, stride=2), :] = dot_t(exchange_rows(pe), xd) + place
    msg[...] = lines[...].astype(bf16)
    gram[...] = lax.dot_general(
        x[:, 0:32],
        energy_column(energy) * x,
        (((0,), (0,)), ((), ())),
        precision=HIGH,
        preferred_element_type=f32,
    )
    for copy in copies:
        copy.wait()


def spectrum(mine, tiles, cos):
    own = iota((NQ, LANES), 1) == mine % LANES
    out = []
    for g in range(2):
        column = jnp.sum(jnp.where(own, tiles[g], 0.0), axis=1, keepdims=True)
        line = jnp.sum(column * cos[...], axis=0, keepdims=True)
        out.append(jnp.broadcast_to(line, (32, NK)))
    return jnp.concatenate(out, axis=0)


def spectral_kernel(
    where, got, gram, coulomb, first, second, table, far, msg, lines, wide, tiles, cos, sem
):
    tile = pl.multiple_of((where[0] // LANES) * LANES, LANES)
    copies = [
        pltpu.make_async_copy(table.at[:, pl.ds(tile + g * HALF, LANES)], tiles.at[g], sem.at[g])
        for g in range(2)
    ]
    copies.append(pltpu.make_async_copy(far, cos, sem.at[2]))
    for copy in copies:
        copy.start()
    lines[0 : 2 * ND, :] = got[...].astype(f32)
    proj = lines[pl.ds(0, ND, stride=2), :].astype(bf16)
    rest = lines[pl.ds(1, ND, stride=2), :]
    basis = []
    hat = None
    slot = iota((ND, 64), 1) % 32
    for k in range(2):
        at = [rest[:, 64 + 2 * k + s : 65 + 2 * k + s].astype(jnp.int32) for s in range(2)]
        ones = [jnp.where(slot == p, 1.0, 0.0).astype(bf16) for p in at]
        ta = jnp.dot(ones[0], first[...], preferred_element_type=f32)
        tb = jnp.dot(ones[1], second[...], preferred_element_type=f32)
        exact = ta * tb
        hi = exact.astype(bf16)
        lo = (exact - hi.astype(f32)).astype(bf16)
        basis.append((hi, lo))
        part = (dot_t(proj, hi) + dot_t(proj, lo))[k * 64 : (k + 1) * 64]
        hat = part if hat is None else hat + part
    for copy in copies:
        copy.wait()
    scale = spectrum(where[0], tiles, cos)
    exact = hat * scale
    scaled = exact.astype(bf16)
    finer = (exact - scaled.astype(f32)).astype(bf16)
    hat = hat.astype(bf16)
    both = jnp.concatenate([scaled, finer], axis=0)
    side = iota((ND, LANES), 1) // 64
    back = []
    for hi, lo in basis:
        r = dot_nt(hi, both)
        back.append(r + pltpu.roll(r, 64, 1) + dot_nt(lo, jnp.concatenate([scaled] * 2, axis=0)))
    back = jnp.where(side == 0, back[0], back[1])
    for b in range(NBB):
        lines[pl.ds(b, NA, stride=ROWS), :] = back[b * NA : (b + 1) * NA]
    direct = dot_nt(hat[0:32], jnp.concatenate([scaled[0:32]] * 4, axis=0)) + dot_nt(
        hat[32:64], jnp.concatenate([scaled[32:64]] * 4, axis=0)
    )
    lane = iota((1, LANES), 1)
    dens = jnp.sum(rest, axis=0, keepdims=True)
    index = iota((8, LANES), 0) * LANES + iota((8, LANES), 1)
    outer = jnp.zeros((32, LANES), f32)
    cd = jnp.zeros((1, LANES), f32)
    for g in range(2):
        factor = jnp.sum(jnp.where(index == where[0] + g * HALF, coulomb[...], 0.0), keepdims=True)
        own = jnp.where(lane // 32 == g, dens, 0.0)
        row = block_sum(own)
        column = jnp.sum(
            jnp.where(iota((32, LANES), 0) == iota((32, LANES), 1), row, 0.0), axis=1, keepdims=True
        )
        outer = outer + column * (factor * row)
        cd = cd + factor * own
    alpha = (gram[...] + (2.0 / NT) * outer - direct / NK) / NT
    wide[...] = keep_block(alpha, iota((32, LANES), 0) % 4)
    packed = wide[pl.ds(0, 8, stride=4), :]
    for c in range(1, 4):
        packed = packed + wide[pl.ds(c, 8, stride=4), :]
    tail = jnp.concatenate([packed, cd, jnp.zeros((1, LANES), f32)], axis=0)
    for r in range(ROWS - NBB):
        lines[pl.ds(NBB + r, NA, stride=ROWS), :] = jnp.broadcast_to(tail[r : r + 1], (NA, LANES))
    msg[...] = lines[0 : NA * ROWS, :].astype(bf16)


def relay_kernel(got, msg, lines):
    lines[...] = got[...].astype(f32)
    alpha = []
    for r in range(8):
        part = lines[pl.ds(NBB + r, NA, stride=ROWS), :]
        alpha.append(jnp.sum(part, axis=0, keepdims=True))
    alpha = jnp.concatenate(alpha, axis=0)
    hi = alpha.astype(bf16).astype(f32)
    cd = lines[pl.ds(NBB + 8, NA, stride=ROWS), :]
    cd = cd[0 : NA // 2] + pltpu.roll(cd[NA // 2 :], 64, 1)
    tail = jnp.concatenate([cd, hi, alpha - hi], axis=0).astype(bf16)
    for b in range(NBB):
        msg[b, 0:NA, :] = lines[pl.ds(b, NA, stride=ROWS), :].astype(bf16)
        msg[b, NA:WIDE, :] = tail


def finish_kernel(got, pairs, pe, vec, energy, out, alpha_out, wide, rows):
    x = spread_vectors(vec, wide)
    potential = got[:, 0:NA, :].reshape(ND, LANES)
    field = []
    for b in range(NBB):
        part = got[b, NA:FIELD, :].astype(f32)
        field += [part, pltpu.roll(part, 64, 1)]
    field = jnp.concatenate(field, axis=0).astype(bf16)
    direct = jnp.dot(pairs[...], potential, preferred_element_type=f32)
    direct = block_sum(keep_block(direct, iota(direct.shape, 0) // 16))
    direct = jnp.concatenate([direct[0:16] + direct[16:32], direct[32:48] + direct[48:64]], axis=0)
    exchange = jnp.dot(exchange_rows(pe), field, preferred_element_type=f32)
    exchange = block_sum(keep_block(exchange, iota(exchange.shape, 0) // 32))
    exchange = exchange[0:32] + exchange[32:64]
    applied = energy_column(energy) * x + (2.0 / NT) * exchange - direct / NK
    alpha = jnp.zeros((16, LANES), f32)
    for b in range(NBB):
        alpha = alpha + got[b, FIELD:WIDE, :].astype(f32)
    alpha = alpha[0:8] + alpha[8:16]
    for c in range(4):
        wide[pl.ds(c, 8, stride=4), :] = alpha
    full = wide[...]
    full = block_sum(keep_block(full, iota(full.shape, 0) % 4))
    alpha_out[...] = full[:, 0:32]
    shift = jnp.dot(x[:, 0:32], full, precision=HIGH, preferred_element_type=f32)
    rows[...] = keep_block(applied - shift, iota((32, LANES), 0) % 4)
    packed = rows[pl.ds(0, 8, stride=4), :]
    for c in range(1, 4):
        packed = packed + rows[pl.ds(c, 8, stride=4), :]
    for k in range(2):
        for v in range(4):
            out[k : k + 1, v * LANES : (v + 1) * LANES] = packed[k * 4 + v : k * 4 + v + 1, :]


def vmem():
    return pl.BlockSpec(memory_space=pltpu.VMEM)


def smem():
    return pl.BlockSpec(memory_space=pltpu.SMEM)


def room(mib):
    return pltpu.CompilerParams(vmem_limit_bytes=mib << 20)


def in_hbm(x):
    return pltpu.with_memory_space_constraint(jnp.asarray(x), pltpu.HBM)


def sds(shape, dtype):
    return jax.ShapeDtypeStruct(shape, dtype)


def on_device(pair_exchange, conduction, valence, coulomb, screening, energies, vectors, k_coords):
    mine = (lax.axis_index(B) * NA + lax.axis_index(A)).reshape(1).astype(jnp.int32)
    first, second = cas_tables()
    near = [
        in_hbm(v) for v in (k_coords, conduction, valence, pair_exchange, vectors, energies)
    ] + [in_hbm(v) for v in (first, second, coulomb.reshape(8, LANES))]
    any_space = pl.BlockSpec(memory_space=pl.ANY)
    fixed2 = lambda i, *w: (0, 0)
    fixed3 = lambda i, *w: (0, 0, 0)
    msg, pairs, gram, first, second, bare = pl.pallas_call(
        pack_kernel,
        out_shape=(
            sds((2 * ND, LANES), bf16),
            sds((64, HALF), bf16),
            sds((32, LANES), f32),
            sds((64, NK), bf16),
            sds((64, NK), bf16),
            sds((8, LANES), f32),
        ),
        grid_spec=pltpu.PrefetchScalarGridSpec(
            num_scalar_prefetch=1,
            grid=(1,),
            in_specs=[
                pl.BlockSpec(k_coords.shape, fixed2),
                pl.BlockSpec(conduction.shape, fixed3),
                pl.BlockSpec(valence.shape, fixed3),
                pl.BlockSpec(pair_exchange.shape, fixed3),
                pl.BlockSpec(vectors.shape, fixed2),
                pl.BlockSpec(energies.shape, fixed2),
                any_space,
                any_space,
                any_space,
            ],
            out_specs=[
                pl.BlockSpec((2 * ND, LANES), fixed2),
                pl.BlockSpec((64, HALF), fixed2),
                pl.BlockSpec((32, LANES), fixed2),
                pl.BlockSpec((64, NK), fixed2),
                pl.BlockSpec((64, NK), fixed2),
                pl.BlockSpec((8, LANES), fixed2),
            ],
            scratch_shapes=[
                pltpu.VMEM((32, LANES), f32),
                pltpu.VMEM((64, HALF), f32),
                pltpu.VMEM((2 * ND, LANES), f32),
                pltpu.SemaphoreType.DMA((3,)),
            ],
        ),
        compiler_params=room(12),
        name="pack",
    )(mine, *near)
    got = lax.all_to_all(msg.reshape(ND, 2, LANES), B + A, 0, 0, tiled=True)
    out = pl.pallas_call(
        spectral_kernel,
        out_shape=sds((NA * ROWS, LANES), bf16),
        in_specs=[smem()] + [vmem()] * 5 + [any_space] * 2,
        out_specs=vmem(),
        scratch_shapes=[
            pltpu.VMEM((max(2 * ND, NA * ROWS), LANES), f32),
            pltpu.VMEM((32, LANES), f32),
            pltpu.VMEM((2, NQ, LANES), f32),
            pltpu.VMEM((NQ, NK), f32),
            pltpu.SemaphoreType.DMA((3,)),
        ],
        compiler_params=room(28),
        name="spectral",
    )(
        mine,
        got.reshape(2 * ND, LANES),
        gram,
        bare,
        first,
        second,
        in_hbm(screening),
        in_hbm(cos_table()),
    )
    got = lax.all_to_all(out.reshape(NA, ROWS // 2, 2, LANES), A, 0, 0, tiled=True)
    out = pl.pallas_call(
        relay_kernel,
        out_shape=sds((NBB, WIDE, LANES), bf16),
        in_specs=[vmem()],
        out_specs=vmem(),
        scratch_shapes=[pltpu.VMEM((NA * ROWS, LANES), f32)],
        compiler_params=room(8),
        name="relay",
    )(got.reshape(NA * ROWS, LANES))
    got = lax.all_to_all(out, B, 0, 0, tiled=True)
    return pl.pallas_call(
        finish_kernel,
        out_shape=(sds((2, NB * NV), f32), sds((NV, NV), f32)),
        in_specs=[vmem()] * 5,
        out_specs=(vmem(), vmem()),
        scratch_shapes=[pltpu.VMEM((32, LANES), f32), pltpu.VMEM((32, LANES), f32)],
        compiler_params=room(8),
        name="finish",
    )(got, pairs, pair_exchange, vectors, energies)


def solution(mesh):
    split = Mesh(mesh.devices.reshape(SIZES), NAMES)
    return jax.shard_map(
        on_device,
        mesh=split,
        in_specs=(
            P(NAMES, None, None),
            P(NAMES, None, None),
            P(NAMES, None, None),
            P(),
            P(),
            P(NAMES, None),
            P(NAMES, None),
            P(NAMES, None),
        ),
        out_specs=(P(NAMES, None), P()),
        check_vma=False,
    )
```

```python
import jax
import jax.numpy as jnp
import numpy as np
from jax import lax
from jax.experimental import pallas as pl
from jax.experimental.pallas import tpu as pltpu
from jax.sharding import Mesh
from jax.sharding import PartitionSpec as P

MX = 32
MY = 32
NK = 1024
NB = 16
NG = 1024
NV = 32
NT = NK * NB
NQ = 289
CHUNK = 256
NAMES = ("zh", "zl", "yl", "c", "x", "yh")
SIZES = (4, 2, 2, 2, 4, 4)
A = ("zh", "zl", "yh")
B = ("x", "yl", "c")
NA = 32
NBB = 16
ND = NA * NBB
HALF = NG // 2
ROWS = NBB + 10
FIELD = NA + NA // 2
WIDE = FIELD + 16
LANES = 128

f32 = jnp.float32
bf16 = jnp.bfloat16
HIGH = lax.Precision.HIGHEST


def split_table(x):
    hi = x.astype(bf16)
    lo = (x - hi.astype(np.float64)).astype(bf16)
    return np.concatenate([hi, lo], axis=0)


def tables():
    m = np.arange(32)
    phase = 2.0 * np.pi * ((m[:, None] * m[None, :]) % 32) / 32.0
    cas = np.cos(phase) + np.sin(phase)
    first = split_table(np.repeat(cas, 32, axis=1))
    second = split_table(np.tile(cas, (1, 4)) / 32.0)
    f = np.arange(17)
    weight = np.where((f == 0) | (f == 16), 1.0, 2.0)
    cos = weight[:, None] * np.cos(2.0 * np.pi * ((f[:, None] * m[None, :]) % 32) / 32.0)
    outer = np.zeros((24, NK), np.float32)
    outer[0:17] = np.repeat(cos, 32, axis=1)
    inner = np.tile(cos, (17, 4)).astype(np.float32)
    return first, second, outer, inner


def iota(shape, axis):
    return lax.broadcasted_iota(jnp.int32, shape, axis)


def block_sum(x):
    x = x + pltpu.roll(x, 32, 1)
    return x + pltpu.roll(x, 64, 1)


def keep_block(x, wanted):
    return jnp.where(iota(x.shape, 1) // 32 == wanted, x, 0.0)


def spread_vectors(vec_ref, wide):
    rows = [
        vec_ref[k : k + 1, v * LANES : (v + 1) * LANES].astype(f32)
        for k in range(2)
        for v in range(4)
    ]
    x8 = jnp.concatenate(rows, axis=0)
    for c in range(4):
        wide[pl.ds(c, 8, stride=4), :] = x8
    x = wide[...]
    return block_sum(keep_block(x, iota(x.shape, 0) % 4))


def energy_column(energy_ref):
    first = jnp.broadcast_to(energy_ref[0:1, :], (NB, NB))
    second = jnp.broadcast_to(energy_ref[1:2, :], (NB, NB))
    e = jnp.concatenate([first, second], axis=0)
    return jnp.sum(
        jnp.where(iota(e.shape, 1) == iota(e.shape, 0) % NB, e, 0.0), axis=1, keepdims=True
    )


def exchange_rows(pe_ref):
    return jnp.concatenate(
        [pe_ref[k, :, g * HALF : (g + 1) * HALF] for g in range(2) for k in range(2)], axis=0
    )


def dot_t(x, y):
    return lax.dot_general(x, y, (((0,), (0,)), ((), ())), preferred_element_type=f32)


def dot_nt(x, y):
    return lax.dot_general(x, y, (((1,), (1,)), ((), ())), preferred_element_type=f32)


def spectrum(lane_at, tiles, outer, inner):
    own = iota((NQ, LANES), 1) == lane_at
    pick = jnp.where(iota((24, NQ), 0) == iota((24, NQ), 1) // 17, 1.0, 0.0)
    out = []
    for g in range(2):
        column = jnp.sum(jnp.where(own, tiles[g], 0.0), axis=1, keepdims=True)
        part = jnp.dot(pick, column * inner[...], precision=HIGH, preferred_element_type=f32)
        line = [
            jnp.sum(outer[:, j * LANES : (j + 1) * LANES] * part, axis=0, keepdims=True)
            for j in range(NK // LANES)
        ]
        out.append(jnp.concatenate(line, axis=1))
    return out


def pack_kernel(*refs):
    far, (msg, pairs, gram, lam, first, second) = refs[:12], refs[12:18]
    coords, cond, val, vec, pe, energy, tiles, bare, outer, inner, wide, rows, lines, sem = refs[18:]
    mine = lax.axis_index(B) * NA + lax.axis_index(A)
    tile = pl.multiple_of((mine // LANES) * LANES, LANES)
    near = (coords, cond, val, vec, pe, energy, inner, outer, bare, first, second)
    pairs_of = list(zip(far[:6] + far[7:], near))
    pairs_of += [(far[6].at[:, pl.ds(tile + g * HALF, LANES)], tiles.at[g]) for g in range(2)]
    copies = [
        pltpu.make_async_copy(src, dst, sem.at[i]) for i, (src, dst) in enumerate(pairs_of)
    ]
    for copy in copies:
        copy.start()
    for copy in copies[:6]:
        copy.wait()
    x = spread_vectors(vec, wide)
    for k in range(2):
        cf = cond[k].astype(f32)
        vf = val[k].astype(f32)
        for v in range(4):
            both = vf[v : v + 1, :] * cf
            for g in range(2):
                at = k * 32 + g * 16 + v * 4
                rows[at : at + 4, :] = both[:, g * HALF : (g + 1) * HALF]
    left = rows[...].astype(bf16)
    pairs[...] = left
    xp = jnp.concatenate([x[0:16], x[0:16], x[16:32], x[16:32]], axis=0)
    xp = keep_block(xp, iota(xp.shape, 0) // 16).astype(bf16)
    xd = jnp.concatenate([x, x], axis=0)
    xd = keep_block(xd, iota(xd.shape, 0) // 32).astype(bf16)
    lane = iota((1, LANES), 1)
    place = jnp.zeros((1, LANES), f32)
    for k in range(2):
        for s in range(2):
            place = jnp.where(lane == 64 + 2 * k + s, coords[k : k + 1, s : s + 1].astype(f32), place)
    lines[pl.ds(0, ND, stride=2), :] = dot_t(left, xp)
    lines[pl.ds(1, ND, stride=2), :] = dot_t(exchange_rows(pe), xd) + place
    msg[...] = lines[...].astype(bf16)
    gram[...] = lax.dot_general(
        x[:, 0:32],
        energy_column(energy) * x,
        (((0,), (0,)), ((), ())),
        precision=HIGH,
        preferred_element_type=f32,
    )
    for copy in copies[6:]:
        copy.wait()
    index = iota((8, LANES), 0) * LANES + iota((8, LANES), 1)
    lines_of = spectrum(mine - tile, tiles, outer, inner)
    for g in range(2):
        factor = jnp.sum(jnp.where(index == mine + g * HALF, bare[...], 0.0), keepdims=True)
        lines_of.append(jnp.broadcast_to(factor, (1, NK)))
    lam[...] = jnp.concatenate(lines_of + [jnp.zeros((4, NK), f32)], axis=0)


def spectral_kernel(got, gram, lam, first, second, msg, lines, wide):
    lines[0 : 2 * ND, :] = got[...].astype(f32)
    proj = jnp.transpose(lines[pl.ds(0, ND, stride=2), :]).astype(bf16)
    rest = lines[pl.ds(1, ND, stride=2), :]
    slot = iota((ND, 64), 1) % 32
    at_first, from_second = [], []
    for k in range(2):
        at = [rest[:, 64 + 2 * k + s : 65 + 2 * k + s].astype(jnp.int32) for s in range(2)]
        ones = [jnp.where(slot == p, 1.0, 0.0).astype(bf16) for p in at]
        at_first.append(ones[0])
        tb = jnp.dot(ones[1], second[...], preferred_element_type=f32)
        from_second.append(jnp.concatenate([tb] * (CHUNK // LANES), axis=1))
    back = [None, None]
    direct = None
    for m in range(0, NK, CHUNK):
        hat = None
        basis = []
        for k in range(2):
            ta = jnp.dot(at_first[k], first[:, m : m + CHUNK], preferred_element_type=f32)
            exact = ta * from_second[k]
            hi = exact.astype(bf16)
            lo = (exact - hi.astype(f32)).astype(bf16)
            basis.append((hi, lo))
            mine = proj[k * 64 : (k + 1) * 64]
            part = jnp.dot(mine, hi, preferred_element_type=f32) + jnp.dot(
                mine, lo, preferred_element_type=f32
            )
            hat = part if hat is None else hat + part
        scale = jnp.concatenate(
            [jnp.broadcast_to(lam[g : g + 1, m : m + CHUNK], (32, CHUNK)) for g in range(2)], axis=0
        )
        exact = hat * scale
        scaled = exact.astype(bf16)
        finer = (exact - scaled.astype(f32)).astype(bf16)
        hat = hat.astype(bf16)
        both = jnp.concatenate([scaled, finer], axis=0)
        again = jnp.concatenate([scaled, jnp.zeros((64, CHUNK), bf16)], axis=0)
        for k in range(2):
            part = dot_nt(basis[k][0], both) + dot_nt(basis[k][1], again)
            back[k] = part if back[k] is None else back[k] + part
        part = dot_nt(hat[0:32], jnp.concatenate([scaled[0:32]] * 4, axis=0)) + dot_nt(
            hat[32:64], jnp.concatenate([scaled[32:64]] * 4, axis=0)
        )
        direct = part if direct is None else direct + part
    back = [r + pltpu.roll(r, 64, 1) for r in back]
    back = jnp.where(iota((ND, LANES), 1) < 64, back[0], back[1])
    for b in range(NBB):
        lines[pl.ds(b, NA, stride=ROWS), :] = back[b * NA : (b + 1) * NA]
    lane = iota((1, LANES), 1)
    dens = jnp.sum(rest, axis=0, keepdims=True)
    outer = jnp.zeros((32, LANES), f32)
    cd = jnp.zeros((1, LANES), f32)
    for g in range(2):
        factor = lam[2 + g : 3 + g, 0:LANES]
        own = jnp.where(lane // 32 == g, dens, 0.0)
        row = block_sum(own)
        column = jnp.sum(
            jnp.where(iota((32, LANES), 0) == iota((32, LANES), 1), row, 0.0), axis=1, keepdims=True
        )
        outer = outer + column * (factor * row)
        cd = cd + factor * own
    alpha = (gram[...] + (2.0 / NT) * outer - direct / NK) / NT
    wide[...] = keep_block(alpha, iota((32, LANES), 0) % 4)
    packed = wide[pl.ds(0, 8, stride=4), :]
    for c in range(1, 4):
        packed = packed + wide[pl.ds(c, 8, stride=4), :]
    tail = jnp.concatenate([packed, cd, jnp.zeros((1, LANES), f32)], axis=0)
    for r in range(ROWS - NBB):
        lines[pl.ds(NBB + r, NA, stride=ROWS), :] = jnp.broadcast_to(tail[r : r + 1], (NA, LANES))
    msg[...] = lines[0 : NA * ROWS, :].astype(bf16)


def relay_kernel(got, msg, lines):
    lines[...] = got[...].astype(f32)
    alpha = []
    for r in range(8):
        part = lines[pl.ds(NBB + r, NA, stride=ROWS), :]
        alpha.append(jnp.sum(part, axis=0, keepdims=True))
    alpha = jnp.concatenate(alpha, axis=0)
    hi = alpha.astype(bf16).astype(f32)
    cd = lines[pl.ds(NBB + 8, NA, stride=ROWS), :]
    cd = cd[0 : NA // 2] + pltpu.roll(cd[NA // 2 :], 64, 1)
    tail = jnp.concatenate([cd, hi, alpha - hi], axis=0).astype(bf16)
    for b in range(NBB):
        msg[b, 0:NA, :] = lines[pl.ds(b, NA, stride=ROWS), :].astype(bf16)
        msg[b, NA:WIDE, :] = tail


def finish_kernel(got, pairs, pe, vec, energy, out, alpha_out, wide, rows):
    x = spread_vectors(vec, wide)
    potential = got[:, 0:NA, :].reshape(ND, LANES)
    field = []
    for b in range(NBB):
        part = got[b, NA:FIELD, :].astype(f32)
        field += [part, pltpu.roll(part, 64, 1)]
    field = jnp.concatenate(field, axis=0).astype(bf16)
    direct = jnp.dot(pairs[...], potential, preferred_element_type=f32)
    direct = block_sum(keep_block(direct, iota(direct.shape, 0) // 16))
    direct = jnp.concatenate([direct[0:16] + direct[16:32], direct[32:48] + direct[48:64]], axis=0)
    exchange = jnp.dot(exchange_rows(pe), field, preferred_element_type=f32)
    exchange = block_sum(keep_block(exchange, iota(exchange.shape, 0) // 32))
    exchange = exchange[0:32] + exchange[32:64]
    applied = energy_column(energy) * x + (2.0 / NT) * exchange - direct / NK
    alpha = jnp.zeros((16, LANES), f32)
    for b in range(NBB):
        alpha = alpha + got[b, FIELD:WIDE, :].astype(f32)
    alpha = alpha[0:8] + alpha[8:16]
    for c in range(4):
        wide[pl.ds(c, 8, stride=4), :] = alpha
    full = wide[...]
    full = block_sum(keep_block(full, iota(full.shape, 0) % 4))
    alpha_out[...] = full[:, 0:32]
    shift = jnp.dot(x[:, 0:32], full, precision=HIGH, preferred_element_type=f32)
    rows[...] = keep_block(applied - shift, iota((32, LANES), 0) % 4)
    packed = rows[pl.ds(0, 8, stride=4), :]
    for c in range(1, 4):
        packed = packed + rows[pl.ds(c, 8, stride=4), :]
    for k in range(2):
        for v in range(4):
            out[k : k + 1, v * LANES : (v + 1) * LANES] = packed[k * 4 + v : k * 4 + v + 1, :]


def vmem():
    return pl.BlockSpec(memory_space=pltpu.VMEM)


def room(mib):
    return pltpu.CompilerParams(vmem_limit_bytes=mib << 20)


def in_hbm(x):
    return pltpu.with_memory_space_constraint(jnp.asarray(x), pltpu.HBM)


def sds(shape, dtype):
    return jax.ShapeDtypeStruct(shape, dtype)


def on_device(pair_exchange, conduction, valence, coulomb, screening, energies, vectors, k_coords):
    first, second, outer, inner = tables()
    far = (k_coords, conduction, valence, vectors, pair_exchange, energies, screening)
    far += (inner, outer, coulomb.reshape(8, LANES), first, second)
    any_space = pl.BlockSpec(memory_space=pl.ANY)
    own = [pltpu.VMEM(v.shape, v.dtype) for v in far[:6]]
    msg, pairs, gram, lam, first, second = pl.pallas_call(
        pack_kernel,
        out_shape=(
            sds((2 * ND, LANES), bf16),
            sds((64, HALF), bf16),
            sds((32, LANES), f32),
            sds((8, NK), f32),
            sds((64, NK), bf16),
            sds((64, LANES), bf16),
        ),
        in_specs=[any_space] * len(far),
        out_specs=(vmem(),) * 6,
        scratch_shapes=own
        + [
            pltpu.VMEM((2, NQ, LANES), f32),
            pltpu.VMEM((8, LANES), f32),
            pltpu.VMEM((24, NK), f32),
            pltpu.VMEM((NQ, LANES), f32),
            pltpu.VMEM((32, LANES), f32),
            pltpu.VMEM((64, HALF), f32),
            pltpu.VMEM((2 * ND, LANES), f32),
            pltpu.SemaphoreType.DMA((13,)),
        ],
        compiler_params=room(12),
        name="pack",
    )(*[in_hbm(v) for v in far])
    got = lax.all_to_all(msg.reshape(ND, 2, LANES), B + A, 0, 0, tiled=True)
    out = pl.pallas_call(
        spectral_kernel,
        out_shape=sds((NA * ROWS, LANES), bf16),
        in_specs=[vmem()] * 5,
        out_specs=vmem(),
        scratch_shapes=[
            pltpu.VMEM((max(2 * ND, NA * ROWS), LANES), f32),
            pltpu.VMEM((32, LANES), f32),
        ],
        compiler_params=room(28),
        name="spectral",
    )(got.reshape(2 * ND, LANES), gram, lam, first, second)
    got = lax.all_to_all(out.reshape(NA, ROWS // 2, 2, LANES), A, 0, 0, tiled=True)
    out = pl.pallas_call(
        relay_kernel,
        out_shape=sds((NBB, WIDE, LANES), bf16),
        in_specs=[vmem()],
        out_specs=vmem(),
        scratch_shapes=[pltpu.VMEM((NA * ROWS, LANES), f32)],
        compiler_params=room(8),
        name="relay",
    )(got.reshape(NA * ROWS, LANES))
    got = lax.all_to_all(out, B, 0, 0, tiled=True)
    return pl.pallas_call(
        finish_kernel,
        out_shape=(sds((2, NB * NV), f32), sds((NV, NV), f32)),
        in_specs=[vmem()] * 5,
        out_specs=(vmem(), vmem()),
        scratch_shapes=[pltpu.VMEM((32, LANES), f32), pltpu.VMEM((32, LANES), f32)],
        compiler_params=room(8),
        name="finish",
    )(got, pairs, pair_exchange, vectors, energies)


def solution(mesh):
    split = Mesh(mesh.devices.reshape(SIZES), NAMES)
    return jax.shard_map(
        on_device,
        mesh=split,
        in_specs=(
            P(NAMES, None, None),
            P(NAMES, None, None),
            P(NAMES, None, None),
            P(),
            P(),
            P(NAMES, None),
            P(NAMES, None),
            P(NAMES, None),
        ),
        out_specs=(P(NAMES, None), P()),
        check_vma=False,
    )
```

```python
import jax
import jax.numpy as jnp
import numpy as np
from jax import lax
from jax.experimental import pallas as pl
from jax.experimental.pallas import tpu as pltpu
from jax.sharding import Mesh
from jax.sharding import PartitionSpec as P

MX = 32
MY = 32
NK = 1024
NB = 16
NG = 1024
NV = 32
NT = NK * NB
NQ = 289
SPAN = NK // 4
NAMES = ("zh", "zl", "yl", "c", "x", "yh")
SIZES = (4, 2, 2, 2, 4, 4)
A = ("zh", "zl", "yh")
B = ("x", "yl", "c")
NA = 32
NBB = 16
ND = NA * NBB
HALF = NG // 2
ROWS = NBB + 10
FIELD = NA + NA // 2
WIDE = FIELD + 16
LANES = 128

f32 = jnp.float32
bf16 = jnp.bfloat16
HIGH = lax.Precision.HIGHEST


def split_table(x):
    hi = x.astype(bf16)
    lo = (x - hi.astype(np.float64)).astype(bf16)
    return np.concatenate([hi, lo], axis=0)


def tables():
    m = np.arange(32)
    phase = 2.0 * np.pi * ((m[:, None] * m[None, :]) % 32) / 32.0
    cas = np.cos(phase) + np.sin(phase)
    first = split_table(np.repeat(cas[:, 0:16], 16, axis=1))
    second = split_table(np.tile(cas[:, 0:16], (1, 8)) / 32.0)
    f = np.arange(17)
    weight = np.where((f == 0) | (f == 16), 1.0, 2.0)
    cos = weight[:, None] * np.cos(2.0 * np.pi * ((f[:, None] * m[None, :]) % 32) / 32.0)
    outer = np.zeros((24, 2 * SPAN), np.float32)
    outer[0:17] = np.repeat(cos, 16, axis=1)
    inner = np.concatenate(
        [np.tile(cos[:, h : h + 16], (17, LANES // 16)) for h in (0, 16)], axis=1
    ).astype(np.float32)
    return first, second, outer, inner


def iota(shape, axis):
    return lax.broadcasted_iota(jnp.int32, shape, axis)


def block_sum(x):
    x = x + pltpu.roll(x, 32, 1)
    return x + pltpu.roll(x, 64, 1)


def keep_block(x, wanted):
    return jnp.where(iota(x.shape, 1) // 32 == wanted, x, 0.0)


def spread_vectors(vec_ref, wide):
    rows = [
        vec_ref[k : k + 1, v * LANES : (v + 1) * LANES].astype(f32)
        for k in range(2)
        for v in range(4)
    ]
    x8 = jnp.concatenate(rows, axis=0)
    for c in range(4):
        wide[pl.ds(c, 8, stride=4), :] = x8
    x = wide[...]
    return block_sum(keep_block(x, iota(x.shape, 0) % 4))


def energy_column(energy_ref):
    first = jnp.broadcast_to(energy_ref[0:1, :], (NB, NB))
    second = jnp.broadcast_to(energy_ref[1:2, :], (NB, NB))
    e = jnp.concatenate([first, second], axis=0)
    return jnp.sum(
        jnp.where(iota(e.shape, 1) == iota(e.shape, 0) % NB, e, 0.0), axis=1, keepdims=True
    )


def exchange_rows(pe_ref):
    return jnp.concatenate(
        [pe_ref[k, :, g * HALF : (g + 1) * HALF] for g in range(2) for k in range(2)], axis=0
    )


def dot_t(x, y):
    return lax.dot_general(x, y, (((0,), (0,)), ((), ())), preferred_element_type=f32)


def dot_nt(x, y):
    return lax.dot_general(x, y, (((1,), (1,)), ((), ())), preferred_element_type=f32)


def spectrum(lane_at, tiles, outer, inner):
    own = iota((NQ, LANES), 1) == lane_at
    pick = jnp.where(iota((24, NQ), 0) == iota((24, NQ), 1) // 17, 1.0, 0.0).astype(bf16)
    parts = []
    for g in range(2):
        column = jnp.sum(jnp.where(own, tiles[g], 0.0), axis=1, keepdims=True)
        exact = column * inner[...]
        hi = exact.astype(bf16)
        lo = (exact - hi.astype(f32)).astype(bf16)
        parts.append(
            jnp.dot(pick, hi, preferred_element_type=f32)
            + jnp.dot(pick, lo, preferred_element_type=f32)
        )
    out = []
    for q in range(4):
        for g in range(2):
            part = parts[g][:, (q % 2) * LANES : (q % 2 + 1) * LANES]
            line = []
            for j in range(SPAN // LANES):
                at = (q // 2) * SPAN + j * LANES
                line.append(
                    jnp.sum(outer[:, at : at + LANES] * part, axis=0, keepdims=True)
                )
            out.append(jnp.concatenate(line, axis=1))
    return out


def pack_kernel(*refs):
    far, (msg, pairs, gram, lam, first, second) = refs[:12], refs[12:18]
    coords, cond, val, vec, pe, energy, tiles, bare, outer, inner, wide, rows, lines, sem = refs[18:]
    mine = lax.axis_index(B) * NA + lax.axis_index(A)
    tile = pl.multiple_of((mine // LANES) * LANES, LANES)
    near = (coords, cond, val, vec, pe, energy, inner, outer, bare, first, second)
    pairs_of = list(zip(far[:6] + far[7:], near))
    pairs_of += [(far[6].at[:, pl.ds(tile + g * HALF, LANES)], tiles.at[g]) for g in range(2)]
    copies = [
        pltpu.make_async_copy(src, dst, sem.at[i]) for i, (src, dst) in enumerate(pairs_of)
    ]
    for copy in copies:
        copy.start()
    for copy in copies[:6]:
        copy.wait()
    x = spread_vectors(vec, wide)
    for k in range(2):
        cf = cond[k].astype(f32)
        vf = val[k].astype(f32)
        for v in range(4):
            both = vf[v : v + 1, :] * cf
            for g in range(2):
                at = k * 32 + g * 16 + v * 4
                rows[at : at + 4, :] = both[:, g * HALF : (g + 1) * HALF]
    left = rows[...].astype(bf16)
    pairs[...] = left
    xp = jnp.concatenate([x[0:16], x[0:16], x[16:32], x[16:32]], axis=0)
    xp = keep_block(xp, iota(xp.shape, 0) // 16).astype(bf16)
    xd = jnp.concatenate([x, x], axis=0)
    xd = keep_block(xd, iota(xd.shape, 0) // 32).astype(bf16)
    lane = iota((1, LANES), 1)
    place = jnp.zeros((1, LANES), f32)
    for k in range(2):
        for s in range(2):
            place = jnp.where(lane == 64 + 2 * k + s, coords[k : k + 1, s : s + 1].astype(f32), place)
    lines[pl.ds(0, ND, stride=2), :] = dot_t(left, xp)
    lines[pl.ds(1, ND, stride=2), :] = dot_t(exchange_rows(pe), xd) + place
    msg[...] = lines[...].astype(bf16)
    gram[...] = lax.dot_general(
        x[:, 0:32],
        energy_column(energy) * x,
        (((0,), (0,)), ((), ())),
        precision=HIGH,
        preferred_element_type=f32,
    )
    for copy in copies[6:]:
        copy.wait()
    index = iota((8, LANES), 0) * LANES + iota((8, LANES), 1)
    lines_of = spectrum(mine - tile, tiles, outer, inner)
    for g in range(2):
        factor = jnp.sum(jnp.where(index == mine + g * HALF, bare[...], 0.0), keepdims=True)
        lines_of.append(jnp.broadcast_to(factor, (1, SPAN)))
    lam[...] = jnp.concatenate(lines_of + [jnp.zeros((6, SPAN), f32)], axis=0)


def spectral_kernel(got, gram, lam, first, second, msg, lines, wide):
    lines[0 : 2 * ND, :] = got[...].astype(f32)
    proj = jnp.transpose(lines[pl.ds(0, ND, stride=2), :])
    rest = lines[pl.ds(1, ND, stride=2), :]
    turned = jnp.transpose(rest)
    slot = iota((ND, 64), 1) % 32
    left = iota((ND, LANES), 1) < 64
    basis, sign = [], []
    hat = None
    for k in range(2):
        at = [rest[:, 64 + 2 * k + s : 65 + 2 * k + s].astype(jnp.int32) for s in range(2)]
        ones = [jnp.where(slot == p, 1.0, 0.0).astype(bf16) for p in at]
        ta = jnp.dot(ones[0], first[...], preferred_element_type=f32)
        tb = jnp.dot(ones[1], second[...], preferred_element_type=f32)
        exact = ta * jnp.concatenate([tb] * (SPAN // LANES), axis=1)
        hi = exact.astype(bf16)
        lo = (exact - hi.astype(f32)).astype(bf16)
        basis.append((hi, lo))
        sa, sb = [(1 - 2 * (p % 2)).astype(f32) for p in at]
        sign.append((sb, sa, sa * sb))
        at = [turned[64 + 2 * k + s : 65 + 2 * k + s].astype(jnp.int32) for s in range(2)]
        sa, sb = [(1 - 2 * (p % 2)).astype(f32) for p in at]
        own = proj[k * 64 : (k + 1) * 64]
        own = jnp.concatenate([own, own * sb, own * sa, own * (sa * sb)], axis=0).astype(bf16)
        part = jnp.dot(own, hi, preferred_element_type=f32) + jnp.dot(
            own, lo, preferred_element_type=f32
        )
        hat = part if hat is None else hat + part
    scale = jnp.concatenate(
        [jnp.broadcast_to(lam[r : r + 1, :], (32, SPAN)) for r in range(8)], axis=0
    )
    exact = hat * scale
    scaled = exact.astype(bf16)
    finer = (exact - scaled.astype(f32)).astype(bf16)
    hat = hat.astype(bf16)
    both = jnp.concatenate(
        [v[q * 64 : (q + 1) * 64] for q in range(4) for v in (scaled, finer)], axis=0
    )
    back = []
    for k in range(2):
        sb, sa, sab = sign[k]
        wide_r = dot_nt(basis[k][0], both)
        r = wide_r[:, 0:LANES] + sb * wide_r[:, LANES : 2 * LANES]
        r = r + sa * wide_r[:, 2 * LANES : 3 * LANES] + sab * wide_r[:, 3 * LANES : 4 * LANES]
        small = dot_nt(basis[k][1], scaled)
        r = r + jnp.where(left, 1.0, sb) * small[:, 0:LANES]
        r = r + jnp.where(left, sa, sab) * small[:, LANES : 2 * LANES]
        back.append(r + pltpu.roll(r, 64, 1))
    back = jnp.where(left, back[0], back[1])
    direct = None
    for g in range(2):
        x, y = [
            jnp.concatenate(
                [v[q * 64 + g * 32 : q * 64 + g * 32 + 32] for q in range(4)], axis=1
            )
            for v in (hat, scaled)
        ]
        part = dot_nt(x, jnp.concatenate([y] * 4, axis=0))
        direct = part if direct is None else direct + part
    for b in range(NBB):
        lines[pl.ds(b, NA, stride=ROWS), :] = back[b * NA : (b + 1) * NA]
    lane = iota((1, LANES), 1)
    dens = jnp.sum(rest, axis=0, keepdims=True)
    outer = jnp.zeros((32, LANES), f32)
    cd = jnp.zeros((1, LANES), f32)
    for g in range(2):
        factor = lam[8 + g : 9 + g, 0:LANES]
        own = jnp.where(lane // 32 == g, dens, 0.0)
        row = block_sum(own)
        column = jnp.sum(
            jnp.where(iota((32, LANES), 0) == iota((32, LANES), 1), row, 0.0), axis=1, keepdims=True
        )
        outer = outer + column * (factor * row)
        cd = cd + factor * own
    alpha = (gram[...] + (2.0 / NT) * outer - direct / NK) / NT
    wide[...] = keep_block(alpha, iota((32, LANES), 0) % 4)
    packed = wide[pl.ds(0, 8, stride=4), :]
    for c in range(1, 4):
        packed = packed + wide[pl.ds(c, 8, stride=4), :]
    tail = jnp.concatenate([packed, cd, jnp.zeros((1, LANES), f32)], axis=0)
    for r in range(ROWS - NBB):
        lines[pl.ds(NBB + r, NA, stride=ROWS), :] = jnp.broadcast_to(tail[r : r + 1], (NA, LANES))
    msg[...] = lines[0 : NA * ROWS, :].astype(bf16)


def relay_kernel(got, msg, lines):
    lines[...] = got[...].astype(f32)
    alpha = []
    for r in range(8):
        part = lines[pl.ds(NBB + r, NA, stride=ROWS), :]
        alpha.append(jnp.sum(part, axis=0, keepdims=True))
    alpha = jnp.concatenate(alpha, axis=0)
    hi = alpha.astype(bf16).astype(f32)
    cd = lines[pl.ds(NBB + 8, NA, stride=ROWS), :]
    cd = cd[0 : NA // 2] + pltpu.roll(cd[NA // 2 :], 64, 1)
    tail = jnp.concatenate([cd, hi, alpha - hi], axis=0).astype(bf16)
    for b in range(NBB):
        msg[b, 0:NA, :] = lines[pl.ds(b, NA, stride=ROWS), :].astype(bf16)
        msg[b, NA:WIDE, :] = tail


def finish_kernel(got, pairs, pe, vec, energy, out, alpha_out, wide, rows):
    x = spread_vectors(vec, wide)
    potential = got[:, 0:NA, :].reshape(ND, LANES)
    field = []
    for b in range(NBB):
        part = got[b, NA:FIELD, :].astype(f32)
        field += [part, pltpu.roll(part, 64, 1)]
    field = jnp.concatenate(field, axis=0).astype(bf16)
    direct = jnp.dot(pairs[...], potential, preferred_element_type=f32)
    direct = block_sum(keep_block(direct, iota(direct.shape, 0) // 16))
    direct = jnp.concatenate([direct[0:16] + direct[16:32], direct[32:48] + direct[48:64]], axis=0)
    exchange = jnp.dot(exchange_rows(pe), field, preferred_element_type=f32)
    exchange = block_sum(keep_block(exchange, iota(exchange.shape, 0) // 32))
    exchange = exchange[0:32] + exchange[32:64]
    applied = energy_column(energy) * x + (2.0 / NT) * exchange - direct / NK
    alpha = jnp.zeros((16, LANES), f32)
    for b in range(NBB):
        alpha = alpha + got[b, FIELD:WIDE, :].astype(f32)
    alpha = alpha[0:8] + alpha[8:16]
    for c in range(4):
        wide[pl.ds(c, 8, stride=4), :] = alpha
    full = wide[...]
    full = block_sum(keep_block(full, iota(full.shape, 0) % 4))
    alpha_out[...] = full[:, 0:32]
    shift = jnp.dot(x[:, 0:32], full, precision=HIGH, preferred_element_type=f32)
    rows[...] = keep_block(applied - shift, iota((32, LANES), 0) % 4)
    packed = rows[pl.ds(0, 8, stride=4), :]
    for c in range(1, 4):
        packed = packed + rows[pl.ds(c, 8, stride=4), :]
    for k in range(2):
        for v in range(4):
            out[k : k + 1, v * LANES : (v + 1) * LANES] = packed[k * 4 + v : k * 4 + v + 1, :]


def vmem():
    return pl.BlockSpec(memory_space=pltpu.VMEM)


def room(mib):
    return pltpu.CompilerParams(vmem_limit_bytes=mib << 20)


def in_hbm(x):
    return pltpu.with_memory_space_constraint(jnp.asarray(x), pltpu.HBM)


def sds(shape, dtype):
    return jax.ShapeDtypeStruct(shape, dtype)


def on_device(pair_exchange, conduction, valence, coulomb, screening, energies, vectors, k_coords):
    first, second, outer, inner = tables()
    far = (k_coords, conduction, valence, vectors, pair_exchange, energies, screening)
    far += (inner, outer, coulomb.reshape(8, LANES), first, second)
    any_space = pl.BlockSpec(memory_space=pl.ANY)
    own = [pltpu.VMEM(v.shape, v.dtype) for v in far[:6]]
    msg, pairs, gram, lam, first, second = pl.pallas_call(
        pack_kernel,
        out_shape=(
            sds((2 * ND, LANES), bf16),
            sds((64, HALF), bf16),
            sds((32, LANES), f32),
            sds((16, SPAN), f32),
            sds((64, SPAN), bf16),
            sds((64, LANES), bf16),
        ),
        in_specs=[any_space] * len(far),
        out_specs=(vmem(),) * 6,
        scratch_shapes=own
        + [
            pltpu.VMEM((2, NQ, LANES), f32),
            pltpu.VMEM((8, LANES), f32),
            pltpu.VMEM((24, 2 * SPAN), f32),
            pltpu.VMEM((NQ, 2 * LANES), f32),
            pltpu.VMEM((32, LANES), f32),
            pltpu.VMEM((64, HALF), f32),
            pltpu.VMEM((2 * ND, LANES), f32),
            pltpu.SemaphoreType.DMA((13,)),
        ],
        compiler_params=room(12),
        name="pack",
    )(*[in_hbm(v) for v in far])
    got = lax.all_to_all(msg.reshape(ND, 2, LANES), B + A, 0, 0, tiled=True)
    out = pl.pallas_call(
        spectral_kernel,
        out_shape=sds((NA * ROWS, LANES), bf16),
        in_specs=[vmem()] * 5,
        out_specs=vmem(),
        scratch_shapes=[
            pltpu.VMEM((max(2 * ND, NA * ROWS), LANES), f32),
            pltpu.VMEM((32, LANES), f32),
        ],
        compiler_params=room(28),
        name="spectral",
    )(got.reshape(2 * ND, LANES), gram, lam, first, second)
    got = lax.all_to_all(out.reshape(NA, ROWS // 2, 2, LANES), A, 0, 0, tiled=True)
    out = pl.pallas_call(
        relay_kernel,
        out_shape=sds((NBB, WIDE, LANES), bf16),
        in_specs=[vmem()],
        out_specs=vmem(),
        scratch_shapes=[pltpu.VMEM((NA * ROWS, LANES), f32)],
        compiler_params=room(8),
        name="relay",
    )(got.reshape(NA * ROWS, LANES))
    got = lax.all_to_all(out, B, 0, 0, tiled=True)
    return pl.pallas_call(
        finish_kernel,
        out_shape=(sds((2, NB * NV), f32), sds((NV, NV), f32)),
        in_specs=[vmem()] * 5,
        out_specs=(vmem(), vmem()),
        scratch_shapes=[pltpu.VMEM((32, LANES), f32), pltpu.VMEM((32, LANES), f32)],
        compiler_params=room(8),
        name="finish",
    )(got, pairs, pair_exchange, vectors, energies)


def solution(mesh):
    split = Mesh(mesh.devices.reshape(SIZES), NAMES)
    return jax.shard_map(
        on_device,
        mesh=split,
        in_specs=(
            P(NAMES, None, None),
            P(NAMES, None, None),
            P(NAMES, None, None),
            P(),
            P(),
            P(NAMES, None),
            P(NAMES, None),
            P(NAMES, None),
        ),
        out_specs=(P(NAMES, None), P()),
        check_vma=False,
    )
```

```python
import jax
import jax.numpy as jnp
import numpy as np
from jax import lax
from jax.experimental import pallas as pl
from jax.experimental.pallas import tpu as pltpu
from jax.sharding import Mesh
from jax.sharding import PartitionSpec as P

MX = 32
MY = 32
NK = 1024
NB = 16
NG = 1024
NV = 32
NT = NK * NB
NQ = 289
SPAN = NK // 4
NAMES = ("zh", "zl", "yl", "c", "x", "yh")
SIZES = (4, 2, 2, 2, 4, 4)
A = ("zh", "zl", "yh")
B = ("c", "x", "yl")
NA = 32
NBB = 16
ND = NA * NBB
HALF = NG // 2
ROWS = NBB + 10
FIELD = NA + NA // 2
WIDE = FIELD + 16
LANES = 128

f32 = jnp.float32
bf16 = jnp.bfloat16
HIGH = lax.Precision.HIGHEST


def split_table(x):
    hi = x.astype(bf16)
    lo = (x - hi.astype(np.float64)).astype(bf16)
    return np.concatenate([hi, lo], axis=0)


def tables():
    m = np.arange(32)
    phase = 2.0 * np.pi * ((m[:, None] * m[None, :]) % 32) / 32.0
    cas = np.cos(phase) + np.sin(phase)
    first = split_table(np.repeat(cas[:, 0:16], 16, axis=1))
    second = split_table(np.tile(cas[:, 0:16], (1, 8)) / 32.0)
    f = np.arange(17)
    weight = np.where((f == 0) | (f == 16), 1.0, 2.0)
    cos = weight[:, None] * np.cos(2.0 * np.pi * ((f[:, None] * m[None, :]) % 32) / 32.0)
    outer = np.zeros((24, 2 * SPAN), np.float32)
    outer[0:17] = np.repeat(cos, 16, axis=1)
    inner = np.concatenate(
        [np.tile(cos[:, h : h + 16], (17, LANES // 16)) for h in (0, 16)], axis=1
    ).astype(np.float32)
    return first, second, outer, inner


def iota(shape, axis):
    return lax.broadcasted_iota(jnp.int32, shape, axis)


def block_sum(x):
    x = x + pltpu.roll(x, 32, 1)
    return x + pltpu.roll(x, 64, 1)


def keep_block(x, wanted):
    return jnp.where(iota(x.shape, 1) >> 5 == wanted, x, 0.0)


def spread_vectors(vec_ref, wide):
    rows = [
        vec_ref[k : k + 1, v * LANES : (v + 1) * LANES].astype(f32)
        for k in range(2)
        for v in range(4)
    ]
    x8 = jnp.concatenate(rows, axis=0)
    for c in range(4):
        wide[pl.ds(c, 8, stride=4), :] = x8
    x = wide[...]
    return block_sum(keep_block(x, iota(x.shape, 0) & 3))


def energy_column(energy_ref):
    first = jnp.broadcast_to(energy_ref[0:1, :], (NB, NB))
    second = jnp.broadcast_to(energy_ref[1:2, :], (NB, NB))
    e = jnp.concatenate([first, second], axis=0)
    return jnp.sum(
        jnp.where(iota(e.shape, 1) == (iota(e.shape, 0) & (NB - 1)), e, 0.0), axis=1, keepdims=True
    )


def exchange_rows(pe_ref):
    return jnp.concatenate(
        [pe_ref[k, :, g * HALF : (g + 1) * HALF] for g in range(2) for k in range(2)], axis=0
    )


def dot_t(x, y):
    return lax.dot_general(x, y, (((0,), (0,)), ((), ())), preferred_element_type=f32)


def dot_nt(x, y):
    return lax.dot_general(x, y, (((1,), (1,)), ((), ())), preferred_element_type=f32)


def spectrum(lane_at, tiles, outer, inner):
    own = iota((NQ, LANES), 1) == lane_at
    pick = jnp.where(iota((24, NQ), 0) == iota((24, NQ), 1) // 17, 1.0, 0.0).astype(bf16)
    parts = []
    for g in range(2):
        column = jnp.sum(jnp.where(own, tiles[g], 0.0), axis=1, keepdims=True)
        exact = column * inner[...]
        hi = exact.astype(bf16)
        lo = (exact - hi.astype(f32)).astype(bf16)
        parts.append(
            jnp.dot(pick, hi, preferred_element_type=f32)
            + jnp.dot(pick, lo, preferred_element_type=f32)
        )
    out = []
    for q in range(4):
        for g in range(2):
            part = parts[g][:, (q % 2) * LANES : (q % 2 + 1) * LANES]
            line = []
            for j in range(SPAN // LANES):
                at = (q // 2) * SPAN + j * LANES
                line.append(
                    jnp.sum(outer[:, at : at + LANES] * part, axis=0, keepdims=True)
                )
            out.append(jnp.concatenate(line, axis=1))
    return out


def pack_kernel(*refs):
    far, (msg, pairs, gram), kept = refs[:12], refs[12:15], refs[15:21]
    coords, cond, val, vec, pe, energy, wide, rows, lines, sem = refs[21:]
    inner, outer, bare, first, second, tiles = kept
    mine = lax.axis_index(B) * NA + lax.axis_index(A)
    tile = pl.multiple_of((mine // LANES) * LANES, LANES)
    near = (coords, cond, val, vec, pe, energy, inner, outer, bare, first, second)
    pairs_of = list(zip(far[:6] + far[7:], near))
    pairs_of += [(far[6].at[:, pl.ds(tile + g * HALF, LANES)], tiles.at[g]) for g in range(2)]
    copies = [
        pltpu.make_async_copy(src, dst, sem.at[i]) for i, (src, dst) in enumerate(pairs_of)
    ]
    for copy in copies:
        copy.start()
    for copy in copies[:6]:
        copy.wait()
    x = spread_vectors(vec, wide)
    for k in range(2):
        cf = cond[k].astype(f32)
        vf = val[k].astype(f32)
        for v in range(4):
            both = vf[v : v + 1, :] * cf
            for g in range(2):
                at = k * 32 + g * 16 + v * 4
                rows[at : at + 4, :] = both[:, g * HALF : (g + 1) * HALF]
    left = rows[...].astype(bf16)
    pairs[...] = left
    xp = jnp.concatenate([x[0:16], x[0:16], x[16:32], x[16:32]], axis=0)
    xp = keep_block(xp, iota(xp.shape, 0) >> 4).astype(bf16)
    xd = jnp.concatenate([x, x], axis=0)
    xd = keep_block(xd, iota(xd.shape, 0) >> 5).astype(bf16)
    lane = iota((1, LANES), 1)
    place = jnp.zeros((1, LANES), f32)
    for k in range(2):
        for s in range(2):
            place = jnp.where(lane == 64 + 2 * k + s, coords[k : k + 1, s : s + 1].astype(f32), place)
    lines[pl.ds(0, ND, stride=2), :] = dot_t(left, xp)
    lines[pl.ds(1, ND, stride=2), :] = dot_t(exchange_rows(pe), xd) + place
    msg[...] = lines[...].astype(bf16)
    gram[...] = lax.dot_general(
        x[:, 0:32],
        energy_column(energy) * x,
        (((0,), (0,)), ((), ())),
        precision=HIGH,
        preferred_element_type=f32,
    )
    for copy in copies[6:]:
        copy.wait()


def spectral_kernel(
    got, gram, inner, outer_table, bare, first, second, tiles, msg, lines, wide
):
    mine = lax.axis_index(B) * NA + lax.axis_index(A)
    lam = spectrum(mine % LANES, tiles, outer_table, inner)
    index = iota((8, LANES), 0) * LANES + iota((8, LANES), 1)
    factors = [
        jnp.sum(jnp.where(index == mine + g * HALF, bare[...], 0.0), keepdims=True)
        for g in range(2)
    ]
    lines[0 : 2 * ND, :] = got[...].astype(f32)
    proj = jnp.transpose(lines[pl.ds(0, ND, stride=2), :])
    rest = lines[pl.ds(1, ND, stride=2), :]
    turned = jnp.transpose(rest)
    slot = iota((ND, 64), 1) & 31
    left = iota((ND, LANES), 1) < 64
    basis, sign = [], []
    hat = None
    for k in range(2):
        at = [
            jnp.broadcast_to(rest[:, 64 + 2 * k + s : 65 + 2 * k + s], (ND, LANES)).astype(jnp.int32)
            for s in range(2)
        ]
        ones = [jnp.where(slot == p[:, 0:64], 1.0, 0.0).astype(bf16) for p in at]
        ta = jnp.dot(ones[0], first[...], preferred_element_type=f32)
        tb = jnp.dot(ones[1], second[...], preferred_element_type=f32)
        exact = ta * jnp.concatenate([tb] * (SPAN // LANES), axis=1)
        hi = exact.astype(bf16)
        lo = (exact - hi.astype(f32)).astype(bf16)
        basis.append((hi, lo))
        sa, sb = [jnp.where((p & 1) == 0, 1.0, -1.0) for p in at]
        sign.append((sb, sa, sa * sb))
        at = [turned[64 + 2 * k + s : 65 + 2 * k + s].astype(jnp.int32) for s in range(2)]
        sa, sb = [jnp.where((p & 1) == 0, 1.0, -1.0) for p in at]
        own = proj[k * 64 : (k + 1) * 64]
        own = jnp.concatenate([own, own * sb, own * sa, own * (sa * sb)], axis=0).astype(bf16)
        part = jnp.dot(own, hi, preferred_element_type=f32) + jnp.dot(
            own, lo, preferred_element_type=f32
        )
        hat = part if hat is None else hat + part
    scale = jnp.concatenate(
        [jnp.broadcast_to(line, (32, SPAN)) for line in lam], axis=0
    )
    exact = hat * scale
    scaled = exact.astype(bf16)
    finer = (exact - scaled.astype(f32)).astype(bf16)
    hat = hat.astype(bf16)
    both = jnp.concatenate(
        [v[q * 64 : (q + 1) * 64] for q in range(4) for v in (scaled, finer)], axis=0
    )
    back = []
    for k in range(2):
        sb, sa, sab = sign[k]
        wide_r = dot_nt(basis[k][0], both)
        r = wide_r[:, 0:LANES] + sb * wide_r[:, LANES : 2 * LANES]
        r = r + sa * wide_r[:, 2 * LANES : 3 * LANES] + sab * wide_r[:, 3 * LANES : 4 * LANES]
        small = dot_nt(basis[k][1], scaled)
        r = r + jnp.where(left, 1.0, sb) * small[:, 0:LANES]
        r = r + jnp.where(left, sa, sab) * small[:, LANES : 2 * LANES]
        back.append(r + pltpu.roll(r, 64, 1))
    back = jnp.where(left, back[0], back[1])
    direct = None
    for g in range(2):
        x, y = [
            jnp.concatenate(
                [v[q * 64 + g * 32 : q * 64 + g * 32 + 32] for q in range(4)], axis=1
            )
            for v in (hat, scaled)
        ]
        part = dot_nt(x, jnp.concatenate([y] * 4, axis=0))
        direct = part if direct is None else direct + part
    for b in range(NBB):
        lines[pl.ds(b, NA, stride=ROWS), :] = back[b * NA : (b + 1) * NA]
    lane = iota((1, LANES), 1)
    dens = jnp.sum(rest, axis=0, keepdims=True)
    outer = jnp.zeros((32, LANES), f32)
    cd = jnp.zeros((1, LANES), f32)
    for g in range(2):
        factor = factors[g]
        own = jnp.where(lane >> 5 == g, dens, 0.0)
        row = block_sum(own)
        column = jnp.sum(
            jnp.where(iota((32, LANES), 0) == iota((32, LANES), 1), row, 0.0), axis=1, keepdims=True
        )
        outer = outer + column * (factor * row)
        cd = cd + factor * own
    alpha = (gram[...] + (2.0 / NT) * outer - direct / NK) / NT
    wide[...] = keep_block(alpha, iota((32, LANES), 0) & 3)
    packed = wide[pl.ds(0, 8, stride=4), :]
    for c in range(1, 4):
        packed = packed + wide[pl.ds(c, 8, stride=4), :]
    tail = jnp.concatenate([packed, cd, jnp.zeros((1, LANES), f32)], axis=0)
    for r in range(ROWS - NBB):
        lines[pl.ds(NBB + r, NA, stride=ROWS), :] = jnp.broadcast_to(tail[r : r + 1], (NA, LANES))
    msg[...] = lines[0 : NA * ROWS, :].astype(bf16)


def relay_kernel(got, msg, lines):
    lines[...] = got[...].astype(f32)
    alpha = []
    for r in range(8):
        part = lines[pl.ds(NBB + r, NA, stride=ROWS), :]
        alpha.append(jnp.sum(part, axis=0, keepdims=True))
    alpha = jnp.concatenate(alpha, axis=0)
    hi = alpha.astype(bf16).astype(f32)
    cd = lines[pl.ds(NBB + 8, NA, stride=ROWS), :]
    cd = cd[0 : NA // 2] + pltpu.roll(cd[NA // 2 :], 64, 1)
    tail = jnp.concatenate([cd, hi, alpha - hi], axis=0).astype(bf16)
    for b in range(NBB):
        msg[b, 0:NA, :] = lines[pl.ds(b, NA, stride=ROWS), :].astype(bf16)
        msg[b, NA:WIDE, :] = tail


def finish_kernel(got, pairs, pe, vec, energy, out, alpha_out, wide, rows):
    x = spread_vectors(vec, wide)
    potential = got[:, 0:NA, :].reshape(ND, LANES)
    field = []
    for b in range(NBB):
        part = got[b, NA:FIELD, :].astype(f32)
        field += [part, pltpu.roll(part, 64, 1)]
    field = jnp.concatenate(field, axis=0).astype(bf16)
    direct = jnp.dot(pairs[...], potential, preferred_element_type=f32)
    direct = block_sum(keep_block(direct, iota(direct.shape, 0) >> 4))
    direct = jnp.concatenate([direct[0:16] + direct[16:32], direct[32:48] + direct[48:64]], axis=0)
    exchange = jnp.dot(exchange_rows(pe), field, preferred_element_type=f32)
    exchange = block_sum(keep_block(exchange, iota(exchange.shape, 0) >> 5))
    exchange = exchange[0:32] + exchange[32:64]
    applied = energy_column(energy) * x + (2.0 / NT) * exchange - direct / NK
    alpha = jnp.zeros((16, LANES), f32)
    for b in range(NBB):
        alpha = alpha + got[b, FIELD:WIDE, :].astype(f32)
    alpha = alpha[0:8] + alpha[8:16]
    for c in range(4):
        wide[pl.ds(c, 8, stride=4), :] = alpha
    full = wide[...]
    full = block_sum(keep_block(full, iota(full.shape, 0) & 3))
    alpha_out[...] = full[:, 0:32]
    shift = jnp.dot(x[:, 0:32], full, precision=HIGH, preferred_element_type=f32)
    rows[...] = keep_block(applied - shift, iota((32, LANES), 0) & 3)
    packed = rows[pl.ds(0, 8, stride=4), :]
    for c in range(1, 4):
        packed = packed + rows[pl.ds(c, 8, stride=4), :]
    for k in range(2):
        for v in range(4):
            out[k : k + 1, v * LANES : (v + 1) * LANES] = packed[k * 4 + v : k * 4 + v + 1, :]


def vmem():
    return pl.BlockSpec(memory_space=pltpu.VMEM)


def room(mib):
    return pltpu.CompilerParams(vmem_limit_bytes=mib << 20)


def in_hbm(x):
    return pltpu.with_memory_space_constraint(jnp.asarray(x), pltpu.HBM)


def sds(shape, dtype):
    return jax.ShapeDtypeStruct(shape, dtype)


def on_device(pair_exchange, conduction, valence, coulomb, screening, energies, vectors, k_coords):
    first, second, outer, inner = tables()
    far = (k_coords, conduction, valence, vectors, pair_exchange, energies, screening)
    far += (inner, outer, coulomb.reshape(8, LANES), first, second)
    any_space = pl.BlockSpec(memory_space=pl.ANY)
    own = [pltpu.VMEM(v.shape, v.dtype) for v in far[:6]]
    msg, pairs, gram, *kept = pl.pallas_call(
        pack_kernel,
        out_shape=(
            sds((2 * ND, LANES), bf16),
            sds((64, HALF), bf16),
            sds((32, LANES), f32),
            sds((NQ, 2 * LANES), f32),
            sds((24, 2 * SPAN), f32),
            sds((8, LANES), f32),
            sds((64, SPAN), bf16),
            sds((64, LANES), bf16),
            sds((2, NQ, LANES), f32),
        ),
        in_specs=[any_space] * len(far),
        out_specs=(vmem(),) * 9,
        scratch_shapes=own
        + [
            pltpu.VMEM((32, LANES), f32),
            pltpu.VMEM((64, HALF), f32),
            pltpu.VMEM((2 * ND, LANES), f32),
            pltpu.SemaphoreType.DMA((13,)),
        ],
        compiler_params=room(12),
        name="pack",
    )(*[in_hbm(v) for v in far])
    got = lax.all_to_all(msg.reshape(ND, 2, LANES), B + A, 0, 0, tiled=True)
    out = pl.pallas_call(
        spectral_kernel,
        out_shape=sds((NA * ROWS, LANES), bf16),
        in_specs=[vmem()] * 8,
        out_specs=vmem(),
        scratch_shapes=[
            pltpu.VMEM((max(2 * ND, NA * ROWS), LANES), f32),
            pltpu.VMEM((32, LANES), f32),
        ],
        compiler_params=room(28),
        name="spectral",
    )(got.reshape(2 * ND, LANES), gram, *kept)
    got = lax.all_to_all(out.reshape(NA, ROWS // 2, 2, LANES), A, 0, 0, tiled=True)
    out = pl.pallas_call(
        relay_kernel,
        out_shape=sds((NBB, WIDE, LANES), bf16),
        in_specs=[vmem()],
        out_specs=vmem(),
        scratch_shapes=[pltpu.VMEM((NA * ROWS, LANES), f32)],
        compiler_params=room(8),
        name="relay",
    )(got.reshape(NA * ROWS, LANES))
    got = lax.all_to_all(out, B, 0, 0, tiled=True)
    return pl.pallas_call(
        finish_kernel,
        out_shape=(sds((2, NB * NV), f32), sds((NV, NV), f32)),
        in_specs=[vmem()] * 5,
        out_specs=(vmem(), vmem()),
        scratch_shapes=[pltpu.VMEM((32, LANES), f32), pltpu.VMEM((32, LANES), f32)],
        compiler_params=room(8),
        name="finish",
    )(got, pairs, pair_exchange, vectors, energies)


def solution(mesh):
    split = Mesh(mesh.devices.reshape(SIZES), NAMES)
    return jax.shard_map(
        on_device,
        mesh=split,
        in_specs=(
            P(NAMES, None, None),
            P(NAMES, None, None),
            P(NAMES, None, None),
            P(),
            P(),
            P(NAMES, None),
            P(NAMES, None),
            P(NAMES, None),
        ),
        out_specs=(P(NAMES, None), P()),
        check_vma=False,
    )
```

```python
import jax
import jax.numpy as jnp
import numpy as np
from jax import lax
from jax.experimental import pallas as pl
from jax.experimental.pallas import tpu as pltpu
from jax.sharding import Mesh
from jax.sharding import PartitionSpec as P

MX = 32
MY = 32
NK = 1024
NB = 16
NG = 1024
NV = 32
NT = NK * NB
NQ = 289
SPAN = NK // 4
NAMES = ("zh", "zl", "yl", "c", "x", "yh")
SIZES = (4, 2, 2, 2, 4, 4)
A = ("zh", "zl", "yh")
B = ("c", "x", "yl")
NA = 32
NBB = 16
ND = NA * NBB
HALF = NG // 2
ROWS = NBB + 6
FIELD = NA + NA // 2
WIDE = FIELD + 8
LANES = 128

f32 = jnp.float32
bf16 = jnp.bfloat16
HIGH = lax.Precision.HIGHEST


def split_table(x):
    hi = x.astype(bf16)
    lo = (x - hi.astype(np.float64)).astype(bf16)
    return np.concatenate([hi, lo], axis=0)


def tables():
    m = np.arange(32)
    phase = 2.0 * np.pi * ((m[:, None] * m[None, :]) % 32) / 32.0
    cas = np.cos(phase) + np.sin(phase)
    first = split_table(np.repeat(cas[:, 0:16], 16, axis=1))
    second = split_table(np.tile(cas[:, 0:16], (1, 8)) / 32.0)
    f = np.arange(17)
    weight = np.where((f == 0) | (f == 16), 1.0, 2.0)
    cos = weight[:, None] * np.cos(2.0 * np.pi * ((f[:, None] * m[None, :]) % 32) / 32.0)
    outer = np.zeros((24, 2 * SPAN), np.float32)
    outer[0:17] = np.repeat(cos, 16, axis=1)
    inner = np.concatenate(
        [np.tile(cos[:, h : h + 16], (17, LANES // 16)) for h in (0, 16)], axis=1
    ).astype(np.float32)
    return first, second, outer, inner


def iota(shape, axis):
    return lax.broadcasted_iota(jnp.int32, shape, axis)


def block_sum(x):
    x = x + pltpu.roll(x, 32, 1)
    return x + pltpu.roll(x, 64, 1)


def keep_block(x, wanted):
    return jnp.where(iota(x.shape, 1) >> 5 == wanted, x, 0.0)


def spread_vectors(vec_ref, wide):
    rows = [
        vec_ref[k : k + 1, v * LANES : (v + 1) * LANES].astype(f32)
        for k in range(2)
        for v in range(4)
    ]
    x8 = jnp.concatenate(rows, axis=0)
    for c in range(4):
        wide[pl.ds(c, 8, stride=4), :] = x8
    x = wide[...]
    return block_sum(keep_block(x, iota(x.shape, 0) & 3))


def energy_column(energy_ref):
    first = jnp.broadcast_to(energy_ref[0:1, :], (NB, NB))
    second = jnp.broadcast_to(energy_ref[1:2, :], (NB, NB))
    e = jnp.concatenate([first, second], axis=0)
    return jnp.sum(
        jnp.where(iota(e.shape, 1) == (iota(e.shape, 0) & (NB - 1)), e, 0.0), axis=1, keepdims=True
    )


def exchange_rows(pe_ref):
    return jnp.concatenate(
        [pe_ref[k, :, g * HALF : (g + 1) * HALF] for g in range(2) for k in range(2)], axis=0
    )


def dot_t(x, y):
    return lax.dot_general(x, y, (((0,), (0,)), ((), ())), preferred_element_type=f32)


def dot_nt(x, y):
    return lax.dot_general(x, y, (((1,), (1,)), ((), ())), preferred_element_type=f32)


def spectrum(lane_at, tiles, outer, inner):
    own = iota((NQ, LANES), 1) == lane_at
    pick = jnp.where(iota((24, NQ), 0) == iota((24, NQ), 1) // 17, 1.0, 0.0).astype(bf16)
    parts = []
    for g in range(2):
        column = jnp.sum(jnp.where(own, tiles[g], 0.0), axis=1, keepdims=True)
        exact = column * inner[...]
        hi = exact.astype(bf16)
        lo = (exact - hi.astype(f32)).astype(bf16)
        parts.append(
            jnp.dot(pick, hi, preferred_element_type=f32)
            + jnp.dot(pick, lo, preferred_element_type=f32)
        )
    out = []
    for q in range(4):
        for g in range(2):
            part = parts[g][:, (q % 2) * LANES : (q % 2 + 1) * LANES]
            line = []
            for j in range(SPAN // LANES):
                at = (q // 2) * SPAN + j * LANES
                line.append(
                    jnp.sum(outer[:, at : at + LANES] * part, axis=0, keepdims=True)
                )
            out.append(jnp.concatenate(line, axis=1))
    return out


def pack_kernel(*refs):
    far, (msg, pairs, gram), kept = refs[:12], refs[12:15], refs[15:21]
    coords, cond, val, vec, pe, energy, wide, rows, lines, sem = refs[21:]
    inner, outer, bare, first, second, tiles = kept
    mine = lax.axis_index(B) * NA + lax.axis_index(A)
    tile = pl.multiple_of((mine // LANES) * LANES, LANES)
    near = (coords, cond, val, vec, pe, energy, inner, outer, bare, first, second)
    pairs_of = list(zip(far[:6] + far[7:], near))
    pairs_of += [(far[6].at[:, pl.ds(tile + g * HALF, LANES)], tiles.at[g]) for g in range(2)]
    copies = [
        pltpu.make_async_copy(src, dst, sem.at[i]) for i, (src, dst) in enumerate(pairs_of)
    ]
    for copy in copies:
        copy.start()
    for copy in copies[:6]:
        copy.wait()
    x = spread_vectors(vec, wide)
    for k in range(2):
        cf = cond[k].astype(f32)
        vf = val[k].astype(f32)
        for v in range(4):
            both = vf[v : v + 1, :] * cf
            for g in range(2):
                at = k * 32 + g * 16 + v * 4
                rows[at : at + 4, :] = both[:, g * HALF : (g + 1) * HALF]
    left = rows[...].astype(bf16)
    pairs[...] = left
    xp = jnp.concatenate([x[0:16], x[0:16], x[16:32], x[16:32]], axis=0)
    xp = keep_block(xp, iota(xp.shape, 0) >> 4).astype(bf16)
    xd = jnp.concatenate([x, x], axis=0)
    xd = keep_block(xd, iota(xd.shape, 0) >> 5).astype(bf16)
    lane = iota((1, LANES), 1)
    place = jnp.zeros((1, LANES), f32)
    for k in range(2):
        for s in range(2):
            place = jnp.where(lane == 64 + 2 * k + s, coords[k : k + 1, s : s + 1].astype(f32), place)
    lines[pl.ds(0, ND, stride=2), :] = dot_t(left, xp)
    lines[pl.ds(1, ND, stride=2), :] = dot_t(exchange_rows(pe), xd) + place
    msg[...] = lines[...].astype(bf16)
    gram[...] = lax.dot_general(
        x[:, 0:32],
        energy_column(energy) * x,
        (((0,), (0,)), ((), ())),
        precision=HIGH,
        preferred_element_type=f32,
    )
    for copy in copies[6:]:
        copy.wait()


def fold(alpha):
    n = iota((16, LANES), 1) & 31
    row = iota((16, LANES), 0)
    last = pltpu.roll(alpha[16:32], LANES - 16, 1)
    half = jnp.where((row > n) & (n < 16), last, alpha[0:16])
    corner = jnp.where(iota((16, LANES), 1) == row + 64, last, 0.0)
    return half, jnp.sum(corner, axis=0, keepdims=True)


def unfold(half, corner):
    lane = iota((16, LANES), 1)
    row = iota((16, LANES), 0)
    half = jnp.where(lane < 32, half, 0.0)
    turned = jnp.transpose(jnp.concatenate([half, jnp.zeros((LANES - 16, LANES), f32)], axis=0))
    upper = jnp.where((lane < 16) & (row > lane), turned[0:16], half)
    last = jnp.where(row > lane - 16, pltpu.roll(half, 16, 1), pltpu.roll(turned[0:16], 16, 1))
    last = jnp.where(row == lane - 16, corner, last)
    lower = jnp.where(lane < 16, turned[16:32], jnp.where(lane < 32, last, 0.0))
    return block_sum(jnp.concatenate([upper, lower], axis=0))


def spectral_kernel(
    got, gram, inner, outer_table, bare, first, second, tiles, msg, lines, wide
):
    mine = lax.axis_index(B) * NA + lax.axis_index(A)
    lam = spectrum(mine % LANES, tiles, outer_table, inner)
    index = iota((8, LANES), 0) * LANES + iota((8, LANES), 1)
    factors = [
        jnp.sum(jnp.where(index == mine + g * HALF, bare[...], 0.0), keepdims=True)
        for g in range(2)
    ]
    lines[0 : 2 * ND, :] = got[...].astype(f32)
    proj = jnp.transpose(lines[pl.ds(0, ND, stride=2), :])
    rest = lines[pl.ds(1, ND, stride=2), :]
    turned = jnp.transpose(rest)
    slot = iota((ND, 64), 1) & 31
    left = iota((ND, LANES), 1) < 64
    basis, sign = [], []
    hat = None
    for k in range(2):
        at = [
            jnp.broadcast_to(rest[:, 64 + 2 * k + s : 65 + 2 * k + s], (ND, LANES)).astype(jnp.int32)
            for s in range(2)
        ]
        ones = [jnp.where(slot == p[:, 0:64], 1.0, 0.0).astype(bf16) for p in at]
        ta = jnp.dot(ones[0], first[...], preferred_element_type=f32)
        tb = jnp.dot(ones[1], second[...], preferred_element_type=f32)
        exact = ta * jnp.concatenate([tb] * (SPAN // LANES), axis=1)
        hi = exact.astype(bf16)
        lo = (exact - hi.astype(f32)).astype(bf16)
        basis.append((hi, lo))
        sa, sb = [jnp.where((p & 1) == 0, 1.0, -1.0) for p in at]
        sign.append((sb, sa, sa * sb))
        at = [turned[64 + 2 * k + s : 65 + 2 * k + s].astype(jnp.int32) for s in range(2)]
        sa, sb = [jnp.where((p & 1) == 0, 1.0, -1.0) for p in at]
        own = proj[k * 64 : (k + 1) * 64]
        own = jnp.concatenate([own, own * sb, own * sa, own * (sa * sb)], axis=0).astype(bf16)
        part = jnp.dot(own, hi, preferred_element_type=f32) + jnp.dot(
            own, lo, preferred_element_type=f32
        )
        hat = part if hat is None else hat + part
    scale = jnp.concatenate(
        [jnp.broadcast_to(line, (32, SPAN)) for line in lam], axis=0
    )
    exact = hat * scale
    scaled = exact.astype(bf16)
    finer = (exact - scaled.astype(f32)).astype(bf16)
    hat = hat.astype(bf16)
    both = jnp.concatenate(
        [v[q * 64 : (q + 1) * 64] for q in range(4) for v in (scaled, finer)], axis=0
    )
    back = []
    for k in range(2):
        sb, sa, sab = sign[k]
        wide_r = dot_nt(basis[k][0], both)
        r = wide_r[:, 0:LANES] + sb * wide_r[:, LANES : 2 * LANES]
        r = r + sa * wide_r[:, 2 * LANES : 3 * LANES] + sab * wide_r[:, 3 * LANES : 4 * LANES]
        small = dot_nt(basis[k][1], scaled)
        r = r + jnp.where(left, 1.0, sb) * small[:, 0:LANES]
        r = r + jnp.where(left, sa, sab) * small[:, LANES : 2 * LANES]
        back.append(r + pltpu.roll(r, 64, 1))
    back = jnp.where(left, back[0], back[1])
    direct = None
    for g in range(2):
        x, y = [
            jnp.concatenate(
                [v[q * 64 + g * 32 : q * 64 + g * 32 + 32] for q in range(4)], axis=1
            )
            for v in (hat, scaled)
        ]
        part = dot_nt(x, jnp.concatenate([y] * 4, axis=0))
        direct = part if direct is None else direct + part
    for b in range(NBB):
        lines[pl.ds(b, NA, stride=ROWS), :] = back[b * NA : (b + 1) * NA]
    lane = iota((1, LANES), 1)
    dens = jnp.sum(rest, axis=0, keepdims=True)
    outer = jnp.zeros((32, LANES), f32)
    cd = jnp.zeros((1, LANES), f32)
    for g in range(2):
        factor = factors[g]
        own = jnp.where(lane >> 5 == g, dens, 0.0)
        row = block_sum(own)
        column = jnp.sum(
            jnp.where(iota((32, LANES), 0) == iota((32, LANES), 1), row, 0.0), axis=1, keepdims=True
        )
        outer = outer + column * (factor * row)
        cd = cd + factor * own
    alpha = (gram[...] + (2.0 / NT) * outer - direct / NK) / NT
    half, corner = fold(alpha)
    wide[0:16, :] = keep_block(half, iota((16, LANES), 0) & 3)
    packed = wide[pl.ds(0, 4, stride=4), :]
    for c in range(1, 4):
        packed = packed + wide[pl.ds(c, 4, stride=4), :]
    tail = jnp.concatenate([packed, cd + corner, jnp.zeros((1, LANES), f32)], axis=0)
    for r in range(ROWS - NBB):
        lines[pl.ds(NBB + r, NA, stride=ROWS), :] = jnp.broadcast_to(tail[r : r + 1], (NA, LANES))
    msg[...] = lines[0 : NA * ROWS, :].astype(bf16)


def relay_kernel(got, msg, lines):
    lines[...] = got[...].astype(f32)
    alpha = []
    for r in range(4):
        part = lines[pl.ds(NBB + r, NA, stride=ROWS), :]
        alpha.append(jnp.sum(part, axis=0, keepdims=True))
    alpha = jnp.concatenate(alpha, axis=0)
    cd = lines[pl.ds(NBB + 4, NA, stride=ROWS), :]
    corner = jnp.sum(cd, axis=0, keepdims=True)
    cd = jnp.where(iota(cd.shape, 1) < 64, cd, 0.0)
    cd = cd[0 : NA // 2] + pltpu.roll(cd[NA // 2 :], 64, 1)
    hi = alpha.astype(bf16).astype(f32)
    lane = iota((4, LANES), 1)
    first = iota((4, LANES), 0) == 0
    rough = corner.astype(bf16).astype(f32)
    lo = jnp.where((lane & 31) < 16, alpha - hi, 0.0)
    lo = jnp.where(first & (lane >> 4 == 1), pltpu.roll(rough, LANES - 48, 1), lo)
    lo = jnp.where(first & (lane >> 4 == 3), pltpu.roll(corner - rough, LANES - 16, 1), lo)
    tail = jnp.concatenate([cd, hi, lo], axis=0).astype(bf16)
    for b in range(NBB):
        msg[b, 0:NA, :] = lines[pl.ds(b, NA, stride=ROWS), :].astype(bf16)
        msg[b, NA:WIDE, :] = tail


def finish_kernel(got, pairs, pe, vec, energy, out, alpha_out, wide, rows):
    x = spread_vectors(vec, wide)
    potential = got[:, 0:NA, :].reshape(ND, LANES)
    field = []
    for b in range(NBB):
        part = got[b, NA:FIELD, :].astype(f32)
        field += [part, pltpu.roll(part, 64, 1)]
    field = jnp.concatenate(field, axis=0).astype(bf16)
    direct = jnp.dot(pairs[...], potential, preferred_element_type=f32)
    direct = block_sum(keep_block(direct, iota(direct.shape, 0) >> 4))
    direct = jnp.concatenate([direct[0:16] + direct[16:32], direct[32:48] + direct[48:64]], axis=0)
    exchange = jnp.dot(exchange_rows(pe), field, preferred_element_type=f32)
    exchange = block_sum(keep_block(exchange, iota(exchange.shape, 0) >> 5))
    exchange = exchange[0:32] + exchange[32:64]
    applied = energy_column(energy) * x + (2.0 / NT) * exchange - direct / NK
    alpha = jnp.zeros((8, LANES), f32)
    for b in range(NBB):
        alpha = alpha + got[b, FIELD:WIDE, :].astype(f32)
    corner = alpha[4:5] + pltpu.roll(alpha[4:5], LANES - 32, 1)
    half = alpha[0:4] + jnp.where((iota((4, LANES), 1) & 31) < 16, alpha[4:8], 0.0)
    for c in range(4):
        wide[pl.ds(c, 4, stride=4), :] = half
    full = wide[0:16, :]
    full = unfold(block_sum(keep_block(full, iota(full.shape, 0) & 3)), corner)
    alpha_out[...] = full[:, 0:32]
    shift = jnp.dot(x[:, 0:32], full, precision=HIGH, preferred_element_type=f32)
    rows[...] = keep_block(applied - shift, iota((32, LANES), 0) & 3)
    packed = rows[pl.ds(0, 8, stride=4), :]
    for c in range(1, 4):
        packed = packed + rows[pl.ds(c, 8, stride=4), :]
    for k in range(2):
        for v in range(4):
            out[k : k + 1, v * LANES : (v + 1) * LANES] = packed[k * 4 + v : k * 4 + v + 1, :]


def vmem():
    return pl.BlockSpec(memory_space=pltpu.VMEM)


def room(mib):
    return pltpu.CompilerParams(vmem_limit_bytes=mib << 20)


def in_hbm(x):
    return pltpu.with_memory_space_constraint(jnp.asarray(x), pltpu.HBM)


def sds(shape, dtype):
    return jax.ShapeDtypeStruct(shape, dtype)


def on_device(pair_exchange, conduction, valence, coulomb, screening, energies, vectors, k_coords):
    first, second, outer, inner = tables()
    far = (k_coords, conduction, valence, vectors, pair_exchange, energies, screening)
    far += (inner, outer, coulomb.reshape(8, LANES), first, second)
    any_space = pl.BlockSpec(memory_space=pl.ANY)
    own = [pltpu.VMEM(v.shape, v.dtype) for v in far[:6]]
    msg, pairs, gram, *kept = pl.pallas_call(
        pack_kernel,
        out_shape=(
            sds((2 * ND, LANES), bf16),
            sds((64, HALF), bf16),
            sds((32, LANES), f32),
            sds((NQ, 2 * LANES), f32),
            sds((24, 2 * SPAN), f32),
            sds((8, LANES), f32),
            sds((64, SPAN), bf16),
            sds((64, LANES), bf16),
            sds((2, NQ, LANES), f32),
        ),
        in_specs=[any_space] * len(far),
        out_specs=(vmem(),) * 9,
        scratch_shapes=own
        + [
            pltpu.VMEM((32, LANES), f32),
            pltpu.VMEM((64, HALF), f32),
            pltpu.VMEM((2 * ND, LANES), f32),
            pltpu.SemaphoreType.DMA((13,)),
        ],
        compiler_params=room(12),
        name="pack",
    )(*[in_hbm(v) for v in far])
    got = lax.all_to_all(msg.reshape(ND, 2, LANES), B + A, 0, 0, tiled=True)
    out = pl.pallas_call(
        spectral_kernel,
        out_shape=sds((NA * ROWS, LANES), bf16),
        in_specs=[vmem()] * 8,
        out_specs=vmem(),
        scratch_shapes=[
            pltpu.VMEM((max(2 * ND, NA * ROWS), LANES), f32),
            pltpu.VMEM((32, LANES), f32),
        ],
        compiler_params=room(28),
        name="spectral",
    )(got.reshape(2 * ND, LANES), gram, *kept)
    got = lax.all_to_all(out.reshape(NA, ROWS // 2, 2, LANES), A, 0, 0, tiled=True)
    out = pl.pallas_call(
        relay_kernel,
        out_shape=sds((NBB, WIDE, LANES), bf16),
        in_specs=[vmem()],
        out_specs=vmem(),
        scratch_shapes=[pltpu.VMEM((NA * ROWS, LANES), f32)],
        compiler_params=room(8),
        name="relay",
    )(got.reshape(NA * ROWS, LANES))
    got = lax.all_to_all(out, B, 0, 0, tiled=True)
    return pl.pallas_call(
        finish_kernel,
        out_shape=(sds((2, NB * NV), f32), sds((NV, NV), f32)),
        in_specs=[vmem()] * 5,
        out_specs=(vmem(), vmem()),
        scratch_shapes=[pltpu.VMEM((32, LANES), f32), pltpu.VMEM((32, LANES), f32)],
        compiler_params=room(8),
        name="finish",
    )(got, pairs, pair_exchange, vectors, energies)


def solution(mesh):
    split = Mesh(mesh.devices.reshape(SIZES), NAMES)
    return jax.shard_map(
        on_device,
        mesh=split,
        in_specs=(
            P(NAMES, None, None),
            P(NAMES, None, None),
            P(NAMES, None, None),
            P(),
            P(),
            P(NAMES, None),
            P(NAMES, None),
            P(NAMES, None),
        ),
        out_specs=(P(NAMES, None), P()),
        check_vma=False,
    )
```

```python
import jax
import jax.numpy as jnp
import numpy as np
from jax import lax
from jax.experimental import pallas as pl
from jax.experimental.pallas import tpu as pltpu
from jax.sharding import Mesh
from jax.sharding import PartitionSpec as P

MX = 32
MY = 32
NK = 1024
NB = 16
NG = 1024
NV = 32
NT = NK * NB
NQ = 289
SPAN = NK // 4
NAMES = ("zh", "zl", "yl", "c", "x", "yh")
SIZES = (4, 2, 2, 2, 4, 4)
A = ("zh", "zl", "yh")
B = ("c", "x", "yl")
NA = 32
NBB = 16
ND = NA * NBB
HALF = NG // 2
ROWS = NBB + 6
FIELD = NA + NA // 2
WIDE = FIELD + 8
LANES = 128

f32 = jnp.float32
bf16 = jnp.bfloat16


def split_table(x):
    hi = x.astype(bf16)
    lo = (x - hi.astype(np.float64)).astype(bf16)
    return np.concatenate([hi, lo], axis=0)


def tables():
    m = np.arange(32)
    phase = 2.0 * np.pi * ((m[:, None] * m[None, :]) % 32) / 32.0
    cas = np.cos(phase) + np.sin(phase)
    first = split_table(np.repeat(cas[:, 0:16], 16, axis=1))
    second = split_table(np.tile(cas[:, 0:16], (1, 8)) / 32.0)
    f = np.arange(17)
    weight = np.where((f == 0) | (f == 16), 1.0, 2.0)
    cos = weight[:, None] * np.cos(2.0 * np.pi * ((f[:, None] * m[None, :]) % 32) / 32.0)
    outer = np.zeros((24, 2 * SPAN), np.float32)
    outer[0:17] = np.repeat(cos, 16, axis=1)
    inner = np.concatenate(
        [np.tile(cos[:, h : h + 16], (17, LANES // 16)) for h in (0, 16)], axis=1
    ).astype(np.float32)
    return first, second, outer, inner


def iota(shape, axis):
    return lax.broadcasted_iota(jnp.int32, shape, axis)


def block_sum(x):
    x = x + pltpu.roll(x, 32, 1)
    return x + pltpu.roll(x, 64, 1)


def keep_block(x, wanted):
    return jnp.where(iota(x.shape, 1) >> 5 == wanted, x, 0.0)


def spread_vectors(vec_ref, wide):
    rows = [
        vec_ref[k : k + 1, v * LANES : (v + 1) * LANES].astype(f32)
        for k in range(2)
        for v in range(4)
    ]
    x8 = jnp.concatenate(rows, axis=0)
    for c in range(4):
        wide[pl.ds(c, 8, stride=4), :] = x8
    x = wide[...]
    return block_sum(keep_block(x, iota(x.shape, 0) & 3))


def energy_column(energy_ref):
    first = jnp.broadcast_to(energy_ref[0:1, :], (NB, NB))
    second = jnp.broadcast_to(energy_ref[1:2, :], (NB, NB))
    e = jnp.concatenate([first, second], axis=0)
    return jnp.sum(
        jnp.where(iota(e.shape, 1) == (iota(e.shape, 0) & (NB - 1)), e, 0.0), axis=1, keepdims=True
    )


def exchange_rows(pe_ref):
    return jnp.concatenate(
        [pe_ref[k, :, g * HALF : (g + 1) * HALF] for g in range(2) for k in range(2)], axis=0
    )


def halves(x):
    hi = x.astype(bf16)
    return hi, (x - hi.astype(f32)).astype(bf16)


def dot_t(x, y):
    return lax.dot_general(x, y, (((0,), (0,)), ((), ())), preferred_element_type=f32)


def dot_nt(x, y):
    return lax.dot_general(x, y, (((1,), (1,)), ((), ())), preferred_element_type=f32)


def spectrum(lane_at, tiles, outer, inner):
    own = iota((NQ, LANES), 1) == lane_at
    pick = jnp.where(iota((24, NQ), 0) == iota((24, NQ), 1) // 17, 1.0, 0.0).astype(bf16)
    parts = []
    for g in range(2):
        column = jnp.sum(jnp.where(own, tiles[g], 0.0), axis=1, keepdims=True)
        exact = column * inner[...]
        hi = exact.astype(bf16)
        lo = (exact - hi.astype(f32)).astype(bf16)
        parts.append(
            jnp.dot(pick, hi, preferred_element_type=f32)
            + jnp.dot(pick, lo, preferred_element_type=f32)
        )
    out = []
    for q in range(4):
        for g in range(2):
            part = parts[g][:, (q % 2) * LANES : (q % 2 + 1) * LANES]
            line = []
            for j in range(SPAN // LANES):
                at = (q // 2) * SPAN + j * LANES
                line.append(
                    jnp.sum(outer[:, at : at + LANES] * part, axis=0, keepdims=True)
                )
            out.append(jnp.concatenate(line, axis=1))
    return out


def pack_kernel(*refs):
    far, (msg, pairs, gram), kept = refs[:12], refs[12:15], refs[15:21]
    coords, cond, val, vec, pe, energy, wide, rows, lines, sem = refs[21:]
    inner, outer, bare, first, second, tiles = kept
    mine = lax.axis_index(B) * NA + lax.axis_index(A)
    tile = pl.multiple_of((mine // LANES) * LANES, LANES)
    near = (coords, cond, val, vec, pe, energy, inner, outer, bare, first, second)
    pairs_of = list(zip(far[:6] + far[7:], near))
    pairs_of += [(far[6].at[:, pl.ds(tile + g * HALF, LANES)], tiles.at[g]) for g in range(2)]
    copies = [
        pltpu.make_async_copy(src, dst, sem.at[i]) for i, (src, dst) in enumerate(pairs_of)
    ]
    for copy in copies:
        copy.start()
    for copy in copies[:6]:
        copy.wait()
    x = spread_vectors(vec, wide)
    for k in range(2):
        cf = cond[k].astype(f32)
        vf = val[k].astype(f32)
        for v in range(4):
            both = vf[v : v + 1, :] * cf
            for g in range(2):
                at = k * 32 + g * 16 + v * 4
                rows[at : at + 4, :] = both[:, g * HALF : (g + 1) * HALF]
    left = rows[...].astype(bf16)
    pairs[...] = left
    xp = jnp.concatenate([x[0:16], x[0:16], x[16:32], x[16:32]], axis=0)
    xp = keep_block(xp, iota(xp.shape, 0) >> 4).astype(bf16)
    xd = jnp.concatenate([x, x], axis=0)
    xd = keep_block(xd, iota(xd.shape, 0) >> 5).astype(bf16)
    lane = iota((1, LANES), 1)
    place = jnp.zeros((1, LANES), f32)
    for k in range(2):
        for s in range(2):
            place = jnp.where(lane == 64 + 2 * k + s, coords[k : k + 1, s : s + 1].astype(f32), place)
    lines[pl.ds(0, ND, stride=2), :] = dot_t(left, xp)
    lines[pl.ds(1, ND, stride=2), :] = dot_t(exchange_rows(pe), xd) + place
    msg[...] = lines[...].astype(bf16)
    hi, lo = halves(energy_column(energy) * x)
    twice = jnp.concatenate([x, x], axis=0).astype(bf16)
    gram[...] = dot_t(twice, jnp.concatenate([hi, lo], axis=0))[0:32]
    for copy in copies[6:]:
        copy.wait()


def fold(alpha):
    n = iota((16, LANES), 1) & 31
    row = iota((16, LANES), 0)
    last = pltpu.roll(alpha[16:32], LANES - 16, 1)
    half = jnp.where((row > n) & (n < 16), last, alpha[0:16])
    corner = jnp.where(iota((16, LANES), 1) == row + 64, last, 0.0)
    return half, jnp.sum(corner, axis=0, keepdims=True)


def unfold(half, corner):
    lane = iota((16, LANES), 1)
    row = iota((16, LANES), 0)
    half = jnp.where(lane < 32, half, 0.0)
    turned = jnp.transpose(jnp.concatenate([half, jnp.zeros((LANES - 16, LANES), f32)], axis=0))
    upper = jnp.where((lane < 16) & (row > lane), turned[0:16], half)
    last = jnp.where(row > lane - 16, pltpu.roll(half, 16, 1), pltpu.roll(turned[0:16], 16, 1))
    last = jnp.where(row == lane - 16, corner, last)
    lower = jnp.where(lane < 16, turned[16:32], jnp.where(lane < 32, last, 0.0))
    return block_sum(jnp.concatenate([upper, lower], axis=0))


def spectral_kernel(
    got, gram, inner, outer_table, bare, first, second, tiles, msg, lines, wide
):
    mine = lax.axis_index(B) * NA + lax.axis_index(A)
    lam = spectrum(mine % LANES, tiles, outer_table, inner)
    index = iota((8, LANES), 0) * LANES + iota((8, LANES), 1)
    factors = [
        jnp.sum(jnp.where(index == mine + g * HALF, bare[...], 0.0), keepdims=True)
        for g in range(2)
    ]
    lines[0 : 2 * ND, :] = got[...].astype(f32)
    proj = jnp.transpose(lines[pl.ds(0, ND, stride=2), :])
    rest = lines[pl.ds(1, ND, stride=2), :]
    turned = jnp.transpose(rest)
    slot = iota((ND, 64), 1) & 31
    left = iota((ND, LANES), 1) < 64
    basis, sign = [], []
    hat = None
    for k in range(2):
        at = [
            jnp.broadcast_to(rest[:, 64 + 2 * k + s : 65 + 2 * k + s], (ND, LANES)).astype(jnp.int32)
            for s in range(2)
        ]
        ones = [jnp.where(slot == p[:, 0:64], 1.0, 0.0).astype(bf16) for p in at]
        ta = jnp.dot(ones[0], first[...], preferred_element_type=f32)
        tb = jnp.dot(ones[1], second[...], preferred_element_type=f32)
        exact = ta * jnp.concatenate([tb] * (SPAN // LANES), axis=1)
        hi = exact.astype(bf16)
        lo = (exact - hi.astype(f32)).astype(bf16)
        basis.append((hi, lo))
        sa, sb = [jnp.where((p & 1) == 0, 1.0, -1.0) for p in at]
        sign.append((sb, sa, sa * sb))
        at = [turned[64 + 2 * k + s : 65 + 2 * k + s].astype(jnp.int32) for s in range(2)]
        sa, sb = [jnp.where((p & 1) == 0, 1.0, -1.0) for p in at]
        own = proj[k * 64 : (k + 1) * 64]
        own = jnp.concatenate([own, own * sb, own * sa, own * (sa * sb)], axis=0).astype(bf16)
        part = jnp.dot(own, hi, preferred_element_type=f32) + jnp.dot(
            own, lo, preferred_element_type=f32
        )
        hat = part if hat is None else hat + part
    scale = jnp.concatenate(
        [jnp.broadcast_to(line, (32, SPAN)) for line in lam], axis=0
    )
    exact = hat * scale
    scaled = exact.astype(bf16)
    finer = (exact - scaled.astype(f32)).astype(bf16)
    hat = hat.astype(bf16)
    both = jnp.concatenate(
        [v[q * 64 : (q + 1) * 64] for q in range(4) for v in (scaled, finer)], axis=0
    )
    back = []
    for k in range(2):
        sb, sa, sab = sign[k]
        wide_r = dot_nt(basis[k][0], both)
        r = wide_r[:, 0:LANES] + sb * wide_r[:, LANES : 2 * LANES]
        r = r + sa * wide_r[:, 2 * LANES : 3 * LANES] + sab * wide_r[:, 3 * LANES : 4 * LANES]
        small = dot_nt(basis[k][1], scaled)
        r = r + jnp.where(left, 1.0, sb) * small[:, 0:LANES]
        r = r + jnp.where(left, sa, sab) * small[:, LANES : 2 * LANES]
        back.append(r + pltpu.roll(r, 64, 1))
    back = jnp.where(left, back[0], back[1])
    direct = None
    for g in range(2):
        x, y = [
            jnp.concatenate(
                [v[q * 64 + g * 32 : q * 64 + g * 32 + 32] for q in range(4)], axis=1
            )
            for v in (hat, scaled)
        ]
        part = dot_nt(x, jnp.concatenate([y] * 4, axis=0))
        direct = part if direct is None else direct + part
    for b in range(NBB):
        lines[pl.ds(b, NA, stride=ROWS), :] = back[b * NA : (b + 1) * NA]
    lane = iota((1, LANES), 1)
    dens = jnp.sum(rest, axis=0, keepdims=True)
    outer = jnp.zeros((32, LANES), f32)
    cd = jnp.zeros((1, LANES), f32)
    for g in range(2):
        factor = factors[g]
        own = jnp.where(lane >> 5 == g, dens, 0.0)
        row = block_sum(own)
        column = jnp.sum(
            jnp.where(iota((32, LANES), 0) == iota((32, LANES), 1), row, 0.0), axis=1, keepdims=True
        )
        outer = outer + column * (factor * row)
        cd = cd + factor * own
    alpha = (gram[...] + (2.0 / NT) * outer - direct / NK) / NT
    half, corner = fold(alpha)
    wide[0:16, :] = keep_block(half, iota((16, LANES), 0) & 3)
    packed = wide[pl.ds(0, 4, stride=4), :]
    for c in range(1, 4):
        packed = packed + wide[pl.ds(c, 4, stride=4), :]
    tail = jnp.concatenate([packed, cd + corner, jnp.zeros((1, LANES), f32)], axis=0)
    for r in range(ROWS - NBB):
        lines[pl.ds(NBB + r, NA, stride=ROWS), :] = jnp.broadcast_to(tail[r : r + 1], (NA, LANES))
    msg[...] = lines[0 : NA * ROWS, :].astype(bf16)


def relay_kernel(got, msg, lines):
    lines[...] = got[...].astype(f32)
    alpha = []
    for r in range(4):
        part = lines[pl.ds(NBB + r, NA, stride=ROWS), :]
        alpha.append(jnp.sum(part, axis=0, keepdims=True))
    alpha = jnp.concatenate(alpha, axis=0)
    cd = lines[pl.ds(NBB + 4, NA, stride=ROWS), :]
    corner = jnp.sum(cd, axis=0, keepdims=True)
    cd = jnp.where(iota(cd.shape, 1) < 64, cd, 0.0)
    cd = cd[0 : NA // 2] + pltpu.roll(cd[NA // 2 :], 64, 1)
    hi = alpha.astype(bf16).astype(f32)
    lane = iota((4, LANES), 1)
    first = iota((4, LANES), 0) == 0
    rough = corner.astype(bf16).astype(f32)
    lo = jnp.where((lane & 31) < 16, alpha - hi, 0.0)
    lo = jnp.where(first & (lane >> 4 == 1), pltpu.roll(rough, LANES - 48, 1), lo)
    lo = jnp.where(first & (lane >> 4 == 3), pltpu.roll(corner - rough, LANES - 16, 1), lo)
    tail = jnp.concatenate([cd, hi, lo], axis=0).astype(bf16)
    for b in range(NBB):
        msg[b, 0:NA, :] = lines[pl.ds(b, NA, stride=ROWS), :].astype(bf16)
        msg[b, NA:WIDE, :] = tail


def finish_kernel(got, pairs, pe, vec, energy, out, alpha_out, wide, rows):
    x = spread_vectors(vec, wide)
    potential = got[:, 0:NA, :].reshape(ND, LANES)
    field = []
    for b in range(NBB):
        part = got[b, NA:FIELD, :].astype(f32)
        field += [part, pltpu.roll(part, 64, 1)]
    field = jnp.concatenate(field, axis=0).astype(bf16)
    direct = jnp.dot(pairs[...], potential, preferred_element_type=f32)
    direct = block_sum(keep_block(direct, iota(direct.shape, 0) >> 4))
    direct = jnp.concatenate([direct[0:16] + direct[16:32], direct[32:48] + direct[48:64]], axis=0)
    exchange = jnp.dot(exchange_rows(pe), field, preferred_element_type=f32)
    exchange = block_sum(keep_block(exchange, iota(exchange.shape, 0) >> 5))
    exchange = exchange[0:32] + exchange[32:64]
    applied = energy_column(energy) * x + (2.0 / NT) * exchange - direct / NK
    alpha = jnp.zeros((8, LANES), f32)
    for b in range(NBB):
        alpha = alpha + got[b, FIELD:WIDE, :].astype(f32)
    corner = alpha[4:5] + pltpu.roll(alpha[4:5], LANES - 32, 1)
    half = alpha[0:4] + jnp.where((iota((4, LANES), 1) & 31) < 16, alpha[4:8], 0.0)
    for c in range(4):
        wide[pl.ds(c, 4, stride=4), :] = half
    full = wide[0:16, :]
    full = unfold(block_sum(keep_block(full, iota(full.shape, 0) & 3)), corner)
    alpha_out[...] = full[:, 0:32]
    none = jnp.zeros((64, LANES), bf16)
    shift = jnp.dot(
        x.astype(bf16),
        jnp.concatenate([*halves(full), none], axis=0),
        preferred_element_type=f32,
    )
    rows[...] = keep_block(applied - shift, iota((32, LANES), 0) & 3)
    packed = rows[pl.ds(0, 8, stride=4), :]
    for c in range(1, 4):
        packed = packed + rows[pl.ds(c, 8, stride=4), :]
    for k in range(2):
        for v in range(4):
            out[k : k + 1, v * LANES : (v + 1) * LANES] = packed[k * 4 + v : k * 4 + v + 1, :]


def vmem():
    return pl.BlockSpec(memory_space=pltpu.VMEM)


def room(mib):
    return pltpu.CompilerParams(vmem_limit_bytes=mib << 20)


def in_hbm(x):
    return pltpu.with_memory_space_constraint(jnp.asarray(x), pltpu.HBM)


def sds(shape, dtype):
    return jax.ShapeDtypeStruct(shape, dtype)


def on_device(pair_exchange, conduction, valence, coulomb, screening, energies, vectors, k_coords):
    first, second, outer, inner = tables()
    far = (k_coords, conduction, valence, vectors, pair_exchange, energies, screening)
    far += (inner, outer, coulomb.reshape(8, LANES), first, second)
    any_space = pl.BlockSpec(memory_space=pl.ANY)
    own = [pltpu.VMEM(v.shape, v.dtype) for v in far[:6]]
    msg, pairs, gram, *kept = pl.pallas_call(
        pack_kernel,
        out_shape=(
            sds((2 * ND, LANES), bf16),
            sds((64, HALF), bf16),
            sds((32, LANES), f32),
            sds((NQ, 2 * LANES), f32),
            sds((24, 2 * SPAN), f32),
            sds((8, LANES), f32),
            sds((64, SPAN), bf16),
            sds((64, LANES), bf16),
            sds((2, NQ, LANES), f32),
        ),
        in_specs=[any_space] * len(far),
        out_specs=(vmem(),) * 9,
        scratch_shapes=own
        + [
            pltpu.VMEM((32, LANES), f32),
            pltpu.VMEM((64, HALF), f32),
            pltpu.VMEM((2 * ND, LANES), f32),
            pltpu.SemaphoreType.DMA((13,)),
        ],
        compiler_params=room(12),
        name="pack",
    )(*[in_hbm(v) for v in far])
    got = lax.all_to_all(msg.reshape(ND, 2, LANES), B + A, 0, 0, tiled=True)
    out = pl.pallas_call(
        spectral_kernel,
        out_shape=sds((NA * ROWS, LANES), bf16),
        in_specs=[vmem()] * 8,
        out_specs=vmem(),
        scratch_shapes=[
            pltpu.VMEM((max(2 * ND, NA * ROWS), LANES), f32),
            pltpu.VMEM((32, LANES), f32),
        ],
        compiler_params=room(28),
        name="spectral",
    )(got.reshape(2 * ND, LANES), gram, *kept)
    got = lax.all_to_all(out.reshape(NA, ROWS // 2, 2, LANES), A, 0, 0, tiled=True)
    out = pl.pallas_call(
        relay_kernel,
        out_shape=sds((NBB, WIDE, LANES), bf16),
        in_specs=[vmem()],
        out_specs=vmem(),
        scratch_shapes=[pltpu.VMEM((NA * ROWS, LANES), f32)],
        compiler_params=room(8),
        name="relay",
    )(got.reshape(NA * ROWS, LANES))
    got = lax.all_to_all(out, B, 0, 0, tiled=True)
    return pl.pallas_call(
        finish_kernel,
        out_shape=(sds((2, NB * NV), f32), sds((NV, NV), f32)),
        in_specs=[vmem()] * 5,
        out_specs=(vmem(), vmem()),
        scratch_shapes=[pltpu.VMEM((32, LANES), f32), pltpu.VMEM((32, LANES), f32)],
        compiler_params=room(8),
        name="finish",
    )(got, pairs, pair_exchange, vectors, energies)


def solution(mesh):
    split = Mesh(mesh.devices.reshape(SIZES), NAMES)
    return jax.shard_map(
        on_device,
        mesh=split,
        in_specs=(
            P(NAMES, None, None),
            P(NAMES, None, None),
            P(NAMES, None, None),
            P(),
            P(),
            P(NAMES, None),
            P(NAMES, None),
            P(NAMES, None),
        ),
        out_specs=(P(NAMES, None), P()),
        check_vma=False,
    )
```

```python
import jax
import jax.numpy as jnp
import numpy as np
from jax import lax
from jax.experimental import pallas as pl
from jax.experimental.pallas import tpu as pltpu
from jax.sharding import Mesh
from jax.sharding import PartitionSpec as P

MX = 32
MY = 32
NK = 1024
NB = 16
NG = 1024
NV = 32
NT = NK * NB
NQ = 289
SPAN = NK // 4
NAMES = ("zh", "zl", "yl", "c", "x", "yh")
SIZES = (4, 2, 2, 2, 4, 4)
A = ("yh", "yl", "zh")
B = ("c", "x", "zl")
NA = 32
NBB = 16
ND = NA * NBB
HALF = NG // 2
ROWS = NBB + 6
FIELD = NA + NA // 2
WIDE = FIELD + 8
LANES = 128

f32 = jnp.float32
bf16 = jnp.bfloat16


def split_table(x):
    hi = x.astype(bf16)
    lo = (x - hi.astype(np.float64)).astype(bf16)
    return np.concatenate([hi, lo], axis=0)


def tables():
    m = np.arange(32)
    phase = 2.0 * np.pi * ((m[:, None] * m[None, :]) % 32) / 32.0
    cas = np.cos(phase) + np.sin(phase)
    first = split_table(np.repeat(cas[:, 0:16], 16, axis=1))
    second = split_table(np.tile(cas[:, 0:16], (1, 8)) / 32.0)
    f = np.arange(17)
    weight = np.where((f == 0) | (f == 16), 1.0, 2.0)
    cos = weight[:, None] * np.cos(2.0 * np.pi * ((f[:, None] * m[None, :]) % 32) / 32.0)
    outer = np.zeros((24, 2 * SPAN), np.float32)
    outer[0:17] = np.repeat(cos, 16, axis=1)
    inner = np.concatenate(
        [np.tile(cos[:, h : h + 16], (17, LANES // 16)) for h in (0, 16)], axis=1
    ).astype(np.float32)
    return first, second, outer, inner


def iota(shape, axis):
    return lax.broadcasted_iota(jnp.int32, shape, axis)


def block_sum(x):
    x = x + pltpu.roll(x, 32, 1)
    return x + pltpu.roll(x, 64, 1)


def keep_block(x, wanted):
    return jnp.where(iota(x.shape, 1) >> 5 == wanted, x, 0.0)


def spread_vectors(vec_ref, wide):
    rows = [
        vec_ref[k : k + 1, v * LANES : (v + 1) * LANES].astype(f32)
        for k in range(2)
        for v in range(4)
    ]
    x8 = jnp.concatenate(rows, axis=0)
    for c in range(4):
        wide[pl.ds(c, 8, stride=4), :] = x8
    x = wide[...]
    return block_sum(keep_block(x, iota(x.shape, 0) & 3))


def energy_column(energy_ref):
    first = jnp.broadcast_to(energy_ref[0:1, :], (NB, NB))
    second = jnp.broadcast_to(energy_ref[1:2, :], (NB, NB))
    e = jnp.concatenate([first, second], axis=0)
    return jnp.sum(
        jnp.where(iota(e.shape, 1) == (iota(e.shape, 0) & (NB - 1)), e, 0.0), axis=1, keepdims=True
    )


def exchange_rows(pe_ref):
    return jnp.concatenate(
        [pe_ref[k, :, g * HALF : (g + 1) * HALF] for g in range(2) for k in range(2)], axis=0
    )


def halves(x):
    hi = x.astype(bf16)
    return hi, (x - hi.astype(f32)).astype(bf16)


def dot_t(x, y):
    return lax.dot_general(x, y, (((0,), (0,)), ((), ())), preferred_element_type=f32)


def dot_nt(x, y):
    return lax.dot_general(x, y, (((1,), (1,)), ((), ())), preferred_element_type=f32)


def spectrum(lane_at, tiles, outer, inner):
    own = iota((NQ, LANES), 1) == lane_at
    pick = jnp.where(iota((24, NQ), 0) == iota((24, NQ), 1) // 17, 1.0, 0.0).astype(bf16)
    parts = []
    for g in range(2):
        column = jnp.sum(jnp.where(own, tiles[g], 0.0), axis=1, keepdims=True)
        exact = column * inner[...]
        hi = exact.astype(bf16)
        lo = (exact - hi.astype(f32)).astype(bf16)
        parts.append(
            jnp.dot(pick, hi, preferred_element_type=f32)
            + jnp.dot(pick, lo, preferred_element_type=f32)
        )
    out = []
    for q in range(4):
        for g in range(2):
            part = parts[g][:, (q % 2) * LANES : (q % 2 + 1) * LANES]
            line = []
            for j in range(SPAN // LANES):
                at = (q // 2) * SPAN + j * LANES
                line.append(
                    jnp.sum(outer[:, at : at + LANES] * part, axis=0, keepdims=True)
                )
            out.append(jnp.concatenate(line, axis=1))
    return out


def pack_kernel(*refs):
    far, (msg, pairs, gram), kept = refs[:12], refs[12:15], refs[15:21]
    coords, cond, val, vec, pe, energy, wide, rows, lines, sem = refs[21:]
    inner, outer, bare, first, second, tiles = kept
    mine = lax.axis_index(B) * NA + lax.axis_index(A)
    tile = pl.multiple_of((mine // LANES) * LANES, LANES)
    near = (coords, cond, val, vec, pe, energy, inner, outer, bare, first, second)
    pairs_of = list(zip(far[:6] + far[7:], near))
    pairs_of += [(far[6].at[:, pl.ds(tile + g * HALF, LANES)], tiles.at[g]) for g in range(2)]
    copies = [
        pltpu.make_async_copy(src, dst, sem.at[i]) for i, (src, dst) in enumerate(pairs_of)
    ]
    for copy in copies:
        copy.start()
    for copy in copies[:6]:
        copy.wait()
    x = spread_vectors(vec, wide)
    for k in range(2):
        cf = cond[k].astype(f32)
        vf = val[k].astype(f32)
        for v in range(4):
            both = vf[v : v + 1, :] * cf
            for g in range(2):
                at = k * 32 + g * 16 + v * 4
                rows[at : at + 4, :] = both[:, g * HALF : (g + 1) * HALF]
    left = rows[...].astype(bf16)
    pairs[...] = left
    xp = jnp.concatenate([x[0:16], x[0:16], x[16:32], x[16:32]], axis=0)
    xp = keep_block(xp, iota(xp.shape, 0) >> 4).astype(bf16)
    xd = jnp.concatenate([x, x], axis=0)
    xd = keep_block(xd, iota(xd.shape, 0) >> 5).astype(bf16)
    lane = iota((1, LANES), 1)
    place = jnp.zeros((1, LANES), f32)
    for k in range(2):
        for s in range(2):
            at = coords[k : k + 1, s : s + 1]
            place = jnp.where(lane == 64 + 2 * k + s, at.astype(f32), place)
            place = jnp.where(lane == 68 + 2 * k + s, (1 - 2 * (at & 1)).astype(f32), place)
    lines[pl.ds(0, ND, stride=2), :] = dot_t(left, xp)
    lines[pl.ds(1, ND, stride=2), :] = dot_t(exchange_rows(pe), xd) + place
    msg[...] = lines[...].astype(bf16)
    hi, lo = halves(energy_column(energy) * x)
    twice = jnp.concatenate([x, x], axis=0).astype(bf16)
    gram[...] = dot_t(twice, jnp.concatenate([hi, lo], axis=0))[0:32]
    for copy in copies[6:]:
        copy.wait()


def fold(alpha):
    n = iota((16, LANES), 1) & 31
    row = iota((16, LANES), 0)
    last = pltpu.roll(alpha[16:32], LANES - 16, 1)
    half = jnp.where((row > n) & (n < 16), last, alpha[0:16])
    corner = jnp.where(iota((16, LANES), 1) == row + 64, last, 0.0)
    return half, jnp.sum(corner, axis=0, keepdims=True)


def unfold(half, corner):
    lane = iota((16, LANES), 1)
    row = iota((16, LANES), 0)
    half = jnp.where(lane < 32, half, 0.0)
    turned = jnp.transpose(jnp.concatenate([half, jnp.zeros((LANES - 16, LANES), f32)], axis=0))
    upper = jnp.where((lane < 16) & (row > lane), turned[0:16], half)
    last = jnp.where(row > lane - 16, pltpu.roll(half, 16, 1), pltpu.roll(turned[0:16], 16, 1))
    last = jnp.where(row == lane - 16, corner, last)
    lower = jnp.where(lane < 16, turned[16:32], jnp.where(lane < 32, last, 0.0))
    return block_sum(jnp.concatenate([upper, lower], axis=0))


def spectral_kernel(
    got, gram, inner, outer_table, bare, first, second, tiles, msg, lines, wide
):
    mine = lax.axis_index(B) * NA + lax.axis_index(A)
    lam = spectrum(mine % LANES, tiles, outer_table, inner)
    index = iota((8, LANES), 0) * LANES + iota((8, LANES), 1)
    factors = [
        jnp.sum(jnp.where(index == mine + g * HALF, bare[...], 0.0), keepdims=True)
        for g in range(2)
    ]
    lines[0 : 2 * ND, :] = got[...].astype(f32)
    proj = jnp.transpose(lines[pl.ds(0, ND, stride=2), :])
    rest = lines[pl.ds(1, ND, stride=2), :]
    turned = jnp.transpose(rest)
    slot = (iota((ND, 64), 1) & 31).astype(f32)
    left = iota((ND, LANES), 1) < 64
    basis, sign = [], []
    hat = None
    for k in range(2):
        ones = [
            jnp.where(slot == rest[:, 64 + 2 * k + s : 65 + 2 * k + s], 1.0, 0.0).astype(bf16)
            for s in range(2)
        ]
        ta = jnp.dot(ones[0], first[...], preferred_element_type=f32)
        tb = jnp.dot(ones[1], second[...], preferred_element_type=f32)
        exact = ta * jnp.concatenate([tb] * (SPAN // LANES), axis=1)
        hi = exact.astype(bf16)
        lo = (exact - hi.astype(f32)).astype(bf16)
        basis.append((hi, lo))
        sa, sb = [
            jnp.broadcast_to(rest[:, 68 + 2 * k + s : 69 + 2 * k + s], (ND, LANES))
            for s in range(2)
        ]
        sign.append((sb, sa, sa * sb))
        sa, sb = [turned[68 + 2 * k + s : 69 + 2 * k + s] for s in range(2)]
        own = proj[k * 64 : (k + 1) * 64]
        own = jnp.concatenate([own, own * sb, own * sa, own * (sa * sb)], axis=0).astype(bf16)
        part = jnp.dot(own, hi, preferred_element_type=f32) + jnp.dot(
            own, lo, preferred_element_type=f32
        )
        hat = part if hat is None else hat + part
    scale = jnp.concatenate(
        [jnp.broadcast_to(line, (32, SPAN)) for line in lam], axis=0
    )
    exact = hat * scale
    scaled = exact.astype(bf16)
    finer = (exact - scaled.astype(f32)).astype(bf16)
    hat = hat.astype(bf16)
    both = jnp.concatenate(
        [v[q * 64 : (q + 1) * 64] for q in range(4) for v in (scaled, finer)], axis=0
    )
    back = []
    for k in range(2):
        sb, sa, sab = sign[k]
        wide_r = dot_nt(basis[k][0], both)
        r = wide_r[:, 0:LANES] + sb * wide_r[:, LANES : 2 * LANES]
        r = r + sa * wide_r[:, 2 * LANES : 3 * LANES] + sab * wide_r[:, 3 * LANES : 4 * LANES]
        small = dot_nt(basis[k][1], scaled)
        r = r + jnp.where(left, 1.0, sb) * small[:, 0:LANES]
        r = r + jnp.where(left, sa, sab) * small[:, LANES : 2 * LANES]
        back.append(r + pltpu.roll(r, 64, 1))
    back = jnp.where(left, back[0], back[1])
    direct = None
    for g in range(2):
        x, y = [
            jnp.concatenate(
                [v[q * 64 + g * 32 : q * 64 + g * 32 + 32] for q in range(4)], axis=1
            )
            for v in (hat, scaled)
        ]
        part = dot_nt(x, jnp.concatenate([y] * 4, axis=0))
        direct = part if direct is None else direct + part
    for b in range(NBB):
        lines[pl.ds(b, NA, stride=ROWS), :] = back[b * NA : (b + 1) * NA]
    lane = iota((1, LANES), 1)
    dens = jnp.sum(rest, axis=0, keepdims=True)
    outer = jnp.zeros((32, LANES), f32)
    cd = jnp.zeros((1, LANES), f32)
    for g in range(2):
        factor = factors[g]
        own = jnp.where(lane >> 5 == g, dens, 0.0)
        row = block_sum(own)
        column = jnp.sum(
            jnp.where(iota((32, LANES), 0) == iota((32, LANES), 1), row, 0.0), axis=1, keepdims=True
        )
        outer = outer + column * (factor * row)
        cd = cd + factor * own
    alpha = (gram[...] + (2.0 / NT) * outer - direct / NK) / NT
    half, corner = fold(alpha)
    wide[0:16, :] = keep_block(half, iota((16, LANES), 0) & 3)
    packed = wide[pl.ds(0, 4, stride=4), :]
    for c in range(1, 4):
        packed = packed + wide[pl.ds(c, 4, stride=4), :]
    tail = jnp.concatenate([packed, cd + corner, jnp.zeros((1, LANES), f32)], axis=0)
    for r in range(ROWS - NBB):
        lines[pl.ds(NBB + r, NA, stride=ROWS), :] = jnp.broadcast_to(tail[r : r + 1], (NA, LANES))
    msg[...] = lines[0 : NA * ROWS, :].astype(bf16)


def relay_kernel(got, msg, lines):
    lines[...] = got[...].astype(f32)
    alpha = []
    for r in range(4):
        part = lines[pl.ds(NBB + r, NA, stride=ROWS), :]
        alpha.append(jnp.sum(part, axis=0, keepdims=True))
    alpha = jnp.concatenate(alpha, axis=0)
    cd = lines[pl.ds(NBB + 4, NA, stride=ROWS), :]
    corner = jnp.sum(cd, axis=0, keepdims=True)
    cd = jnp.where(iota(cd.shape, 1) < 64, cd, 0.0)
    cd = cd[0 : NA // 2] + pltpu.roll(cd[NA // 2 :], 64, 1)
    hi = alpha.astype(bf16).astype(f32)
    lane = iota((4, LANES), 1)
    first = iota((4, LANES), 0) == 0
    rough = corner.astype(bf16).astype(f32)
    lo = jnp.where((lane & 31) < 16, alpha - hi, 0.0)
    lo = jnp.where(first & (lane >> 4 == 1), pltpu.roll(rough, LANES - 48, 1), lo)
    lo = jnp.where(first & (lane >> 4 == 3), pltpu.roll(corner - rough, LANES - 16, 1), lo)
    tail = jnp.concatenate([cd, hi, lo], axis=0).astype(bf16)
    for b in range(NBB):
        msg[b, 0:NA, :] = lines[pl.ds(b, NA, stride=ROWS), :].astype(bf16)
        msg[b, NA:WIDE, :] = tail


def finish_kernel(got, pairs, pe, vec, energy, out, alpha_out, wide, rows):
    x = spread_vectors(vec, wide)
    potential = got[:, 0:NA, :].reshape(ND, LANES)
    field = []
    for b in range(NBB):
        part = got[b, NA:FIELD, :].astype(f32)
        field += [part, pltpu.roll(part, 64, 1)]
    field = jnp.concatenate(field, axis=0).astype(bf16)
    direct = jnp.dot(pairs[...], potential, preferred_element_type=f32)
    direct = block_sum(keep_block(direct, iota(direct.shape, 0) >> 4))
    direct = jnp.concatenate([direct[0:16] + direct[16:32], direct[32:48] + direct[48:64]], axis=0)
    exchange = jnp.dot(exchange_rows(pe), field, preferred_element_type=f32)
    exchange = block_sum(keep_block(exchange, iota(exchange.shape, 0) >> 5))
    exchange = exchange[0:32] + exchange[32:64]
    applied = energy_column(energy) * x + (2.0 / NT) * exchange - direct / NK
    alpha = jnp.zeros((8, LANES), f32)
    for b in range(NBB):
        alpha = alpha + got[b, FIELD:WIDE, :].astype(f32)
    corner = alpha[4:5] + pltpu.roll(alpha[4:5], LANES - 32, 1)
    half = alpha[0:4] + jnp.where((iota((4, LANES), 1) & 31) < 16, alpha[4:8], 0.0)
    for c in range(4):
        wide[pl.ds(c, 4, stride=4), :] = half
    full = wide[0:16, :]
    full = unfold(block_sum(keep_block(full, iota(full.shape, 0) & 3)), corner)
    alpha_out[...] = full[:, 0:32]
    none = jnp.zeros((64, LANES), bf16)
    shift = jnp.dot(
        x.astype(bf16),
        jnp.concatenate([*halves(full), none], axis=0),
        preferred_element_type=f32,
    )
    rows[...] = keep_block(applied - shift, iota((32, LANES), 0) & 3)
    packed = rows[pl.ds(0, 8, stride=4), :]
    for c in range(1, 4):
        packed = packed + rows[pl.ds(c, 8, stride=4), :]
    for k in range(2):
        for v in range(4):
            out[k : k + 1, v * LANES : (v + 1) * LANES] = packed[k * 4 + v : k * 4 + v + 1, :]


def vmem():
    return pl.BlockSpec(memory_space=pltpu.VMEM)


def room(mib):
    return pltpu.CompilerParams(vmem_limit_bytes=mib << 20)


def in_hbm(x):
    return pltpu.with_memory_space_constraint(jnp.asarray(x), pltpu.HBM)


def sds(shape, dtype):
    return jax.ShapeDtypeStruct(shape, dtype)


def on_device(pair_exchange, conduction, valence, coulomb, screening, energies, vectors, k_coords):
    first, second, outer, inner = tables()
    far = (k_coords, conduction, valence, vectors, pair_exchange, energies, screening)
    far += (inner, outer, coulomb.reshape(8, LANES), first, second)
    any_space = pl.BlockSpec(memory_space=pl.ANY)
    own = [pltpu.VMEM(v.shape, v.dtype) for v in far[:6]]
    msg, pairs, gram, *kept = pl.pallas_call(
        pack_kernel,
        out_shape=(
            sds((2 * ND, LANES), bf16),
            sds((64, HALF), bf16),
            sds((32, LANES), f32),
            sds((NQ, 2 * LANES), f32),
            sds((24, 2 * SPAN), f32),
            sds((8, LANES), f32),
            sds((64, SPAN), bf16),
            sds((64, LANES), bf16),
            sds((2, NQ, LANES), f32),
        ),
        in_specs=[any_space] * len(far),
        out_specs=(vmem(),) * 9,
        scratch_shapes=own
        + [
            pltpu.VMEM((32, LANES), f32),
            pltpu.VMEM((64, HALF), f32),
            pltpu.VMEM((2 * ND, LANES), f32),
            pltpu.SemaphoreType.DMA((13,)),
        ],
        compiler_params=room(12),
        name="pack",
    )(*[in_hbm(v) for v in far])
    got = lax.all_to_all(msg.reshape(ND, 2, LANES), B + A, 0, 0, tiled=True)
    out = pl.pallas_call(
        spectral_kernel,
        out_shape=sds((NA * ROWS, LANES), bf16),
        in_specs=[vmem()] * 8,
        out_specs=vmem(),
        scratch_shapes=[
            pltpu.VMEM((max(2 * ND, NA * ROWS), LANES), f32),
            pltpu.VMEM((32, LANES), f32),
        ],
        compiler_params=room(28),
        name="spectral",
    )(got.reshape(2 * ND, LANES), gram, *kept)
    got = lax.all_to_all(out.reshape(NA, ROWS // 2, 2, LANES), A, 0, 0, tiled=True)
    out = pl.pallas_call(
        relay_kernel,
        out_shape=sds((NBB, WIDE, LANES), bf16),
        in_specs=[vmem()],
        out_specs=vmem(),
        scratch_shapes=[pltpu.VMEM((NA * ROWS, LANES), f32)],
        compiler_params=room(8),
        name="relay",
    )(got.reshape(NA * ROWS, LANES))
    got = lax.all_to_all(out, B, 0, 0, tiled=True)
    return pl.pallas_call(
        finish_kernel,
        out_shape=(sds((2, NB * NV), f32), sds((NV, NV), f32)),
        in_specs=[vmem()] * 5,
        out_specs=(vmem(), vmem()),
        scratch_shapes=[pltpu.VMEM((32, LANES), f32), pltpu.VMEM((32, LANES), f32)],
        compiler_params=room(8),
        name="finish",
    )(got, pairs, pair_exchange, vectors, energies)


def solution(mesh):
    split = Mesh(mesh.devices.reshape(SIZES), NAMES)
    return jax.shard_map(
        on_device,
        mesh=split,
        in_specs=(
            P(NAMES, None, None),
            P(NAMES, None, None),
            P(NAMES, None, None),
            P(),
            P(),
            P(NAMES, None),
            P(NAMES, None),
            P(NAMES, None),
        ),
        out_specs=(P(NAMES, None), P()),
        check_vma=False,
    )
```

```python
import jax
import jax.numpy as jnp
import numpy as np
from jax import lax
from jax.experimental import pallas as pl
from jax.experimental.pallas import tpu as pltpu
from jax.sharding import Mesh
from jax.sharding import PartitionSpec as P

MX = 32
MY = 32
NK = 1024
NB = 16
NG = 1024
NV = 32
NT = NK * NB
NQ = 289
SPAN = NK // 4
NAMES = ("zh", "zl", "yl", "c", "x", "yh")
SIZES = (4, 2, 2, 2, 4, 4)
A = ("yh", "yl", "zh")
B = ("c", "x", "zl")
NA = 32
NBB = 16
ND = NA * NBB
HALF = NG // 2
ROWS = NBB + 6
FIELD = NA + NA // 2
WIDE = FIELD + 8
LANES = 128

f32 = jnp.float32
bf16 = jnp.bfloat16


def split_table(x):
    hi = x.astype(bf16)
    lo = (x - hi.astype(np.float64)).astype(bf16)
    return np.concatenate([hi, lo], axis=0)


def tables():
    m = np.arange(32)
    phase = 2.0 * np.pi * ((m[:, None] * m[None, :]) % 32) / 32.0
    cas = np.cos(phase) + np.sin(phase)
    first = split_table(np.repeat(cas[:, 0:16], 16, axis=1))
    second = split_table(np.tile(cas[:, 0:16], (1, 8)) / 32.0)
    f = np.arange(17)
    weight = np.where((f == 0) | (f == 16), 1.0, 2.0)
    cos = weight[:, None] * np.cos(2.0 * np.pi * ((f[:, None] * m[None, :]) % 32) / 32.0)
    outer = np.zeros((24, 2 * SPAN), np.float32)
    outer[0:17] = np.repeat(cos, 16, axis=1)
    inner = np.concatenate(
        [np.tile(cos[:, h : h + 16], (17, LANES // 16)) for h in (0, 16)], axis=1
    ).astype(np.float32)
    return first, second, outer, inner


def iota(shape, axis):
    return lax.broadcasted_iota(jnp.int32, shape, axis)


def block_sum(x):
    x = x + pltpu.roll(x, 32, 1)
    return x + pltpu.roll(x, 64, 1)


def keep_block(x, wanted):
    return jnp.where(iota(x.shape, 1) >> 5 == wanted, x, 0.0)


def spread_vectors(vec_ref, wide):
    rows = [
        vec_ref[k : k + 1, v * LANES : (v + 1) * LANES].astype(f32)
        for k in range(2)
        for v in range(4)
    ]
    x8 = jnp.concatenate(rows, axis=0)
    for c in range(4):
        wide[pl.ds(c, 8, stride=4), :] = x8
    x = wide[...]
    return block_sum(keep_block(x, iota(x.shape, 0) & 3))


def energy_column(energy_ref):
    first = jnp.broadcast_to(energy_ref[0:1, :], (NB, NB))
    second = jnp.broadcast_to(energy_ref[1:2, :], (NB, NB))
    e = jnp.concatenate([first, second], axis=0)
    return jnp.sum(
        jnp.where(iota(e.shape, 1) == (iota(e.shape, 0) & (NB - 1)), e, 0.0), axis=1, keepdims=True
    )


def exchange_rows(pe_ref):
    return jnp.concatenate(
        [pe_ref[k, :, g * HALF : (g + 1) * HALF] for g in range(2) for k in range(2)], axis=0
    )


def halves(x):
    hi = x.astype(bf16)
    return hi, (x - hi.astype(f32)).astype(bf16)


def dot_t(x, y):
    return lax.dot_general(x, y, (((0,), (0,)), ((), ())), preferred_element_type=f32)


def dot_nt(x, y):
    return lax.dot_general(x, y, (((1,), (1,)), ((), ())), preferred_element_type=f32)


def spectrum(lane_at, tiles, outer, inner):
    own = iota((NQ, LANES), 1) == lane_at
    pick = jnp.where(iota((24, NQ), 0) == iota((24, NQ), 1) // 17, 1.0, 0.0).astype(bf16)
    parts = []
    for g in range(2):
        column = jnp.sum(jnp.where(own, tiles[g], 0.0), axis=1, keepdims=True)
        exact = column * inner[...]
        hi = exact.astype(bf16)
        lo = (exact - hi.astype(f32)).astype(bf16)
        parts.append(
            jnp.dot(pick, hi, preferred_element_type=f32)
            + jnp.dot(pick, lo, preferred_element_type=f32)
        )
    out = []
    for q in range(4):
        for g in range(2):
            part = parts[g][:, (q % 2) * LANES : (q % 2 + 1) * LANES]
            line = []
            for j in range(SPAN // LANES):
                at = (q // 2) * SPAN + j * LANES
                line.append(
                    jnp.sum(outer[:, at : at + LANES] * part, axis=0, keepdims=True)
                )
            out.append(jnp.concatenate(line, axis=1))
    return out


def pack_kernel(*refs):
    far, (msg, pairs, gram), kept = refs[:12], refs[12:15], refs[15:21]
    coords, cond, val, vec, pe, energy, wide, rows, lines, sem = refs[21:]
    inner, outer, bare, first, second, tiles = kept
    mine = lax.axis_index(B) * NA + lax.axis_index(A)
    tile = pl.multiple_of((mine // LANES) * LANES, LANES)
    near = (coords, cond, val, vec, pe, energy, inner, outer, bare, first, second)
    pairs_of = list(zip(far[:6] + far[7:], near))
    pairs_of += [(far[6].at[:, pl.ds(tile + g * HALF, LANES)], tiles.at[g]) for g in range(2)]
    copies = [
        pltpu.make_async_copy(src, dst, sem.at[i]) for i, (src, dst) in enumerate(pairs_of)
    ]
    for copy in copies:
        copy.start()
    for copy in copies[:4]:
        copy.wait()
    x = spread_vectors(vec, wide)
    for k in range(2):
        cf = cond[k].astype(f32)
        vf = val[k].astype(f32)
        for v in range(4):
            both = vf[v : v + 1, :] * cf
            for g in range(2):
                at = k * 32 + g * 16 + v * 4
                rows[at : at + 4, :] = both[:, g * HALF : (g + 1) * HALF]
    left = rows[...].astype(bf16)
    pairs[...] = left
    xp = jnp.concatenate([x[0:16], x[0:16], x[16:32], x[16:32]], axis=0)
    xp = keep_block(xp, iota(xp.shape, 0) >> 4).astype(bf16)
    xd = jnp.concatenate([x, x], axis=0)
    xd = keep_block(xd, iota(xd.shape, 0) >> 5).astype(bf16)
    lane = iota((1, LANES), 1)
    place = jnp.zeros((1, LANES), f32)
    for k in range(2):
        for s in range(2):
            at = coords[k : k + 1, s : s + 1]
            place = jnp.where(lane == 64 + 2 * k + s, at.astype(f32), place)
            place = jnp.where(lane == 68 + 2 * k + s, (1 - 2 * (at & 1)).astype(f32), place)
    lines[pl.ds(0, ND, stride=2), :] = dot_t(left, xp)
    for copy in copies[4:6]:
        copy.wait()
    lines[pl.ds(1, ND, stride=2), :] = dot_t(exchange_rows(pe), xd) + place
    msg[...] = lines[...].astype(bf16)
    hi, lo = halves(energy_column(energy) * x)
    twice = jnp.concatenate([x, x], axis=0).astype(bf16)
    gram[...] = dot_t(twice, jnp.concatenate([hi, lo], axis=0))[0:32]
    for copy in copies[6:]:
        copy.wait()


def fold(alpha):
    n = iota((16, LANES), 1) & 31
    row = iota((16, LANES), 0)
    last = pltpu.roll(alpha[16:32], LANES - 16, 1)
    half = jnp.where((row > n) & (n < 16), last, alpha[0:16])
    corner = jnp.where(iota((16, LANES), 1) == row + 64, last, 0.0)
    return half, jnp.sum(corner, axis=0, keepdims=True)


def unfold(half, corner):
    lane = iota((16, LANES), 1)
    row = iota((16, LANES), 0)
    half = jnp.where(lane < 32, half, 0.0)
    turned = jnp.transpose(jnp.concatenate([half, jnp.zeros((LANES - 16, LANES), f32)], axis=0))
    upper = jnp.where((lane < 16) & (row > lane), turned[0:16], half)
    last = jnp.where(row > lane - 16, pltpu.roll(half, 16, 1), pltpu.roll(turned[0:16], 16, 1))
    last = jnp.where(row == lane - 16, corner, last)
    lower = jnp.where(lane < 16, turned[16:32], jnp.where(lane < 32, last, 0.0))
    return block_sum(jnp.concatenate([upper, lower], axis=0))


def spectral_kernel(
    got, gram, inner, outer_table, bare, first, second, tiles, msg, lines, wide
):
    mine = lax.axis_index(B) * NA + lax.axis_index(A)
    lam = spectrum(mine % LANES, tiles, outer_table, inner)
    index = iota((8, LANES), 0) * LANES + iota((8, LANES), 1)
    factors = [
        jnp.sum(jnp.where(index == mine + g * HALF, bare[...], 0.0), keepdims=True)
        for g in range(2)
    ]
    lines[0 : 2 * ND, :] = got[...].astype(f32)
    proj = jnp.transpose(lines[pl.ds(0, ND, stride=2), :])
    rest = lines[pl.ds(1, ND, stride=2), :]
    turned = jnp.transpose(rest)
    slot = (iota((ND, 64), 1) & 31).astype(f32)
    left = iota((ND, LANES), 1) < 64
    basis, sign = [], []
    hat = None
    for k in range(2):
        ones = [
            jnp.where(slot == rest[:, 64 + 2 * k + s : 65 + 2 * k + s], 1.0, 0.0).astype(bf16)
            for s in range(2)
        ]
        ta = jnp.dot(ones[0], first[...], preferred_element_type=f32)
        tb = jnp.dot(ones[1], second[...], preferred_element_type=f32)
        exact = ta * jnp.concatenate([tb] * (SPAN // LANES), axis=1)
        hi = exact.astype(bf16)
        lo = (exact - hi.astype(f32)).astype(bf16)
        basis.append((hi, lo))
        sa, sb = [
            jnp.broadcast_to(rest[:, 68 + 2 * k + s : 69 + 2 * k + s], (ND, LANES))
            for s in range(2)
        ]
        sign.append((sb, sa, sa * sb))
        sa, sb = [turned[68 + 2 * k + s : 69 + 2 * k + s] for s in range(2)]
        own = proj[k * 64 : (k + 1) * 64]
        own = jnp.concatenate([own, own * sb, own * sa, own * (sa * sb)], axis=0).astype(bf16)
        part = jnp.dot(own, hi, preferred_element_type=f32) + jnp.dot(
            own, lo, preferred_element_type=f32
        )
        hat = part if hat is None else hat + part
    scale = jnp.concatenate(
        [jnp.broadcast_to(line, (32, SPAN)) for line in lam], axis=0
    )
    exact = hat * scale
    scaled = exact.astype(bf16)
    finer = (exact - scaled.astype(f32)).astype(bf16)
    hat = hat.astype(bf16)
    both = jnp.concatenate(
        [v[q * 64 : (q + 1) * 64] for q in range(4) for v in (scaled, finer)], axis=0
    )
    back = []
    for k in range(2):
        sb, sa, sab = sign[k]
        wide_r = dot_nt(basis[k][0], both)
        r = wide_r[:, 0:LANES] + sb * wide_r[:, LANES : 2 * LANES]
        r = r + sa * wide_r[:, 2 * LANES : 3 * LANES] + sab * wide_r[:, 3 * LANES : 4 * LANES]
        small = dot_nt(basis[k][1], scaled)
        r = r + jnp.where(left, 1.0, sb) * small[:, 0:LANES]
        r = r + jnp.where(left, sa, sab) * small[:, LANES : 2 * LANES]
        back.append(r + pltpu.roll(r, 64, 1))
    back = jnp.where(left, back[0], back[1])
    direct = None
    for g in range(2):
        x, y = [
            jnp.concatenate(
                [v[q * 64 + g * 32 : q * 64 + g * 32 + 32] for q in range(4)], axis=1
            )
            for v in (hat, scaled)
        ]
        part = dot_nt(x, jnp.concatenate([y] * 4, axis=0))
        direct = part if direct is None else direct + part
    for b in range(NBB):
        lines[pl.ds(b, NA, stride=ROWS), :] = back[b * NA : (b + 1) * NA]
    lane = iota((1, LANES), 1)
    dens = jnp.sum(rest, axis=0, keepdims=True)
    outer = jnp.zeros((32, LANES), f32)
    cd = jnp.zeros((1, LANES), f32)
    for g in range(2):
        factor = factors[g]
        own = jnp.where(lane >> 5 == g, dens, 0.0)
        row = block_sum(own)
        column = jnp.sum(
            jnp.where(iota((32, LANES), 0) == iota((32, LANES), 1), row, 0.0), axis=1, keepdims=True
        )
        outer = outer + column * (factor * row)
        cd = cd + factor * own
    alpha = (gram[...] + (2.0 / NT) * outer - direct / NK) / NT
    half, corner = fold(alpha)
    wide[0:16, :] = keep_block(half, iota((16, LANES), 0) & 3)
    packed = wide[pl.ds(0, 4, stride=4), :]
    for c in range(1, 4):
        packed = packed + wide[pl.ds(c, 4, stride=4), :]
    tail = jnp.concatenate([packed, cd + corner, jnp.zeros((1, LANES), f32)], axis=0)
    for r in range(ROWS - NBB):
        lines[pl.ds(NBB + r, NA, stride=ROWS), :] = jnp.broadcast_to(tail[r : r + 1], (NA, LANES))
    msg[...] = lines[0 : NA * ROWS, :].astype(bf16)


def relay_kernel(got, msg, lines):
    lines[...] = got[...].astype(f32)
    alpha = []
    for r in range(4):
        part = lines[pl.ds(NBB + r, NA, stride=ROWS), :]
        alpha.append(jnp.sum(part, axis=0, keepdims=True))
    alpha = jnp.concatenate(alpha, axis=0)
    cd = lines[pl.ds(NBB + 4, NA, stride=ROWS), :]
    corner = jnp.sum(cd, axis=0, keepdims=True)
    cd = jnp.where(iota(cd.shape, 1) < 64, cd, 0.0)
    cd = cd[0 : NA // 2] + pltpu.roll(cd[NA // 2 :], 64, 1)
    hi = alpha.astype(bf16).astype(f32)
    lane = iota((4, LANES), 1)
    first = iota((4, LANES), 0) == 0
    rough = corner.astype(bf16).astype(f32)
    lo = jnp.where((lane & 31) < 16, alpha - hi, 0.0)
    lo = jnp.where(first & (lane >> 4 == 1), pltpu.roll(rough, LANES - 48, 1), lo)
    lo = jnp.where(first & (lane >> 4 == 3), pltpu.roll(corner - rough, LANES - 16, 1), lo)
    tail = jnp.concatenate([cd, hi, lo], axis=0).astype(bf16)
    for b in range(NBB):
        msg[b, 0:NA, :] = lines[pl.ds(b, NA, stride=ROWS), :].astype(bf16)
        msg[b, NA:WIDE, :] = tail


def finish_kernel(got, pairs, pe, vec, energy, out, alpha_out, wide, rows):
    x = spread_vectors(vec, wide)
    potential = got[:, 0:NA, :].reshape(ND, LANES)
    field = []
    for b in range(NBB):
        part = got[b, NA:FIELD, :].astype(f32)
        field += [part, pltpu.roll(part, 64, 1)]
    field = jnp.concatenate(field, axis=0).astype(bf16)
    direct = jnp.dot(pairs[...], potential, preferred_element_type=f32)
    direct = block_sum(keep_block(direct, iota(direct.shape, 0) >> 4))
    direct = jnp.concatenate([direct[0:16] + direct[16:32], direct[32:48] + direct[48:64]], axis=0)
    exchange = jnp.dot(exchange_rows(pe), field, preferred_element_type=f32)
    exchange = block_sum(keep_block(exchange, iota(exchange.shape, 0) >> 5))
    exchange = exchange[0:32] + exchange[32:64]
    applied = energy_column(energy) * x + (2.0 / NT) * exchange - direct / NK
    alpha = jnp.zeros((8, LANES), f32)
    for b in range(NBB):
        alpha = alpha + got[b, FIELD:WIDE, :].astype(f32)
    corner = alpha[4:5] + pltpu.roll(alpha[4:5], LANES - 32, 1)
    half = alpha[0:4] + jnp.where((iota((4, LANES), 1) & 31) < 16, alpha[4:8], 0.0)
    for c in range(4):
        wide[pl.ds(c, 4, stride=4), :] = half
    full = wide[0:16, :]
    full = unfold(block_sum(keep_block(full, iota(full.shape, 0) & 3)), corner)
    alpha_out[...] = full[:, 0:32]
    none = jnp.zeros((64, LANES), bf16)
    shift = jnp.dot(
        x.astype(bf16),
        jnp.concatenate([*halves(full), none], axis=0),
        preferred_element_type=f32,
    )
    rows[...] = keep_block(applied - shift, iota((32, LANES), 0) & 3)
    packed = rows[pl.ds(0, 8, stride=4), :]
    for c in range(1, 4):
        packed = packed + rows[pl.ds(c, 8, stride=4), :]
    for k in range(2):
        for v in range(4):
            out[k : k + 1, v * LANES : (v + 1) * LANES] = packed[k * 4 + v : k * 4 + v + 1, :]


def vmem():
    return pl.BlockSpec(memory_space=pltpu.VMEM)


def room(mib):
    return pltpu.CompilerParams(vmem_limit_bytes=mib << 20)


def in_hbm(x):
    return pltpu.with_memory_space_constraint(jnp.asarray(x), pltpu.HBM)


def sds(shape, dtype):
    return jax.ShapeDtypeStruct(shape, dtype)


def on_device(pair_exchange, conduction, valence, coulomb, screening, energies, vectors, k_coords):
    first, second, outer, inner = tables()
    far = (k_coords, conduction, valence, vectors, pair_exchange, energies, screening)
    far += (inner, outer, coulomb.reshape(8, LANES), first, second)
    any_space = pl.BlockSpec(memory_space=pl.ANY)
    own = [pltpu.VMEM(v.shape, v.dtype) for v in far[:6]]
    msg, pairs, gram, *kept = pl.pallas_call(
        pack_kernel,
        out_shape=(
            sds((2 * ND, LANES), bf16),
            sds((64, HALF), bf16),
            sds((32, LANES), f32),
            sds((NQ, 2 * LANES), f32),
            sds((24, 2 * SPAN), f32),
            sds((8, LANES), f32),
            sds((64, SPAN), bf16),
            sds((64, LANES), bf16),
            sds((2, NQ, LANES), f32),
        ),
        in_specs=[any_space] * len(far),
        out_specs=(vmem(),) * 9,
        scratch_shapes=own
        + [
            pltpu.VMEM((32, LANES), f32),
            pltpu.VMEM((64, HALF), f32),
            pltpu.VMEM((2 * ND, LANES), f32),
            pltpu.SemaphoreType.DMA((13,)),
        ],
        compiler_params=room(12),
        name="pack",
    )(*[in_hbm(v) for v in far])
    got = lax.all_to_all(msg.reshape(ND, 2, LANES), B + A, 0, 0, tiled=True)
    out = pl.pallas_call(
        spectral_kernel,
        out_shape=sds((NA * ROWS, LANES), bf16),
        in_specs=[vmem()] * 8,
        out_specs=vmem(),
        scratch_shapes=[
            pltpu.VMEM((max(2 * ND, NA * ROWS), LANES), f32),
            pltpu.VMEM((32, LANES), f32),
        ],
        compiler_params=room(28),
        name="spectral",
    )(got.reshape(2 * ND, LANES), gram, *kept)
    got = lax.all_to_all(out.reshape(NA, ROWS // 2, 2, LANES), A, 0, 0, tiled=True)
    out = pl.pallas_call(
        relay_kernel,
        out_shape=sds((NBB, WIDE, LANES), bf16),
        in_specs=[vmem()],
        out_specs=vmem(),
        scratch_shapes=[pltpu.VMEM((NA * ROWS, LANES), f32)],
        compiler_params=room(8),
        name="relay",
    )(got.reshape(NA * ROWS, LANES))
    got = lax.all_to_all(out, B, 0, 0, tiled=True)
    return pl.pallas_call(
        finish_kernel,
        out_shape=(sds((2, NB * NV), f32), sds((NV, NV), f32)),
        in_specs=[vmem()] * 5,
        out_specs=(vmem(), vmem()),
        scratch_shapes=[pltpu.VMEM((32, LANES), f32), pltpu.VMEM((32, LANES), f32)],
        compiler_params=room(8),
        name="finish",
    )(got, pairs, pair_exchange, vectors, energies)


def solution(mesh):
    split = Mesh(mesh.devices.reshape(SIZES), NAMES)
    return jax.shard_map(
        on_device,
        mesh=split,
        in_specs=(
            P(NAMES, None, None),
            P(NAMES, None, None),
            P(NAMES, None, None),
            P(),
            P(),
            P(NAMES, None),
            P(NAMES, None),
            P(NAMES, None),
        ),
        out_specs=(P(NAMES, None), P()),
        check_vma=False,
    )
```

```python
import jax
import jax.numpy as jnp
import numpy as np
from jax import lax
from jax.experimental import pallas as pl
from jax.experimental.pallas import tpu as pltpu
from jax.sharding import Mesh
from jax.sharding import PartitionSpec as P

MX = 32
MY = 32
NK = 1024
NB = 16
NG = 1024
NV = 32
NT = NK * NB
NQ = 289
SPAN = NK // 4
NAMES = ("zh", "zl", "yl", "c", "x", "yh")
SIZES = (4, 2, 2, 2, 4, 4)
A = ("zh", "yh", "yl")
B = ("c", "x", "zl")
NA = 32
NBB = 16
ND = NA * NBB
HALF = NG // 2
ROWS = NBB + 6
FIELD = NA + NA // 2
WIDE = FIELD + 8
LANES = 128

f32 = jnp.float32
bf16 = jnp.bfloat16


def split_table(x):
    hi = x.astype(bf16)
    lo = (x - hi.astype(np.float64)).astype(bf16)
    return np.concatenate([hi, lo], axis=0)


def tables():
    m = np.arange(32)
    phase = 2.0 * np.pi * ((m[:, None] * m[None, :]) % 32) / 32.0
    cas = np.cos(phase) + np.sin(phase)
    first = split_table(np.repeat(cas[:, 0:16], 16, axis=1))
    second = split_table(np.tile(cas[:, 0:16], (1, 8)) / 32.0)
    f = np.arange(17)
    weight = np.where((f == 0) | (f == 16), 1.0, 2.0)
    cos = weight[:, None] * np.cos(2.0 * np.pi * ((f[:, None] * m[None, :]) % 32) / 32.0)
    outer = np.zeros((24, 2 * SPAN), np.float32)
    outer[0:17] = np.repeat(cos, 16, axis=1)
    inner = np.concatenate(
        [np.tile(cos[:, h : h + 16], (17, LANES // 16)) for h in (0, 16)], axis=1
    ).astype(np.float32)
    return first, second, outer, inner


def iota(shape, axis):
    return lax.broadcasted_iota(jnp.int32, shape, axis)


def block_sum(x):
    x = x + pltpu.roll(x, 32, 1)
    return x + pltpu.roll(x, 64, 1)


def keep_block(x, wanted):
    return jnp.where(iota(x.shape, 1) >> 5 == wanted, x, 0.0)


def spread_vectors(vec_ref, wide):
    rows = [
        vec_ref[k : k + 1, v * LANES : (v + 1) * LANES].astype(f32)
        for k in range(2)
        for v in range(4)
    ]
    x8 = jnp.concatenate(rows, axis=0)
    for c in range(4):
        wide[pl.ds(c, 8, stride=4), :] = x8
    x = wide[...]
    return block_sum(keep_block(x, iota(x.shape, 0) & 3))


def energy_column(energy_ref):
    first = jnp.broadcast_to(energy_ref[0:1, :], (NB, NB))
    second = jnp.broadcast_to(energy_ref[1:2, :], (NB, NB))
    e = jnp.concatenate([first, second], axis=0)
    return jnp.sum(
        jnp.where(iota(e.shape, 1) == (iota(e.shape, 0) & (NB - 1)), e, 0.0), axis=1, keepdims=True
    )


def exchange_rows(pe_ref):
    return jnp.concatenate(
        [pe_ref[k, :, g * HALF : (g + 1) * HALF] for g in range(2) for k in range(2)], axis=0
    )


def halves(x):
    hi = x.astype(bf16)
    return hi, (x - hi.astype(f32)).astype(bf16)


def dot_t(x, y):
    return lax.dot_general(x, y, (((0,), (0,)), ((), ())), preferred_element_type=f32)


def dot_nt(x, y):
    return lax.dot_general(x, y, (((1,), (1,)), ((), ())), preferred_element_type=f32)


def spectrum(lane_at, tiles, outer, inner):
    own = iota((NQ, LANES), 1) == lane_at
    pick = jnp.where(iota((24, NQ), 0) == iota((24, NQ), 1) // 17, 1.0, 0.0).astype(bf16)
    parts = []
    for g in range(2):
        column = jnp.sum(jnp.where(own, tiles[g], 0.0), axis=1, keepdims=True)
        exact = column * inner[...]
        hi = exact.astype(bf16)
        lo = (exact - hi.astype(f32)).astype(bf16)
        parts.append(
            jnp.dot(pick, hi, preferred_element_type=f32)
            + jnp.dot(pick, lo, preferred_element_type=f32)
        )
    out = []
    for q in range(4):
        for g in range(2):
            part = parts[g][:, (q % 2) * LANES : (q % 2 + 1) * LANES]
            line = []
            for j in range(SPAN // LANES):
                at = (q // 2) * SPAN + j * LANES
                line.append(
                    jnp.sum(outer[:, at : at + LANES] * part, axis=0, keepdims=True)
                )
            out.append(jnp.concatenate(line, axis=1))
    return out


def pack_kernel(*refs):
    far, (msg, pairs, gram), kept = refs[:12], refs[12:15], refs[15:21]
    coords, cond, val, vec, pe, energy, wide, rows, lines, sem = refs[21:]
    inner, outer, bare, first, second, tiles = kept
    mine = lax.axis_index(B) * NA + lax.axis_index(A)
    tile = pl.multiple_of((mine // LANES) * LANES, LANES)
    near = (coords, cond, val, vec, pe, energy, inner, outer, bare, first, second)
    pairs_of = list(zip(far[:6] + far[7:], near))
    pairs_of += [(far[6].at[:, pl.ds(tile + g * HALF, LANES)], tiles.at[g]) for g in range(2)]
    copies = [
        pltpu.make_async_copy(src, dst, sem.at[i]) for i, (src, dst) in enumerate(pairs_of)
    ]
    for copy in copies:
        copy.start()
    for copy in copies[:6]:
        copy.wait()
    x = spread_vectors(vec, wide)
    for k in range(2):
        cf = cond[k].astype(f32)
        vf = val[k].astype(f32)
        for v in range(4):
            both = vf[v : v + 1, :] * cf
            for g in range(2):
                at = k * 32 + g * 16 + v * 4
                rows[at : at + 4, :] = both[:, g * HALF : (g + 1) * HALF]
    left = rows[...].astype(bf16)
    pairs[...] = left
    xp = jnp.concatenate([x[0:16], x[0:16], x[16:32], x[16:32]], axis=0)
    xp = keep_block(xp, iota(xp.shape, 0) >> 4).astype(bf16)
    xd = jnp.concatenate([x, x], axis=0)
    xd = keep_block(xd, iota(xd.shape, 0) >> 5).astype(bf16)
    lane = iota((1, LANES), 1)
    place = jnp.zeros((1, LANES), f32)
    for k in range(2):
        for s in range(2):
            at = coords[k : k + 1, s : s + 1]
            place = jnp.where(lane == 64 + 2 * k + s, at.astype(f32), place)
            place = jnp.where(lane == 68 + 2 * k + s, (1 - 2 * (at & 1)).astype(f32), place)
    lines[pl.ds(0, ND, stride=2), :] = dot_t(left, xp)
    lines[pl.ds(1, ND, stride=2), :] = dot_t(exchange_rows(pe), xd) + place
    msg[...] = lines[...].astype(bf16)
    hi, lo = halves(energy_column(energy) * x)
    twice = jnp.concatenate([x, x], axis=0).astype(bf16)
    gram[...] = dot_t(twice, jnp.concatenate([hi, lo], axis=0))[0:32]
    for copy in copies[6:]:
        copy.wait()


def fold(alpha):
    n = iota((16, LANES), 1) & 31
    row = iota((16, LANES), 0)
    last = pltpu.roll(alpha[16:32], LANES - 16, 1)
    half = jnp.where((row > n) & (n < 16), last, alpha[0:16])
    corner = jnp.where(iota((16, LANES), 1) == row + 64, last, 0.0)
    return half, jnp.sum(corner, axis=0, keepdims=True)


def unfold(half, corner):
    lane = iota((16, LANES), 1)
    row = iota((16, LANES), 0)
    half = jnp.where(lane < 32, half, 0.0)
    turned = jnp.transpose(jnp.concatenate([half, jnp.zeros((LANES - 16, LANES), f32)], axis=0))
    upper = jnp.where((lane < 16) & (row > lane), turned[0:16], half)
    last = jnp.where(row > lane - 16, pltpu.roll(half, 16, 1), pltpu.roll(turned[0:16], 16, 1))
    last = jnp.where(row == lane - 16, corner, last)
    lower = jnp.where(lane < 16, turned[16:32], jnp.where(lane < 32, last, 0.0))
    return block_sum(jnp.concatenate([upper, lower], axis=0))


def spectral_kernel(
    got, gram, inner, outer_table, bare, first, second, tiles, msg, lines, wide
):
    mine = lax.axis_index(B) * NA + lax.axis_index(A)
    lam = spectrum(mine % LANES, tiles, outer_table, inner)
    index = iota((8, LANES), 0) * LANES + iota((8, LANES), 1)
    factors = [
        jnp.sum(jnp.where(index == mine + g * HALF, bare[...], 0.0), keepdims=True)
        for g in range(2)
    ]
    lines[0 : 2 * ND, :] = got[...].astype(f32)
    proj = jnp.transpose(lines[pl.ds(0, ND, stride=2), :])
    rest = lines[pl.ds(1, ND, stride=2), :]
    turned = jnp.transpose(rest)
    slot = (iota((ND, 64), 1) & 31).astype(f32)
    left = iota((ND, LANES), 1) < 64
    basis, sign = [], []
    hat = None
    for k in range(2):
        ones = [
            jnp.where(slot == rest[:, 64 + 2 * k + s : 65 + 2 * k + s], 1.0, 0.0).astype(bf16)
            for s in range(2)
        ]
        ta = jnp.dot(ones[0], first[...], preferred_element_type=f32)
        tb = jnp.dot(ones[1], second[...], preferred_element_type=f32)
        exact = ta * jnp.concatenate([tb] * (SPAN // LANES), axis=1)
        hi = exact.astype(bf16)
        lo = (exact - hi.astype(f32)).astype(bf16)
        basis.append((hi, lo))
        sa, sb = [
            jnp.broadcast_to(rest[:, 68 + 2 * k + s : 69 + 2 * k + s], (ND, LANES))
            for s in range(2)
        ]
        sign.append((sb, sa, sa * sb))
        sa, sb = [turned[68 + 2 * k + s : 69 + 2 * k + s] for s in range(2)]
        own = proj[k * 64 : (k + 1) * 64]
        own = jnp.concatenate([own, own * sb, own * sa, own * (sa * sb)], axis=0).astype(bf16)
        part = jnp.dot(own, hi, preferred_element_type=f32) + jnp.dot(
            own, lo, preferred_element_type=f32
        )
        hat = part if hat is None else hat + part
    scale = jnp.concatenate(
        [jnp.broadcast_to(line, (32, SPAN)) for line in lam], axis=0
    )
    exact = hat * scale
    scaled = exact.astype(bf16)
    finer = (exact - scaled.astype(f32)).astype(bf16)
    hat = hat.astype(bf16)
    both = jnp.concatenate(
        [v[q * 64 : (q + 1) * 64] for q in range(4) for v in (scaled, finer)], axis=0
    )
    back = []
    for k in range(2):
        sb, sa, sab = sign[k]
        wide_r = dot_nt(basis[k][0], both)
        r = wide_r[:, 0:LANES] + sb * wide_r[:, LANES : 2 * LANES]
        r = r + sa * wide_r[:, 2 * LANES : 3 * LANES] + sab * wide_r[:, 3 * LANES : 4 * LANES]
        small = dot_nt(basis[k][1], scaled)
        r = r + jnp.where(left, 1.0, sb) * small[:, 0:LANES]
        r = r + jnp.where(left, sa, sab) * small[:, LANES : 2 * LANES]
        back.append(r + pltpu.roll(r, 64, 1))
    back = jnp.where(left, back[0], back[1])
    direct = None
    for g in range(2):
        x, y = [
            jnp.concatenate(
                [v[q * 64 + g * 32 : q * 64 + g * 32 + 32] for q in range(4)], axis=1
            )
            for v in (hat, scaled)
        ]
        part = dot_nt(x, jnp.concatenate([y] * 4, axis=0))
        direct = part if direct is None else direct + part
    for b in range(NBB):
        lines[pl.ds(b, NA, stride=ROWS), :] = back[b * NA : (b + 1) * NA]
    lane = iota((1, LANES), 1)
    dens = jnp.sum(rest, axis=0, keepdims=True)
    outer = jnp.zeros((32, LANES), f32)
    cd = jnp.zeros((1, LANES), f32)
    for g in range(2):
        factor = factors[g]
        own = jnp.where(lane >> 5 == g, dens, 0.0)
        row = block_sum(own)
        column = jnp.sum(
            jnp.where(iota((32, LANES), 0) == iota((32, LANES), 1), row, 0.0), axis=1, keepdims=True
        )
        outer = outer + column * (factor * row)
        cd = cd + factor * own
    alpha = (gram[...] + (2.0 / NT) * outer - direct / NK) / NT
    half, corner = fold(alpha)
    wide[0:16, :] = keep_block(half, iota((16, LANES), 0) & 3)
    packed = wide[pl.ds(0, 4, stride=4), :]
    for c in range(1, 4):
        packed = packed + wide[pl.ds(c, 4, stride=4), :]
    tail = jnp.concatenate([packed, cd + corner, jnp.zeros((1, LANES), f32)], axis=0)
    for r in range(ROWS - NBB):
        lines[pl.ds(NBB + r, NA, stride=ROWS), :] = jnp.broadcast_to(tail[r : r + 1], (NA, LANES))
    msg[...] = lines[0 : NA * ROWS, :].astype(bf16)


def relay_kernel(got, msg, lines):
    lines[...] = got[...].astype(f32)
    alpha = []
    for r in range(4):
        part = lines[pl.ds(NBB + r, NA, stride=ROWS), :]
        alpha.append(jnp.sum(part, axis=0, keepdims=True))
    alpha = jnp.concatenate(alpha, axis=0)
    cd = lines[pl.ds(NBB + 4, NA, stride=ROWS), :]
    corner = jnp.sum(cd, axis=0, keepdims=True)
    cd = jnp.where(iota(cd.shape, 1) < 64, cd, 0.0)
    cd = cd[0 : NA // 2] + pltpu.roll(cd[NA // 2 :], 64, 1)
    hi = alpha.astype(bf16).astype(f32)
    lane = iota((4, LANES), 1)
    first = iota((4, LANES), 0) == 0
    rough = corner.astype(bf16).astype(f32)
    lo = jnp.where((lane & 31) < 16, alpha - hi, 0.0)
    lo = jnp.where(first & (lane >> 4 == 1), pltpu.roll(rough, LANES - 48, 1), lo)
    lo = jnp.where(first & (lane >> 4 == 3), pltpu.roll(corner - rough, LANES - 16, 1), lo)
    tail = jnp.concatenate([cd, hi, lo], axis=0).astype(bf16)
    for b in range(NBB):
        msg[b, 0:NA, :] = lines[pl.ds(b, NA, stride=ROWS), :].astype(bf16)
        msg[b, NA:WIDE, :] = tail


def finish_kernel(got, pairs, pe, vec, energy, out, alpha_out, wide, rows):
    x = spread_vectors(vec, wide)
    potential = got[:, 0:NA, :].reshape(ND, LANES)
    field = []
    for b in range(NBB):
        part = got[b, NA:FIELD, :].astype(f32)
        field += [part, pltpu.roll(part, 64, 1)]
    field = jnp.concatenate(field, axis=0).astype(bf16)
    direct = jnp.dot(pairs[...], potential, preferred_element_type=f32)
    direct = block_sum(keep_block(direct, iota(direct.shape, 0) >> 4))
    direct = jnp.concatenate([direct[0:16] + direct[16:32], direct[32:48] + direct[48:64]], axis=0)
    exchange = jnp.dot(exchange_rows(pe), field, preferred_element_type=f32)
    exchange = block_sum(keep_block(exchange, iota(exchange.shape, 0) >> 5))
    exchange = exchange[0:32] + exchange[32:64]
    applied = energy_column(energy) * x + (2.0 / NT) * exchange - direct / NK
    alpha = jnp.zeros((8, LANES), f32)
    for b in range(NBB):
        alpha = alpha + got[b, FIELD:WIDE, :].astype(f32)
    corner = alpha[4:5] + pltpu.roll(alpha[4:5], LANES - 32, 1)
    half = alpha[0:4] + jnp.where((iota((4, LANES), 1) & 31) < 16, alpha[4:8], 0.0)
    for c in range(4):
        wide[pl.ds(c, 4, stride=4), :] = half
    full = wide[0:16, :]
    full = unfold(block_sum(keep_block(full, iota(full.shape, 0) & 3)), corner)
    alpha_out[...] = full[:, 0:32]
    none = jnp.zeros((64, LANES), bf16)
    shift = jnp.dot(
        x.astype(bf16),
        jnp.concatenate([*halves(full), none], axis=0),
        preferred_element_type=f32,
    )
    rows[...] = keep_block(applied - shift, iota((32, LANES), 0) & 3)
    packed = rows[pl.ds(0, 8, stride=4), :]
    for c in range(1, 4):
        packed = packed + rows[pl.ds(c, 8, stride=4), :]
    for k in range(2):
        for v in range(4):
            out[k : k + 1, v * LANES : (v + 1) * LANES] = packed[k * 4 + v : k * 4 + v + 1, :]


def vmem():
    return pl.BlockSpec(memory_space=pltpu.VMEM)


def room(mib):
    return pltpu.CompilerParams(vmem_limit_bytes=mib << 20)


def in_hbm(x):
    return pltpu.with_memory_space_constraint(jnp.asarray(x), pltpu.HBM)


def sds(shape, dtype):
    return jax.ShapeDtypeStruct(shape, dtype)


def on_device(pair_exchange, conduction, valence, coulomb, screening, energies, vectors, k_coords):
    first, second, outer, inner = tables()
    far = (k_coords, conduction, valence, vectors, pair_exchange, energies, screening)
    far += (inner, outer, coulomb.reshape(8, LANES), first, second)
    any_space = pl.BlockSpec(memory_space=pl.ANY)
    own = [pltpu.VMEM(v.shape, v.dtype) for v in far[:6]]
    msg, pairs, gram, *kept = pl.pallas_call(
        pack_kernel,
        out_shape=(
            sds((2 * ND, LANES), bf16),
            sds((64, HALF), bf16),
            sds((32, LANES), f32),
            sds((NQ, 2 * LANES), f32),
            sds((24, 2 * SPAN), f32),
            sds((8, LANES), f32),
            sds((64, SPAN), bf16),
            sds((64, LANES), bf16),
            sds((2, NQ, LANES), f32),
        ),
        in_specs=[any_space] * len(far),
        out_specs=(vmem(),) * 9,
        scratch_shapes=own
        + [
            pltpu.VMEM((32, LANES), f32),
            pltpu.VMEM((64, HALF), f32),
            pltpu.VMEM((2 * ND, LANES), f32),
            pltpu.SemaphoreType.DMA((13,)),
        ],
        compiler_params=room(12),
        name="pack",
    )(*[in_hbm(v) for v in far])
    got = lax.all_to_all(msg.reshape(ND, 2, LANES), B + A, 0, 0, tiled=True)
    out = pl.pallas_call(
        spectral_kernel,
        out_shape=sds((NA * ROWS, LANES), bf16),
        in_specs=[vmem()] * 8,
        out_specs=vmem(),
        scratch_shapes=[
            pltpu.VMEM((max(2 * ND, NA * ROWS), LANES), f32),
            pltpu.VMEM((32, LANES), f32),
        ],
        compiler_params=room(28),
        name="spectral",
    )(got.reshape(2 * ND, LANES), gram, *kept)
    got = lax.all_to_all(out.reshape(NA, ROWS // 2, 2, LANES), A, 0, 0, tiled=True)
    out = pl.pallas_call(
        relay_kernel,
        out_shape=sds((NBB, WIDE, LANES), bf16),
        in_specs=[vmem()],
        out_specs=vmem(),
        scratch_shapes=[pltpu.VMEM((NA * ROWS, LANES), f32)],
        compiler_params=room(8),
        name="relay",
    )(got.reshape(NA * ROWS, LANES))
    got = lax.all_to_all(out, B, 0, 0, tiled=True)
    return pl.pallas_call(
        finish_kernel,
        out_shape=(sds((2, NB * NV), f32), sds((NV, NV), f32)),
        in_specs=[vmem()] * 5,
        out_specs=(vmem(), vmem()),
        scratch_shapes=[pltpu.VMEM((32, LANES), f32), pltpu.VMEM((32, LANES), f32)],
        compiler_params=room(8),
        name="finish",
    )(got, pairs, pair_exchange, vectors, energies)


def solution(mesh):
    split = Mesh(mesh.devices.reshape(SIZES), NAMES)
    return jax.shard_map(
        on_device,
        mesh=split,
        in_specs=(
            P(NAMES, None, None),
            P(NAMES, None, None),
            P(NAMES, None, None),
            P(),
            P(),
            P(NAMES, None),
            P(NAMES, None),
            P(NAMES, None),
        ),
        out_specs=(P(NAMES, None), P()),
        check_vma=False,
    )
```
